32 devices in a mesh: gx: 2 (over x), gy: 4 (over z), band: 4 (over y, core).
Axes of the slice: x: 2, y: 2, z: 4, core: 2. Of those that a mesh axis runs over, the one named last changes fastest.
Arguments:
- orbitals: float32 [2, 16, 16, 48, 128], P(None, 'band', 'gx', 'gy'), may hold values from -3 to 3
- external: float32 [16, 48, 128], P('gx', 'gy'), may hold values from 2 to 6
Outputs:
- orbitals_next: float32 [2, 16, 16, 48, 128], P(None, 'band', 'gx', 'gy')
- potential_next: float32 [16, 48, 128], P('gx', 'gy')
The draws below stay inside these ranges and needn't reach their ends.
All inputs are finite; a program needn't handle non-finite values.
Results may differ from the reference program's by a relative error of at most 0.00002.
Values sent between devices are 32-bit elements; how exact they have to be, the bound alone decides.
A program may use at most 64 MiB of HBM per device.

```python
import jax
import jax.numpy as jnp
from jax import lax

NZ = 128
BANDS = 16
NX = 16
NY = 48


def draw_orbitals(key, part):
    shape = (2, BANDS, NX, NY, NZ)
    first_rows = jnp.arange(NX, dtype=jnp.int32)[:, None, None]
    second_rows = jnp.arange(NY, dtype=jnp.int32)[None, :, None]
    third_rows = jnp.arange(NZ, dtype=jnp.int32)[None, None, :]
    parity = (first_rows + second_rows + third_rows) % 2
    pattern = (1 - 2 * parity).astype(jnp.float32)
    amplitude = jax.random.uniform(key, shape, jnp.float32, 0.5, 2.0)
    return (amplitude * pattern[None, None]).astype(jnp.float32)


def level_of(stream_key, shape, split, low, high):
    def one(axis_at, blocks):
        heights = jax.random.uniform(jax.random.fold_in(jax.random.fold_in(stream_key, 6), axis_at), (blocks,), jnp.float32, low / len(split), high / len(split))
        return jnp.repeat(jnp.exp(heights), shape[axis_at] // blocks).reshape((-1,) + (1,) * (len(shape) - axis_at - 1))

    loudness = one(*split[0])
    for cut in split[1:]:
        loudness = loudness * one(*cut)
    return loudness


def setup_inputs(seed: int = 0) -> dict:
    streams_of = jax.random.split(jax.random.key(seed), 3)
    return {
        "orbitals": draw_orbitals(jax.random.fold_in(streams_of[2], 71), 0),
        "external": jnp.clip(2.0 + 4.0 * jax.random.uniform(streams_of[1], (NX, NY, NZ), jnp.float32) ** level_of(streams_of[1], (NX, NY, NZ), ((0, 2), (1, 4)), -0.2, 0.2), 2.0, 6.0),
    }


step_length = 0.15
exchange_coef = 0.7386
centre_weight = -2.5
near_weight = 4.0 / 3.0
far_weight = -1.0 / 12.0


def shifted(padded, which_axis, offset):
    dimensions = padded.ndim
    selector = []
    for position in range(dimensions):
        if position < dimensions - 3:
            selector.append(slice(None))
        elif position == which_axis:
            selector.append(slice(2 + offset, padded.shape[position] - 2 + offset))
        else:
            selector.append(slice(2, padded.shape[position] - 2))
    return padded[tuple(selector)]


def laplacian(padded):
    dimensions = padded.ndim
    centre = shifted(padded, dimensions - 1, 0)
    summed = 3.0 * centre_weight * centre
    for which_axis in range(dimensions - 3, dimensions):
        summed = summed + near_weight * (shifted(padded, which_axis, 1) + shifted(padded, which_axis, -1))
        summed = summed + far_weight * (shifted(padded, which_axis, 2) + shifted(padded, which_axis, -2))
    return summed


def taylor(values, apply_fn, interval):
    summed = values
    taylor_term = values
    for degree in range(1, 5):
        image = apply_fn(taylor_term)
        factor = interval / degree
        taylor_term = jnp.stack([factor * image[1], -factor * image[0]])
        summed = summed + taylor_term
    return summed


def hamiltonian(values, potential):
    padded = jnp.pad(values, ((0, 0), (2, 2), (2, 2), (2, 2)))
    return -0.5 * laplacian(padded) + potential * values


def reference(orbitals, external):
    density_now = jnp.sum(orbitals * orbitals, axis=(0, 1))
    potential_now = external - exchange_coef * jnp.cbrt(density_now)
    by_band = jnp.moveaxis(orbitals, 1, 0)

    def apply_now(values):
        return hamiltonian(values, potential_now)

    def predict(values):
        return taylor(values, apply_now, step_length)

    predicted = lax.map(predict, by_band)
    density_next = jnp.sum(predicted * predicted, axis=(0, 1))
    potential_next = external - exchange_coef * jnp.cbrt(density_next)

    def apply_next(values):
        return hamiltonian(values, potential_next)

    def finish(values):
        halfway = taylor(values, apply_now, step_length / 2)
        return taylor(halfway, apply_next, step_length / 2)

    result = lax.map(finish, by_band)
    return jnp.moveaxis(result, 0, 1), potential_next
```

```python
import functools

import jax
import jax.numpy as jnp
from jax import lax
from jax.experimental import pallas as pl
from jax.experimental.pallas import tpu as pltpu
from jax.sharding import PartitionSpec as P

step_length = 0.15
exchange_coef = 0.7386
centre_weight = -2.5
near_weight = 4.0 / 3.0
far_weight = -1.0 / 12.0
MESH = pl.DeviceIdType.MESH


def cube_root(d):
    guess = jnp.exp(jnp.log(d) * (1.0 / 3.0))
    better = guess - (guess - d / (guess * guess)) * (1.0 / 3.0)
    return jnp.where(d > 1e-30, better, guess)


def step_kernel(counts, orb_hbm, ext_hbm, out_ref, pot_ref, *scratch):
    terms = scratch[:8]
    orb_ref, ext_ref, pot_wide, density, in_sem, x_send, x_recv, y_send, y_recv, d_send, d_recv = scratch[8:]
    n_x, n_y, n_b = counts
    nf, ny, nx, nz = orb_ref.shape
    gx = lax.axis_index("gx")
    gy = lax.axis_index("gy")
    gb = lax.axis_index("band")
    has = {
        ("gx", 0): gx > 0,
        ("gx", 1): gx < n_x - 1,
        ("gy", 0): gy > 0,
        ("gy", 1): gy < n_y - 1,
    }
    place = {"gx": gx, "gy": gy}
    if n_x == 2:
        x_sides = [("gx", 1 - gx)]
    else:
        x_sides = [("gx", 0), ("gx", 1)]
    y_sides = [("gy", 0), ("gy", 1)]
    sides = [("gx", 0), ("gx", 1)] + y_sides
    peers = [lax.rem(gb + j, n_b) for j in range(1, n_b)]

    def target(side):
        axis, up = side
        return {axis: place[axis] + (2 * up - 1)}

    barrier = pltpu.get_barrier_semaphore()
    partners = n_b - 1
    for side in sides:
        partners = partners + has[side].astype(jnp.int32)

        @pl.when(has[side])
        def _():
            pl.semaphore_signal(barrier, inc=1, device_id=target(side), device_id_type=MESH)

    for peer in peers:
        pl.semaphore_signal(barrier, inc=1, device_id={"band": peer}, device_id_type=MESH)
    orb_in = pltpu.make_async_copy(orb_hbm, orb_ref, in_sem.at[0])
    orb_in.start()
    ext_in = pltpu.make_async_copy(ext_hbm, ext_ref, in_sem.at[1])
    ext_in.start()

    chunks = max(1, min(6, ny // 2))
    x_cuts = [(j * (ny // chunks), ny // chunks + (ny % chunks if j == chunks - 1 else 0)) for j in range(chunks)]
    mid = (nx - 4) // 2
    y_cuts = [(0, 2), (nx - 2, 2), (2, mid), (2 + mid, nx - 4 - mid)]
    d_cuts = [(0, 2), (ny - 2, 2), (2, ny - 4)]
    order = sorted(range(chunks), key=lambda j: 0 if j in (0, chunks - 1) else 1)
    sems = {"gx": (x_send, x_recv), "gy": (y_send, y_recv)}

    def cells(axis, edge, piece):
        if axis == "gx":
            return pl.ds(edge, 2), pl.ds(2 + x_cuts[piece][0], x_cuts[piece][1])
        return pl.ds(2 + y_cuts[piece][0], y_cuts[piece][1]), pl.ds(edge, 2)

    def pick(up, high, low):
        if isinstance(up, int):
            return high if up else low
        return low + up * (high - low)

    def send_copy(step, side, piece):
        axis, up = side
        extent = nx if axis == "gx" else ny
        return pltpu.make_async_remote_copy(
            src_ref=terms[step].at[cells(axis, pick(up, extent, 2), piece)],
            dst_ref=terms[step].at[cells(axis, pick(up, 0, extent + 2), piece)],
            send_sem=sems[axis][0].at[step, up, piece],
            recv_sem=sems[axis][1].at[step, 1 - up, piece],
            device_id=target(side),
            device_id_type=MESH,
        )

    def recv_copy(step, side, piece):
        axis, up = side
        extent = nx if axis == "gx" else ny
        land = terms[step].at[cells(axis, pick(up, extent + 2, 0), piece)]
        return pltpu.make_async_remote_copy(
            src_ref=land,
            dst_ref=land,
            send_sem=sems[axis][0].at[step, up, piece],
            recv_sem=sems[axis][1].at[step, up, piece],
            device_id=target(side),
            device_id_type=MESH,
        )

    def each(side, act):
        if side[0] == "gx" and n_x == 2:
            act()
        else:
            pl.when(has[side])(act)

    def start(step, side, pieces):
        def act():
            for piece in pieces:
                send_copy(step, side, piece).start()

        each(side, act)

    def await_pieces(step, side, pieces):
        def act():
            for piece in pieces:
                recv_copy(step, side, piece).wait_recv()

        each(side, act)

    def density_copy(which, j, piece):
        rows = pl.ds(*d_cuts[piece])
        return pltpu.make_async_remote_copy(
            src_ref=density.at[which, 0, rows],
            dst_ref=density.at[which, n_b - 1 - j, rows],
            send_sem=d_send.at[which, j, piece],
            recv_sem=d_recv.at[which, n_b - 2 - j, piece],
            device_id={"band": peers[j]},
            device_id_type=MESH,
        )

    def start_density(which, piece):
        for j in range(n_b - 1):
            density_copy(which, j, piece).start()

    def finish_potential(which):
        for piece in range(3):
            rows = pl.ds(*d_cuts[piece])
            for slot in range(1, n_b):
                pltpu.make_async_remote_copy(
                    src_ref=density.at[which, slot, rows],
                    dst_ref=density.at[which, slot, rows],
                    send_sem=d_send.at[which, slot - 1, piece],
                    recv_sem=d_recv.at[which, slot - 1, piece],
                    device_id={"band": peers[slot - 1]},
                    device_id_type=MESH,
                ).wait_recv()
        total = density[which, 0]
        for slot in range(1, n_b):
            total = total + density[which, slot]
        pot = ext_ref[...] - exchange_coef * cube_root(total)
        if which == 1:
            pot_ref[...] = pot
        wide = pot - 1.5 * centre_weight
        for y in range(ny):
            for x in range(nx):
                pot_wide[x, y] = jnp.broadcast_to(wide[y, x : x + 1], (nf, nz))

    for side in sides:
        axis, up = side

        @pl.when(jnp.logical_not(has[side]))
        def _():
            for step in range(8):
                if axis == "gx":
                    shape = (2, ny, nf, nz)
                    terms[step][pl.ds(nx + 2 if up else 0, 2), pl.ds(2, ny)] = jnp.zeros(shape, jnp.float32)
                else:
                    shape = (nx, 2, nf, nz)
                    terms[step][pl.ds(2, nx), pl.ds(ny + 2 if up else 0, 2)] = jnp.zeros(shape, jnp.float32)

    orb_in.wait()
    for y in range(ny):
        block = orb_ref[:, y]
        terms[0][pl.ds(2, nx), y + 2] = jnp.swapaxes(block, 0, 1)
        density[0, 0, y] = jnp.sum(block * block, axis=0)
    pl.semaphore_wait(barrier, partners)
    for side in x_sides:
        start(0, side, order)
    for side in y_sides:
        start(0, side, range(4))
    for piece in range(3):
        start_density(0, piece)
    ext_in.wait()

    lane = lax.broadcasted_iota(jnp.int32, (nf, nz), 1)
    near = -0.5 * near_weight
    far = -0.5 * far_weight
    below1 = jnp.where(lane >= 1, near, 0.0)
    above1 = jnp.where(lane < nz - 1, near, 0.0)
    below2 = jnp.where(lane >= 2, far, 0.0)
    above2 = jnp.where(lane < nz - 2, far, 0.0)
    half = nf // 2
    field = lax.broadcasted_iota(jnp.int32, (nf, nz), 0)
    turn_sign = jnp.where(field < half, 1.0, -1.0)

    def turned(v):
        return jnp.concatenate([v[half:], v[:half]], axis=0) * turn_sign

    def image(step, x, y):
        t = terms[step]
        c = t[x + 2, y + 2]
        one = (t[x + 1, y + 2] + t[x + 3, y + 2]) + (
            t[x + 2, y + 1] + t[x + 2, y + 3]
        )
        two = (t[x, y + 2] + t[x + 4, y + 2]) + (
            t[x + 2, y] + t[x + 2, y + 4]
        )
        total = pot_wide[x, y] * c + near * one + far * two
        total = total + pltpu.roll(c, 1, 1) * below1 + pltpu.roll(c, nz - 1, 1) * above1
        return total + (pltpu.roll(c, 2, 1) * below2 + pltpu.roll(c, nz - 2, 1) * above2)

    def combine(parts, s):
        even = parts[0] + (-(s**2) / 2) * parts[2] + (s**4 / 24) * parts[4]
        odd = s * parts[1] + (-(s**3) / 6) * parts[3]
        return even + turned(odd)

    def advance(step, xs, ys):
        at = [(x, y) for x in xs for y in ys]
        new = [image(step, x, y) for x, y in at]
        if step % 4 < 3:
            for (x, y), value in zip(at, new):
                terms[step + 1][x + 2, y + 2] = value
            return
        parts = [[terms[step - 3 + k][x + 2, y + 2] for k in range(4)] + [value] for (x, y), value in zip(at, new)]
        halves = [combine(part, step_length / 2) for part in parts]
        if step == 7:
            for (x, y), value in zip(at, halves):
                out_ref[x, y] = value
            return
        predicted = [combine(part, step_length) for part in parts]
        squares = [jnp.sum(value * value, axis=0, keepdims=True) for value in predicted]
        for (x, y), value, square in zip(at, halves, squares):
            terms[4][x + 2, y + 2] = value
            density[1, 0, y, pl.ds(x, 1)] = square

    rim = [0, 1, nx - 2, nx - 1]
    for step in range(8):
        if step % 4 == 0:
            finish_potential(step // 4)
        for n, j in enumerate(order):
            edges = [("gy", up) for up, at in ((0, 0), (1, chunks - 1)) if at == j]
            for side in x_sides:
                await_pieces(step, side, [j])
            for side in edges:
                await_pieces(step, side, [0, 1])
            advance(step, rim, range(x_cuts[j][0], sum(x_cuts[j])))
            if step < 7:
                for side in x_sides:
                    start(step + 1, side, [j])
                for side in edges:
                    start(step + 1, side, [0, 1])
            if n == min(1, chunks - 1):
                for piece in (2, 3):
                    for side in y_sides:
                        await_pieces(step, side, [piece])
                    advance(step, range(y_cuts[piece][0], sum(y_cuts[piece])), [0, 1, ny - 2, ny - 1])
                    if step < 7:
                        for side in y_sides:
                            start(step + 1, side, [piece])
                if step == 3:
                    start_density(1, 0)
                    start_density(1, 1)
        for x in range(2, nx - 2):
            advance(step, [x], range(2, ny - 2))
        if step == 3:
            start_density(1, 2)

    for side in x_sides + y_sides:

        def drain():
            for step in range(8):
                for piece in range(chunks if side[0] == "gx" else 4):
                    send_copy(step, side, piece).wait_send()

        each(side, drain)

    for which in (0, 1):
        for j in range(n_b - 1):
            for piece in range(3):
                density_copy(which, j, piece).wait_send()


def step_body(counts, orbitals, external):
    parts, bands, nx, ny, nz = orbitals.shape
    nf = parts * bands
    fields = jnp.transpose(orbitals.reshape(nf, nx, ny, nz), (0, 2, 1, 3))
    n_b = counts[2]
    dma = pltpu.SemaphoreType.DMA
    result, potential = pl.pallas_call(
        functools.partial(step_kernel, counts),
        out_shape=(
            jax.ShapeDtypeStruct((nx, ny, nf, nz), jnp.float32),
            jax.ShapeDtypeStruct((ny, nx, nz), jnp.float32),
        ),
        in_specs=[pl.BlockSpec(memory_space=pltpu.HBM)] * 2,
        out_specs=(pl.BlockSpec(memory_space=pltpu.VMEM),) * 2,
        scratch_shapes=[
            *[pltpu.VMEM((nx + 4, ny + 4, nf, nz), jnp.float32)] * 8,
            pltpu.VMEM((nf, ny, nx, nz), jnp.float32),
            pltpu.VMEM((ny, nx, nz), jnp.float32),
            pltpu.VMEM((nx, ny, nf, nz), jnp.float32),
            pltpu.VMEM((2, n_b, ny, nx, nz), jnp.float32),
            dma((2,)),
            dma((8, 2, 6)),
            dma((8, 2, 6)),
            dma((8, 2, 4)),
            dma((8, 2, 4)),
            dma((2, n_b - 1, 3)),
            dma((2, n_b - 1, 3)),
        ],
        compiler_params=pltpu.CompilerParams(
            collective_id=0, has_side_effects=True, vmem_limit_bytes=40 * 1024 * 1024
        ),
    )(fields, jnp.swapaxes(external, 0, 1))
    result = jnp.transpose(result, (2, 0, 1, 3)).reshape(orbitals.shape)
    return (result, jnp.swapaxes(potential, 0, 1))


DEEP = 8
VDEEP = 6


def whole_kernel(counts, orb_hbm, ext_hbm, out_ref, pot_ref, *scratch):
    (
        psi, half, t1, t2, t3, orb_v, ext_all, v_now, v_next, dens, chip_in, chip_sum, plane_in, partial, swap_in,
        pieces_in, done, result, in_sem, x_send, x_recv, z_send, z_recv, f_send, f_recv, h_send, h_recv,
        a_send, a_recv, b_send, b_recv, c_send, c_recv, e_send, e_recv, r_send, r_recv, l_sem,
    ) = scratch
    n_x, n_y, n_b = counts
    parts, nb, ny, nx, nz = orb_hbm.shape
    own = nb // 2
    mid = ny // 2
    gx = lax.axis_index("gx")
    gy = lax.axis_index("gy")
    gb = lax.axis_index("band")
    ox = 1 - gx
    core = lax.rem(gb, 2)
    mate = gb + 1 - 2 * core
    far_gb = lax.rem(gb + 2, n_b)
    has = (gy > 0, gy < n_y - 1)
    edge = 8
    here = pl.ds(pl.multiple_of(nx * gx, nx), nx)
    there = pl.ds(pl.multiple_of(nx * ox, nx), nx)
    here_pad = pl.ds(pl.multiple_of(edge + nx * gx, 8), nx)
    there_pad = pl.ds(pl.multiple_of(edge + nx * ox, 8), nx)

    def z_peer(d):
        return gy + (2 * d - 1)

    in_plane = [{"band": mate}, {"band": far_gb}, {"gx": ox}, {"gx": ox, "band": mate}, {"gx": ox, "band": far_gb}]
    barrier = pltpu.get_barrier_semaphore()
    partners = len(in_plane)
    for peer in in_plane:
        pl.semaphore_signal(barrier, inc=1, device_id=peer, device_id_type=MESH)
    for d in (0, 1):
        partners = partners + 4 * has[d].astype(jnp.int32)

        @pl.when(has[d])
        def _():
            for x in (gx, ox):
                for b in (gb, mate):
                    pl.semaphore_signal(
                        barrier, inc=1, device_id={"gx": x, "gy": z_peer(d), "band": b}, device_id_type=MESH
                    )

    give = pl.ds(pl.multiple_of(own * ox, own), own)
    keep = pl.ds(pl.multiple_of(own * gx, own), own)
    give_in = pltpu.make_async_copy(orb_hbm.at[:, give], orb_v.at[:, give], in_sem.at[0])
    keep_in = pltpu.make_async_copy(orb_hbm.at[:, keep], orb_v.at[:, keep], in_sem.at[1])
    ext_in = pltpu.make_async_copy(ext_hbm, ext_all.at[:, here], in_sem.at[2])
    psi_in = pltpu.make_async_copy(
        orb_hbm.at[:, keep], psi.at[:, :, pl.ds(DEEP, ny), here_pad], in_sem.at[3]
    )
    give_in.start()
    keep_in.start()
    ext_in.start()
    psi_in.start()

    def remote(src, dst, send, recv, peer):
        return pltpu.make_async_remote_copy(
            src_ref=src, dst_ref=dst, send_sem=send, recv_sem=recv, device_id=peer, device_id_type=MESH
        )

    quarter = 4
    pieces = list(range(ny // quarter))
    goes = ([q for q in pieces if quarter * q < DEEP], [q for q in pieces if quarter * q >= ny - DEEP])
    piece_order = sorted(pieces, key=lambda q: 0 if q in goes[0] and q in goes[1] else 1)

    def x_copy(j, q):
        return remote(
            orb_v.at[:, own * ox + j, pl.ds(quarter * q, quarter)],
            psi.at[:, j, pl.ds(DEEP + quarter * q, quarter), here_pad],
            x_send.at[j, q], x_recv.at[j, q], {"gx": ox},
        )

    def x_land(j, q):
        land = psi.at[:, j, pl.ds(DEEP + quarter * q, quarter), there_pad]
        return remote(land, land, x_send.at[j, q], x_recv.at[j, q], {"gx": ox})

    def halo_row(d):
        return 0 if d else DEEP + ny

    def z_copy(j, d):
        return remote(
            orb_v.at[:, own * gx + j, pl.ds(ny - DEEP if d else 0, DEEP)],
            psi.at[:, j, pl.ds(halo_row(d), DEEP), here_pad],
            z_send.at[d, j], z_recv.at[d, j], {"gy": z_peer(d)},
        )

    def z_land(j, d):
        land = psi.at[:, j, pl.ds(halo_row(d), DEEP), here_pad]
        return remote(land, land, z_send.at[d, j], z_recv.at[d, j], {"gy": z_peer(1 - d)})

    def f_row(d, q):
        return DEEP + quarter * q + (-ny if d else ny)

    def f_copy(j, d, q):
        return remote(
            psi.at[:, j, pl.ds(DEEP + quarter * q, quarter), there_pad],
            psi.at[:, j, pl.ds(f_row(d, q), quarter), there_pad],
            f_send.at[d, j, q], f_recv.at[d, j, q], {"gy": z_peer(d)},
        )

    def f_land(j, d, q):
        land = psi.at[:, j, pl.ds(f_row(d, q), quarter), there_pad]
        return remote(land, land, f_send.at[d, j, q], f_recv.at[d, j, q], {"gy": z_peer(1 - d)})

    def h_copy(j, d):
        return remote(
            half.at[:, j, pl.ds(ny if d else DEEP, DEEP), pl.ds(edge, 2 * nx)],
            half.at[:, j, pl.ds(halo_row(d), DEEP), pl.ds(edge, 2 * nx)],
            h_send.at[d, j], h_recv.at[d, j], {"gy": z_peer(d)},
        )

    def h_land(j, d):
        land = half.at[:, j, pl.ds(halo_row(d), DEEP), pl.ds(edge, 2 * nx)]
        return remote(land, land, h_send.at[d, j], h_recv.at[d, j], {"gy": z_peer(1 - d)})

    zero = jnp.zeros((8, nz), jnp.float32)
    rows_all = ny + 2 * DEEP

    def clear(r, _):
        for p in range(parts):
            for j in range(own):
                for ref in (psi, half, t1, t2, t3):
                    ref[p, j, r, pl.ds(0, 8)] = zero
                    ref[p, j, r, pl.ds(edge + 2 * nx, 8)] = zero
        return 0

    lax.fori_loop(0, rows_all, clear, 0)
    for d in (0, 1):

        @pl.when(jnp.logical_not(has[d]))
        def _():
            def clear_row(i, _):
                r = i + halo_row(1 - d)
                for p in range(parts):
                    for j in range(own):
                        for ref in (psi, half, t1, t2, t3):
                            for x in range(0, 2 * nx, 8):
                                ref[p, j, r, pl.ds(edge + x, 8)] = zero
                return 0

            lax.fori_loop(0, DEEP, clear_row, 0)

    give_in.wait()
    keep_in.wait()
    pl.semaphore_wait(barrier, partners)
    for j in range(own):
        for q in piece_order:
            x_copy(j, q).start()
    for d in (0, 1):

        @pl.when(has[d])
        def _():
            for j in range(own):
                z_copy(j, d).start()

    for y in range(ny):
        total = None
        for p in range(parts):
            for j in range(nb):
                v = orb_v[p, j, y]
                total = v * v if total is None else total + v * v
        dens[y] = total
    first = remote(dens, chip_in, a_send.at[0], a_recv.at[0], {"band": mate})
    first.start()
    ext_in.wait()
    first.wait_recv()
    my_rows = pl.ds(mid * core, mid)
    chip_sum[...] = dens[my_rows] + chip_in[my_rows]
    second = remote(chip_sum, plane_in, b_send.at[0], b_recv.at[0], {"band": far_gb})
    second.start()

    def forward(j, q):
        x_land(j, q).wait_recv()
        for d in (0, 1):
            if q in goes[d]:

                @pl.when(has[d])
                def _():
                    f_copy(j, d, q).start()

    todo = [(j, q) for j in range(own) for q in piece_order]
    forward(*todo[0])
    second.wait_recv()
    shift = -1.5 * centre_weight
    v_rows = pl.ds(VDEEP + mid * core, mid)
    v_now[v_rows, here] = ext_all[my_rows, here] - exchange_coef * cube_root(chip_sum[...] + plane_in[...]) + shift

    own_slot = v_now.at[v_rows, here]
    to_mate = remote(own_slot, own_slot, c_send.at[0, 0], c_recv.at[0, 0], {"band": mate})
    to_x = [
        remote(own_slot, own_slot, c_send.at[0, 1 + n], c_recv.at[0, 1 + core], {"gx": ox, "band": b})
        for n, b in enumerate((gb, mate))
    ]
    z_src = v_now.at[pl.ds(VDEEP + core * (ny - VDEEP), VDEEP), here]
    z_dst = v_now.at[pl.ds((1 - core) * (ny + VDEEP), VDEEP), here]
    z_to = gy + 2 * core - 1
    z_ok = jnp.logical_and(z_to >= 0, z_to < n_y)
    to_z = [
        remote(
            z_src, z_dst, c_send.at[0, 3 + 2 * m + n], c_recv.at[0, 5 - 2 * core + m],
            {"gx": x, "gy": z_to, "band": b},
        )
        for m, x in enumerate((gx, ox))
        for n, b in enumerate((gb, mate))
    ]
    for copy in to_x:
        copy.start()

    @pl.when(z_ok)
    def _():
        for copy in to_z[2:] + to_z[:2]:
            copy.start()

    to_mate.start()
    ext_here, ext_there = ext_all.at[:, here], ext_all.at[:, there]
    ext_over = remote(ext_here, ext_here, e_send.at[0], e_recv.at[0], {"gx": ox})
    ext_over.start()
    for pair in todo[1:]:
        forward(*pair)

    def v_wait(ref, which, slot, rows, cols):
        land = ref.at[rows, cols]
        remote(land, land, c_send.at[which, slot], c_recv.at[which, slot], {"band": mate}).wait_recv()

    v_wait(v_now, 0, 0, pl.ds(VDEEP + mid * (1 - core), mid), here)
    for c in (0, 1):
        v_wait(v_now, 0, 1 + c, pl.ds(VDEEP + mid * c, mid), there)
    for side in (0, 1):

        @pl.when(has[side])
        def _():
            rows = pl.ds(side * (ny + VDEEP), VDEEP)
            v_wait(v_now, 0, 3 + 2 * side, rows, here)
            v_wait(v_now, 0, 4 + 2 * side, rows, there)

    psi_in.wait()

    lane = lax.broadcasted_iota(jnp.int32, (8, nz), 1)
    near = -0.5 * near_weight
    far = -0.5 * far_weight
    below1 = jnp.where(lane >= 1, near, 0.0)
    above1 = jnp.where(lane < nz - 1, near, 0.0)
    below2 = jnp.where(lane >= 2, far, 0.0)
    above2 = jnp.where(lane < nz - 2, far, 0.0)

    def image(src, v, p, j, r, x):
        def at(row, col):
            return src[p, j, row, pl.ds(edge + col, 8)]

        c = at(r, x)
        one = (at(r, x - 1) + at(r, x + 1)) + (at(r - 1, x) + at(r + 1, x))
        two = (at(r, x - 2) + at(r, x + 2)) + (at(r - 2, x) + at(r + 2, x))
        total = v * c + near * one + far * two
        total = total + pltpu.roll(c, 1, 1) * below1 + pltpu.roll(c, nz - 1, 1) * above1
        return total + (pltpu.roll(c, 2, 1) * below2 + pltpu.roll(c, nz - 2, 1) * above2)

    cols = range(0, 2 * nx, 8)

    def level(src, dst, pot, j, first_row, count):
        for i in range(count):
            r = first_row + i
            for x in cols:
                v = pot[r - DEEP + VDEEP, pl.ds(x, 8)]
                for p in range(parts):
                    dst[p, j, r, pl.ds(edge + x, 8)] = image(src, v, p, j, r, x)

    def rows_of(src, dst, pot, j, first_row, count, group):
        def some(i, _):
            level(src, dst, pot, j, first_row + i * group, group)
            return 0

        lax.fori_loop(0, count // group, some, 0)

    def chain(start, pot, j):
        for src, dst, deep in ((start, t1, 6), (t1, t2, 4), (t2, t3, 2)):
            for side in (0, 1):

                @pl.when(has[side])
                def _():
                    rows_of(src, dst, pot, j, DEEP + ny if side else DEEP - deep, deep, 2)

            rows_of(src, dst, pot, j, DEEP, ny, 4)

    def last(start, pot, j, r, x, act):
        v = pot[r - DEEP + VDEEP, pl.ds(x, 8)]
        ts = [[t[p, j, r, pl.ds(edge + x, 8)] for t in (start, t1, t2, t3)] for p in range(parts)]
        for p in range(parts):
            ts[p].append(image(t3, v, p, j, r, x))

        def combine(s):
            even = [ts[p][0] + (-(s**2) / 2) * ts[p][2] + (s**4 / 24) * ts[p][4] for p in range(2)]
            odd = [s * ts[p][1] + (-(s**3) / 6) * ts[p][3] for p in range(2)]
            return even[0] + odd[1], even[1] - odd[0]

        act(combine)

    for j in range(own):
        for side in (0, 1):

            @pl.when(has[side])
            def _():
                d = 1 - side
                z_land(j, d).wait_recv()
                for q in goes[d]:
                    f_land(j, d, q).wait_recv()

        chain(psi, v_now, j)

        def finish_row(i, _):
            for k in range(2):
                y = 2 * i + k
                r = DEEP + y
                for x in cols:

                    def act(combine):
                        for p, value in enumerate(combine(step_length / 2)):
                            half[p, j, r, pl.ds(edge + x, 8)] = value
                        a, b = combine(step_length)
                        square = a * a + b * b
                        if j:
                            square = square + partial[y, pl.ds(x, 8)]
                        partial[y, pl.ds(x, 8)] = square

                    last(psi, v_now, j, r, x, act)
            return 0

        lax.fori_loop(0, ny // 2, finish_row, 0)
        if j == own - 1:
            mine = pl.ds(pl.multiple_of(nx * core, nx), nx)
            theirs = pl.ds(pl.multiple_of(nx * (1 - core), nx), nx)
            third = remote(partial.at[:, theirs], swap_in, a_send.at[1], a_recv.at[1], {"band": mate})
            third.start()
        for d in (0, 1):

            @pl.when(has[d])
            def _():
                h_copy(j, d).start()

    third.wait_recv()
    done[...] = partial[:, mine] + swap_in[...]
    spread = [
        remote(done, pieces_in.at[n], b_send.at[1 + n], b_recv.at[1 + n], peer)
        for n, peer in enumerate(({"gx": ox}, {"band": far_gb}, {"gx": ox, "band": far_gb}))
    ]
    for copy in (spread[2], spread[0], spread[1]):
        copy.start()
    remote(ext_there, ext_there, e_send.at[0], e_recv.at[0], {"gx": ox}).wait_recv()
    for copy in spread:
        copy.wait_recv()
    total = (done[...] + pieces_in[0]) + (pieces_in[1] + pieces_in[2])
    v_next[pl.ds(VDEEP, ny), mine] = ext_all[:, mine] - exchange_coef * cube_root(total) + shift
    next_z = []
    for d in (0, 1):
        z_src = v_next.at[pl.ds(ny if d else VDEEP, VDEEP), mine]
        z_dst = v_next.at[pl.ds(0 if d else ny + VDEEP, VDEEP), mine]
        copies = [
            remote(z_src, z_dst, c_send.at[1, 1 + 2 * d + n], c_recv.at[1, 1 + 2 * d + core], {"gy": z_peer(d), "band": b})
            for n, b in enumerate((gb, mate))
        ]
        next_z.append(copies)

        @pl.when(has[d])
        def _():
            for copy in copies:
                copy.start()

    whole = v_next.at[pl.ds(VDEEP, ny), mine]
    next_mate = remote(whole, whole, c_send.at[1, 0], c_recv.at[1, 0], {"band": mate})
    next_mate.start()
    v_wait(v_next, 1, 0, pl.ds(VDEEP, ny), theirs)
    pot_ref[...] = v_next[pl.ds(VDEEP, ny), here] - shift
    for side in (0, 1):

        @pl.when(has[side])
        def _():
            d = 1 - side
            rows = pl.ds(side * (ny + VDEEP), VDEEP)
            for c in (0, 1):
                v_wait(v_next, 1, 1 + 2 * d + c, rows, pl.ds(nx * c, nx))

    def back_copy(j, q):
        rows = pl.ds(quarter * q, quarter)
        return remote(
            result.at[:, j, rows, there],
            out_ref.at[:, own * gx + j, rows],
            r_send.at[j, q], r_recv.at[j, q], {"gx": ox},
        )

    def back_land(j, q):
        land = out_ref.at[:, own * ox + j, pl.ds(quarter * q, quarter)]
        return remote(land, land, r_send.at[j, q], r_recv.at[j, q], {"gx": ox})

    def stay_copy(j, q):
        rows = pl.ds(quarter * q, quarter)
        return pltpu.make_async_copy(result.at[:, j, rows, here], out_ref.at[:, own * gx + j, rows], l_sem.at[j, q])

    for j in range(own):
        for side in (0, 1):

            @pl.when(has[side])
            def _():
                h_land(j, 1 - side).wait_recv()

        chain(half, v_next, j)
        for q in pieces:
            for k in range(quarter):
                y = quarter * q + k
                for x in cols:

                    def act(combine):
                        for p, value in enumerate(combine(step_length / 2)):
                            result[p, j, y, pl.ds(x, 8)] = value

                    last(half, v_next, j, DEEP + y, x, act)
            back_copy(j, q).start()
            stay_copy(j, q).start()

    first.wait_send()
    second.wait_send()
    third.wait_send()
    to_mate.wait_send()
    ext_over.wait_send()
    next_mate.wait_send()
    for copy in to_x + spread:
        copy.wait_send()

    @pl.when(z_ok)
    def _():
        for copy in to_z:
            copy.wait_send()

    for d in (0, 1):

        @pl.when(has[d])
        def _():
            for copy in next_z[d]:
                copy.wait_send()
            for j in range(own):
                z_copy(j, d).wait_send()
                h_copy(j, d).wait_send()
                for q in goes[d]:
                    f_copy(j, d, q).wait_send()

    for j in range(own):
        for q in pieces:
            x_copy(j, q).wait_send()
            back_copy(j, q).wait_send()
            stay_copy(j, q).wait()
            back_land(j, q).wait_recv()


def whole_body(counts, orbitals, external):
    parts, nb, nx, ny, nz = orbitals.shape
    own = nb // 2
    nq = ny // 4
    dma = pltpu.SemaphoreType.DMA
    term = pltpu.VMEM((parts, own, ny + 2 * DEEP, 2 * nx + 16, nz), jnp.float32)
    block = pltpu.VMEM((ny, nx, nz), jnp.float32)
    half_block = pltpu.VMEM((ny // 2, nx, nz), jnp.float32)
    wide = pltpu.VMEM((ny + 2 * VDEEP, 2 * nx, nz), jnp.float32)
    result, potential = pl.pallas_call(
        functools.partial(whole_kernel, counts),
        out_shape=(
            jax.ShapeDtypeStruct((parts, nb, ny, nx, nz), jnp.float32),
            jax.ShapeDtypeStruct((ny, nx, nz), jnp.float32),
        ),
        in_specs=[pl.BlockSpec(memory_space=pltpu.HBM)] * 2,
        out_specs=(pl.BlockSpec(memory_space=pltpu.VMEM),) * 2,
        scratch_shapes=[
            term, term, term, term, term,
            pltpu.VMEM((parts, nb, ny, nx, nz), jnp.float32),
            pltpu.VMEM((ny, 2 * nx, nz), jnp.float32),
            wide, wide,
            block, block, half_block, half_block,
            pltpu.VMEM((ny, 2 * nx, nz), jnp.float32),
            block,
            pltpu.VMEM((3, ny, nx, nz), jnp.float32),
            block,
            pltpu.VMEM((parts, own, ny, 2 * nx, nz), jnp.float32),
            dma((4,)),
            dma((own, nq)), dma((own, nq)),
            dma((2, own)), dma((2, own)),
            dma((2, own, nq)), dma((2, own, nq)),
            dma((2, own)), dma((2, own)),
            dma((2,)), dma((2,)),
            dma((4,)), dma((4,)),
            dma((2, 7)), dma((2, 7)),
            dma((1,)), dma((1,)),
            dma((own, nq)), dma((own, nq)),
            dma((own, nq)),
        ],
        compiler_params=pltpu.CompilerParams(
            collective_id=0, has_side_effects=True, vmem_limit_bytes=60 * 1024 * 1024
        ),
    )(jnp.transpose(orbitals, (0, 1, 3, 2, 4)), jnp.swapaxes(external, 0, 1))
    return jnp.transpose(result, (0, 1, 3, 2, 4)), jnp.swapaxes(potential, 0, 1)


def body(counts, orbitals, external):
    parts, nb, nx, ny, nz = orbitals.shape
    n_x, n_y, n_b = counts
    if n_x == 2 and n_b == 4 and nb % 2 == 0 and nx % 8 == 0 and ny % 4 == 0 and ny >= 2 * VDEEP:
        return whole_body(counts, orbitals, external)
    return step_body(counts, orbitals, external)


def solution(mesh):
    counts = (mesh.shape["gx"], mesh.shape["gy"], mesh.shape["band"])
    in_specs = (P(None, "band", "gx", "gy", None), P("gx", "gy", None))
    out_specs = (P(None, "band", "gx", "gy", None), P("gx", "gy", None))
    return jax.shard_map(
        functools.partial(body, counts), mesh=mesh, in_specs=in_specs, out_specs=out_specs, check_vma=False
    )
```

```python
import functools

import jax
import jax.numpy as jnp
from jax import lax
from jax.experimental import pallas as pl
from jax.experimental.pallas import tpu as pltpu
from jax.sharding import PartitionSpec as P

step_length = 0.15
exchange_coef = 0.7386
centre_weight = -2.5
near_weight = 4.0 / 3.0
far_weight = -1.0 / 12.0
MESH = pl.DeviceIdType.MESH


def cube_root(d):
    guess = jnp.exp(jnp.log(d) * (1.0 / 3.0))
    better = guess - (guess - d / (guess * guess)) * (1.0 / 3.0)
    return jnp.where(d > 1e-30, better, guess)


def step_kernel(counts, orb_hbm, ext_hbm, out_ref, pot_ref, *scratch):
    terms = scratch[:8]
    orb_ref, ext_ref, pot_wide, density, in_sem, x_send, x_recv, y_send, y_recv, d_send, d_recv = scratch[8:]
    n_x, n_y, n_b = counts
    nf, ny, nx, nz = orb_ref.shape
    gx = lax.axis_index("gx")
    gy = lax.axis_index("gy")
    gb = lax.axis_index("band")
    has = {
        ("gx", 0): gx > 0,
        ("gx", 1): gx < n_x - 1,
        ("gy", 0): gy > 0,
        ("gy", 1): gy < n_y - 1,
    }
    place = {"gx": gx, "gy": gy}
    if n_x == 2:
        x_sides = [("gx", 1 - gx)]
    else:
        x_sides = [("gx", 0), ("gx", 1)]
    y_sides = [("gy", 0), ("gy", 1)]
    sides = [("gx", 0), ("gx", 1)] + y_sides
    peers = [lax.rem(gb + j, n_b) for j in range(1, n_b)]

    def target(side):
        axis, up = side
        return {axis: place[axis] + (2 * up - 1)}

    barrier = pltpu.get_barrier_semaphore()
    partners = n_b - 1
    for side in sides:
        partners = partners + has[side].astype(jnp.int32)

        @pl.when(has[side])
        def _():
            pl.semaphore_signal(barrier, inc=1, device_id=target(side), device_id_type=MESH)

    for peer in peers:
        pl.semaphore_signal(barrier, inc=1, device_id={"band": peer}, device_id_type=MESH)
    orb_in = pltpu.make_async_copy(orb_hbm, orb_ref, in_sem.at[0])
    orb_in.start()
    ext_in = pltpu.make_async_copy(ext_hbm, ext_ref, in_sem.at[1])
    ext_in.start()

    chunks = max(1, min(6, ny // 2))
    x_cuts = [(j * (ny // chunks), ny // chunks + (ny % chunks if j == chunks - 1 else 0)) for j in range(chunks)]
    mid = (nx - 4) // 2
    y_cuts = [(0, 2), (nx - 2, 2), (2, mid), (2 + mid, nx - 4 - mid)]
    d_cuts = [(0, 2), (ny - 2, 2), (2, ny - 4)]
    order = sorted(range(chunks), key=lambda j: 0 if j in (0, chunks - 1) else 1)
    sems = {"gx": (x_send, x_recv), "gy": (y_send, y_recv)}

    def cells(axis, edge, piece):
        if axis == "gx":
            return pl.ds(edge, 2), pl.ds(2 + x_cuts[piece][0], x_cuts[piece][1])
        return pl.ds(2 + y_cuts[piece][0], y_cuts[piece][1]), pl.ds(edge, 2)

    def pick(up, high, low):
        if isinstance(up, int):
            return high if up else low
        return low + up * (high - low)

    def send_copy(step, side, piece):
        axis, up = side
        extent = nx if axis == "gx" else ny
        return pltpu.make_async_remote_copy(
            src_ref=terms[step].at[cells(axis, pick(up, extent, 2), piece)],
            dst_ref=terms[step].at[cells(axis, pick(up, 0, extent + 2), piece)],
            send_sem=sems[axis][0].at[step, up, piece],
            recv_sem=sems[axis][1].at[step, 1 - up, piece],
            device_id=target(side),
            device_id_type=MESH,
        )

    def recv_copy(step, side, piece):
        axis, up = side
        extent = nx if axis == "gx" else ny
        land = terms[step].at[cells(axis, pick(up, extent + 2, 0), piece)]
        return pltpu.make_async_remote_copy(
            src_ref=land,
            dst_ref=land,
            send_sem=sems[axis][0].at[step, up, piece],
            recv_sem=sems[axis][1].at[step, up, piece],
            device_id=target(side),
            device_id_type=MESH,
        )

    def each(side, act):
        if side[0] == "gx" and n_x == 2:
            act()
        else:
            pl.when(has[side])(act)

    def start(step, side, pieces):
        def act():
            for piece in pieces:
                send_copy(step, side, piece).start()

        each(side, act)

    def await_pieces(step, side, pieces):
        def act():
            for piece in pieces:
                recv_copy(step, side, piece).wait_recv()

        each(side, act)

    def density_copy(which, j, piece):
        rows = pl.ds(*d_cuts[piece])
        return pltpu.make_async_remote_copy(
            src_ref=density.at[which, 0, rows],
            dst_ref=density.at[which, n_b - 1 - j, rows],
            send_sem=d_send.at[which, j, piece],
            recv_sem=d_recv.at[which, n_b - 2 - j, piece],
            device_id={"band": peers[j]},
            device_id_type=MESH,
        )

    def start_density(which, piece):
        for j in range(n_b - 1):
            density_copy(which, j, piece).start()

    def finish_potential(which):
        for piece in range(3):
            rows = pl.ds(*d_cuts[piece])
            for slot in range(1, n_b):
                pltpu.make_async_remote_copy(
                    src_ref=density.at[which, slot, rows],
                    dst_ref=density.at[which, slot, rows],
                    send_sem=d_send.at[which, slot - 1, piece],
                    recv_sem=d_recv.at[which, slot - 1, piece],
                    device_id={"band": peers[slot - 1]},
                    device_id_type=MESH,
                ).wait_recv()
        total = density[which, 0]
        for slot in range(1, n_b):
            total = total + density[which, slot]
        pot = ext_ref[...] - exchange_coef * cube_root(total)
        if which == 1:
            pot_ref[...] = pot
        wide = pot - 1.5 * centre_weight
        for y in range(ny):
            for x in range(nx):
                pot_wide[x, y] = jnp.broadcast_to(wide[y, x : x + 1], (nf, nz))

    for side in sides:
        axis, up = side

        @pl.when(jnp.logical_not(has[side]))
        def _():
            for step in range(8):
                if axis == "gx":
                    shape = (2, ny, nf, nz)
                    terms[step][pl.ds(nx + 2 if up else 0, 2), pl.ds(2, ny)] = jnp.zeros(shape, jnp.float32)
                else:
                    shape = (nx, 2, nf, nz)
                    terms[step][pl.ds(2, nx), pl.ds(ny + 2 if up else 0, 2)] = jnp.zeros(shape, jnp.float32)

    orb_in.wait()
    for y in range(ny):
        block = orb_ref[:, y]
        terms[0][pl.ds(2, nx), y + 2] = jnp.swapaxes(block, 0, 1)
        density[0, 0, y] = jnp.sum(block * block, axis=0)
    pl.semaphore_wait(barrier, partners)
    for side in x_sides:
        start(0, side, order)
    for side in y_sides:
        start(0, side, range(4))
    for piece in range(3):
        start_density(0, piece)
    ext_in.wait()

    lane = lax.broadcasted_iota(jnp.int32, (nf, nz), 1)
    near = -0.5 * near_weight
    far = -0.5 * far_weight
    below1 = jnp.where(lane >= 1, near, 0.0)
    above1 = jnp.where(lane < nz - 1, near, 0.0)
    below2 = jnp.where(lane >= 2, far, 0.0)
    above2 = jnp.where(lane < nz - 2, far, 0.0)
    half = nf // 2
    field = lax.broadcasted_iota(jnp.int32, (nf, nz), 0)
    turn_sign = jnp.where(field < half, 1.0, -1.0)

    def turned(v):
        return jnp.concatenate([v[half:], v[:half]], axis=0) * turn_sign

    def image(step, x, y):
        t = terms[step]
        c = t[x + 2, y + 2]
        one = (t[x + 1, y + 2] + t[x + 3, y + 2]) + (
            t[x + 2, y + 1] + t[x + 2, y + 3]
        )
        two = (t[x, y + 2] + t[x + 4, y + 2]) + (
            t[x + 2, y] + t[x + 2, y + 4]
        )
        total = pot_wide[x, y] * c + near * one + far * two
        total = total + pltpu.roll(c, 1, 1) * below1 + pltpu.roll(c, nz - 1, 1) * above1
        return total + (pltpu.roll(c, 2, 1) * below2 + pltpu.roll(c, nz - 2, 1) * above2)

    def combine(parts, s):
        even = parts[0] + (-(s**2) / 2) * parts[2] + (s**4 / 24) * parts[4]
        odd = s * parts[1] + (-(s**3) / 6) * parts[3]
        return even + turned(odd)

    def advance(step, xs, ys):
        at = [(x, y) for x in xs for y in ys]
        new = [image(step, x, y) for x, y in at]
        if step % 4 < 3:
            for (x, y), value in zip(at, new):
                terms[step + 1][x + 2, y + 2] = value
            return
        parts = [[terms[step - 3 + k][x + 2, y + 2] for k in range(4)] + [value] for (x, y), value in zip(at, new)]
        halves = [combine(part, step_length / 2) for part in parts]
        if step == 7:
            for (x, y), value in zip(at, halves):
                out_ref[x, y] = value
            return
        predicted = [combine(part, step_length) for part in parts]
        squares = [jnp.sum(value * value, axis=0, keepdims=True) for value in predicted]
        for (x, y), value, square in zip(at, halves, squares):
            terms[4][x + 2, y + 2] = value
            density[1, 0, y, pl.ds(x, 1)] = square

    rim = [0, 1, nx - 2, nx - 1]
    for step in range(8):
        if step % 4 == 0:
            finish_potential(step // 4)
        for n, j in enumerate(order):
            edges = [("gy", up) for up, at in ((0, 0), (1, chunks - 1)) if at == j]
            for side in x_sides:
                await_pieces(step, side, [j])
            for side in edges:
                await_pieces(step, side, [0, 1])
            advance(step, rim, range(x_cuts[j][0], sum(x_cuts[j])))
            if step < 7:
                for side in x_sides:
                    start(step + 1, side, [j])
                for side in edges:
                    start(step + 1, side, [0, 1])
            if n == min(1, chunks - 1):
                for piece in (2, 3):
                    for side in y_sides:
                        await_pieces(step, side, [piece])
                    advance(step, range(y_cuts[piece][0], sum(y_cuts[piece])), [0, 1, ny - 2, ny - 1])
                    if step < 7:
                        for side in y_sides:
                            start(step + 1, side, [piece])
                if step == 3:
                    start_density(1, 0)
                    start_density(1, 1)
        for x in range(2, nx - 2):
            advance(step, [x], range(2, ny - 2))
        if step == 3:
            start_density(1, 2)

    for side in x_sides + y_sides:

        def drain():
            for step in range(8):
                for piece in range(chunks if side[0] == "gx" else 4):
                    send_copy(step, side, piece).wait_send()

        each(side, drain)

    for which in (0, 1):
        for j in range(n_b - 1):
            for piece in range(3):
                density_copy(which, j, piece).wait_send()


def step_body(counts, orbitals, external):
    parts, bands, nx, ny, nz = orbitals.shape
    nf = parts * bands
    fields = jnp.transpose(orbitals.reshape(nf, nx, ny, nz), (0, 2, 1, 3))
    n_b = counts[2]
    dma = pltpu.SemaphoreType.DMA
    result, potential = pl.pallas_call(
        functools.partial(step_kernel, counts),
        out_shape=(
            jax.ShapeDtypeStruct((nx, ny, nf, nz), jnp.float32),
            jax.ShapeDtypeStruct((ny, nx, nz), jnp.float32),
        ),
        in_specs=[pl.BlockSpec(memory_space=pltpu.HBM)] * 2,
        out_specs=(pl.BlockSpec(memory_space=pltpu.VMEM),) * 2,
        scratch_shapes=[
            *[pltpu.VMEM((nx + 4, ny + 4, nf, nz), jnp.float32)] * 8,
            pltpu.VMEM((nf, ny, nx, nz), jnp.float32),
            pltpu.VMEM((ny, nx, nz), jnp.float32),
            pltpu.VMEM((nx, ny, nf, nz), jnp.float32),
            pltpu.VMEM((2, n_b, ny, nx, nz), jnp.float32),
            dma((2,)),
            dma((8, 2, 6)),
            dma((8, 2, 6)),
            dma((8, 2, 4)),
            dma((8, 2, 4)),
            dma((2, n_b - 1, 3)),
            dma((2, n_b - 1, 3)),
        ],
        compiler_params=pltpu.CompilerParams(
            collective_id=0, has_side_effects=True, vmem_limit_bytes=40 * 1024 * 1024
        ),
    )(fields, jnp.swapaxes(external, 0, 1))
    result = jnp.transpose(result, (2, 0, 1, 3)).reshape(orbitals.shape)
    return (result, jnp.swapaxes(potential, 0, 1))


DEEP = 8
VDEEP = 6
SCALE = 24.0


def whole_kernel(counts, orb_hbm, ext_hbm, out_ref, pot_ref, *scratch):
    (
        psi, half, t1, t2, t3, orb_v, ext_all, v_now, v_next, dens, chip_in, chip_sum, plane_in, partial, swap_in,
        pieces_in, done, result, weights, in_sem, x_send, x_recv, z_send, z_recv, f_send, f_recv, h_send, h_recv,
        a_send, a_recv, b_send, b_recv, c_send, c_recv, e_send, e_recv, r_send, r_recv, l_sem, ready,
    ) = scratch
    n_x, n_y, n_b = counts
    parts, nb, ny, nx, nz = orb_hbm.shape
    own = nb // 2
    mid = ny // 2
    gx = lax.axis_index("gx")
    gy = lax.axis_index("gy")
    gb = lax.axis_index("band")
    ox = 1 - gx
    core = lax.rem(gb, 2)
    mate = gb + 1 - 2 * core
    far_gb = lax.rem(gb + 2, n_b)
    has = (gy > 0, gy < n_y - 1)
    edge = 8
    here = pl.ds(pl.multiple_of(nx * gx, nx), nx)
    there = pl.ds(pl.multiple_of(nx * ox, nx), nx)
    here_pad = pl.ds(pl.multiple_of(edge + nx * gx, 8), nx)
    there_pad = pl.ds(pl.multiple_of(edge + nx * ox, 8), nx)

    def z_peer(d):
        return gy + (2 * d - 1)

    in_plane = [{"band": mate}, {"band": far_gb}, {"gx": ox}]
    barrier = pltpu.get_barrier_semaphore()
    partners = len(in_plane)
    for peer in in_plane:
        pl.semaphore_signal(barrier, inc=1, device_id=peer, device_id_type=MESH)
    for d in (0, 1):
        partners = partners + has[d].astype(jnp.int32)

        @pl.when(has[d])
        def _():
            pl.semaphore_signal(barrier, inc=1, device_id={"gy": z_peer(d)}, device_id_type=MESH)

    give = pl.ds(pl.multiple_of(own * ox, own), own)
    keep = pl.ds(pl.multiple_of(own * gx, own), own)
    give_in = pltpu.make_async_copy(orb_hbm.at[:, give], orb_v.at[:, give], in_sem.at[0])
    keep_in = pltpu.make_async_copy(orb_hbm.at[:, keep], orb_v.at[:, keep], in_sem.at[1])
    ext_in = pltpu.make_async_copy(ext_hbm, ext_all.at[:, here], in_sem.at[2])
    psi_in = pltpu.make_async_copy(
        orb_hbm.at[:, keep], psi.at[:, :, pl.ds(DEEP, ny), here_pad], in_sem.at[3]
    )
    give_in.start()
    keep_in.start()
    ext_in.start()
    psi_in.start()

    def remote(src, dst, send, recv, peer):
        return pltpu.make_async_remote_copy(
            src_ref=src, dst_ref=dst, send_sem=send, recv_sem=recv, device_id=peer, device_id_type=MESH
        )

    quarter = 4
    pieces = list(range(ny // quarter))
    goes = ([q for q in pieces if quarter * q < DEEP], [q for q in pieces if quarter * q >= ny - DEEP])
    piece_order = sorted(pieces, key=lambda q: 0 if q in goes[0] and q in goes[1] else 1)

    def x_copy(j, q):
        return remote(
            orb_v.at[:, own * ox + j, pl.ds(quarter * q, quarter)],
            psi.at[:, j, pl.ds(DEEP + quarter * q, quarter), here_pad],
            x_send.at[j, q], x_recv.at[j, q], {"gx": ox},
        )

    def x_land(j, q):
        land = psi.at[:, j, pl.ds(DEEP + quarter * q, quarter), there_pad]
        return remote(land, land, x_send.at[j, q], x_recv.at[j, q], {"gx": ox})

    def halo_row(d):
        return 0 if d else DEEP + ny

    def z_copy(j, d):
        return remote(
            orb_v.at[:, own * gx + j, pl.ds(ny - DEEP if d else 0, DEEP)],
            psi.at[:, j, pl.ds(halo_row(d), DEEP), here_pad],
            z_send.at[d, j], z_recv.at[d, j], {"gy": z_peer(d)},
        )

    def z_land(j, d):
        land = psi.at[:, j, pl.ds(halo_row(d), DEEP), here_pad]
        return remote(land, land, z_send.at[d, j], z_recv.at[d, j], {"gy": z_peer(1 - d)})

    def f_row(d, q):
        return DEEP + quarter * q + (-ny if d else ny)

    def f_copy(j, d, q):
        return remote(
            psi.at[:, j, pl.ds(DEEP + quarter * q, quarter), there_pad],
            psi.at[:, j, pl.ds(f_row(d, q), quarter), there_pad],
            f_send.at[d, j, q], f_recv.at[d, j, q], {"gy": z_peer(d)},
        )

    def f_land(j, d, q):
        land = psi.at[:, j, pl.ds(f_row(d, q), quarter), there_pad]
        return remote(land, land, f_send.at[d, j, q], f_recv.at[d, j, q], {"gy": z_peer(1 - d)})

    def h_copy(j, d):
        return remote(
            half.at[:, j, pl.ds(ny if d else DEEP, DEEP), pl.ds(edge, 2 * nx)],
            half.at[:, j, pl.ds(halo_row(d), DEEP), pl.ds(edge, 2 * nx)],
            h_send.at[d, j], h_recv.at[d, j], {"gy": z_peer(d)},
        )

    def h_land(j, d):
        land = half.at[:, j, pl.ds(halo_row(d), DEEP), pl.ds(edge, 2 * nx)]
        return remote(land, land, h_send.at[d, j], h_recv.at[d, j], {"gy": z_peer(1 - d)})

    apart = lax.broadcasted_iota(jnp.int32, (2, nz, nz), 1) - lax.broadcasted_iota(jnp.int32, (2, nz, nz), 2)
    apart = jnp.abs(apart).reshape(2 * nz, nz)
    weights[...] = jnp.where(apart == 1, -16.0, jnp.where(apart == 2, 1.0, 0.0)).astype(jnp.bfloat16)
    zero = jnp.zeros((8, nz), jnp.float32)
    rows_all = ny + 2 * DEEP

    def clear(r, _):
        for p in range(parts):
            for j in range(own):
                for ref in (psi, half, t1, t2, t3):
                    ref[p, j, r, pl.ds(0, 8)] = zero
                    ref[p, j, r, pl.ds(edge + 2 * nx, 8)] = zero
        return 0

    lax.fori_loop(0, rows_all, clear, 0)
    for d in (0, 1):

        @pl.when(jnp.logical_not(has[d]))
        def _():
            def clear_row(i, _):
                r = i + halo_row(1 - d)
                for p in range(parts):
                    for j in range(own):
                        for ref in (psi, half):
                            for x in range(0, 2 * nx, 8):
                                ref[p, j, r, pl.ds(edge + x, 8)] = zero
                return 0

            lax.fori_loop(0, DEEP, clear_row, 0)
            for i in range(VDEEP):
                for x in range(0, 2 * nx, 8):
                    v_now[i + (0 if d == 0 else ny + VDEEP), pl.ds(x, 8)] = zero
                    v_next[i + (0 if d == 0 else ny + VDEEP), pl.ds(x, 8)] = zero

    give_in.wait()
    keep_in.wait()
    pl.semaphore_wait(barrier, partners)
    for j in range(own):
        for q in piece_order:
            x_copy(j, q).start()
    for d in (0, 1):

        @pl.when(has[d])
        def _():
            for j in range(own):
                z_copy(j, d).start()

    for y in range(ny):
        total = None
        for p in range(parts):
            for j in range(nb):
                v = orb_v[p, j, y]
                total = v * v if total is None else total + v * v
        dens[y] = total
    first = remote(dens, chip_in, a_send.at[0], a_recv.at[0], {"band": mate})
    first.start()
    ext_in.wait()
    first.wait_recv()
    pl.semaphore_signal(ready, inc=1, device_id={"gx": ox}, device_id_type=MESH)
    my_rows = pl.ds(mid * core, mid)
    chip_sum[...] = dens[my_rows] + chip_in[my_rows]
    second = remote(chip_sum, plane_in, b_send.at[0], b_recv.at[0], {"band": far_gb})
    second.start()

    def forward(j, q):
        x_land(j, q).wait_recv()
        for d in (0, 1):
            if q in goes[d]:

                @pl.when(has[d])
                def _():
                    f_copy(j, d, q).start()

    todo = [(j, q) for j in range(own) for q in piece_order]
    forward(*todo[0])
    second.wait_recv()
    pl.semaphore_wait(ready, 1)
    shift = -1.5 * centre_weight
    v_rows = pl.ds(VDEEP + mid * core, mid)
    mine_now = ext_all[my_rows, here] - exchange_coef * cube_root(chip_sum[...] + plane_in[...])
    v_now[v_rows, here] = (mine_now + shift) * SCALE

    own_slot = v_now.at[v_rows, here]
    to_mate = remote(own_slot, own_slot, c_send.at[0, 0], c_recv.at[0, 0], {"band": mate})
    to_x = [
        remote(own_slot, own_slot, c_send.at[0, 1 + n], c_recv.at[0, 1 + core], {"gx": ox, "band": b})
        for n, b in enumerate((gb, mate))
    ]
    z_src = v_now.at[pl.ds(VDEEP + core * (ny - VDEEP), VDEEP), here]
    z_dst = v_now.at[pl.ds((1 - core) * (ny + VDEEP), VDEEP), here]
    z_to = gy + 2 * core - 1
    z_ok = jnp.logical_and(z_to >= 0, z_to < n_y)
    to_z = [
        remote(
            z_src, z_dst, c_send.at[0, 3 + 2 * m + n], c_recv.at[0, 5 - 2 * core + m],
            {"gx": x, "gy": z_to, "band": b},
        )
        for m, x in enumerate((gx, ox))
        for n, b in enumerate((gb, mate))
    ]
    for copy in to_x:
        copy.start()

    @pl.when(z_ok)
    def _():
        for copy in to_z[2:] + to_z[:2]:
            copy.start()

    to_mate.start()
    ext_here, ext_there = ext_all.at[:, here], ext_all.at[:, there]
    ext_over = remote(ext_here, ext_here, e_send.at[0], e_recv.at[0], {"gx": ox})
    ext_over.start()
    for pair in todo[1:]:
        forward(*pair)

    def v_wait(ref, which, slot, rows, cols):
        land = ref.at[rows, cols]
        remote(land, land, c_send.at[which, slot], c_recv.at[which, slot], {"band": mate}).wait_recv()

    v_wait(v_now, 0, 0, pl.ds(VDEEP + mid * (1 - core), mid), here)
    for c in (0, 1):
        v_wait(v_now, 0, 1 + c, pl.ds(VDEEP + mid * c, mid), there)
    for side in (0, 1):

        @pl.when(has[side])
        def _():
            rows = pl.ds(side * (ny + VDEEP), VDEEP)
            v_wait(v_now, 0, 3 + 2 * side, rows, here)
            v_wait(v_now, 0, 4 + 2 * side, rows, there)

    psi_in.wait()

    cols = range(0, 2 * nx, 8)
    inside = [has[d].astype(jnp.float32) for d in (0, 1)]
    group = 4

    def images(src, pot, j, first_row, emit):
        centres, lhs = {}, []
        for r in range(first_row, first_row + group):
            for p in range(parts):
                c = src[p, j, r, pl.ds(edge, 2 * nx)]
                top = c.astype(jnp.bfloat16)
                rest = (c - top.astype(jnp.float32)).astype(jnp.bfloat16)
                centres[r, p] = c, 2 * nx * len(lhs)
                lhs.append(jnp.concatenate([top, rest], axis=1))
        lines = jnp.dot(jnp.concatenate(lhs, axis=0), weights[...], preferred_element_type=jnp.float32)
        for r in range(first_row, first_row + group):
            for x in cols:
                v = pot[r - DEEP + VDEEP, pl.ds(x, 8)]
                values = []
                for p in range(parts):

                    def at(row, col):
                        return src[p, j, row, pl.ds(edge + col, 8)]

                    c, place = centres[r, p]
                    one = (at(r, x - 1) + at(r, x + 1)) + (at(r - 1, x) + at(r + 1, x))
                    two = (at(r, x - 2) + at(r, x + 2)) + (at(r - 2, x) + at(r + 2, x))
                    line = lines[place + x : place + x + 8]
                    value = v * c[x : x + 8] + ((two - 16.0 * one) + line)
                    if r < DEEP:
                        value = value * inside[0]
                    if r >= DEEP + ny:
                        value = value * inside[1]
                    values.append(value)
                emit(r, x, values)

    def exponential(start, pot, j, act, after):
        terms = (start, t1, t2, t3)

        def store(dst):
            def emit(r, x, values):
                for p, value in enumerate(values):
                    dst[p, j, r, pl.ds(edge + x, 8)] = value

            return emit

        def finish(r, x, values):
            ts = [[t[p, j, r, pl.ds(edge + x, 8)] for t in terms] + [values[p]] for p in range(parts)]

            def combine(s):
                u = s / SCALE
                even = [ts[p][0] + (-(u**2) / 2) * ts[p][2] + (u**4 / 24) * ts[p][4] for p in range(2)]
                odd = [u * ts[p][1] + (-(u**3) / 6) * ts[p][3] for p in range(2)]
                return even[0] + odd[1], even[1] - odd[0]

            act(r - DEEP, x, combine)

        emits = [store(t1), store(t2), store(t3), finish]
        for g in range((ny + 12) // group + 3):
            for k, emit in enumerate(emits):
                deep = 6 - 2 * k
                i = g - k
                if 0 <= i < (ny + 2 * deep) // group:
                    images(terms[k], pot, j, DEEP - deep + group * i, emit)
                    if k == 3:
                        after(i)

    for j in range(own):
        for side in (0, 1):

            @pl.when(has[side])
            def _():
                d = 1 - side
                z_land(j, d).wait_recv()
                for q in goes[d]:
                    f_land(j, d, q).wait_recv()

        def keep_both(y, x, combine):
            for p, value in enumerate(combine(step_length / 2)):
                half[p, j, DEEP + y, pl.ds(edge + x, 8)] = value
            re, im = combine(step_length)
            square = re * re + im * im
            if j:
                square = square + partial[y, pl.ds(x, 8)]
            partial[y, pl.ds(x, 8)] = square

        exponential(psi, v_now, j, keep_both, lambda i: None)
        if j == own - 1:
            mine = pl.ds(pl.multiple_of(nx * core, nx), nx)
            theirs = pl.ds(pl.multiple_of(nx * (1 - core), nx), nx)
            third = remote(partial.at[:, theirs], swap_in, a_send.at[1], a_recv.at[1], {"band": mate})
            third.start()
        for d in (0, 1):

            @pl.when(has[d])
            def _():
                h_copy(j, d).start()

    third.wait_recv()
    done[...] = partial[:, mine] + swap_in[...]
    spread = [
        remote(done, pieces_in.at[n], b_send.at[1 + n], b_recv.at[1 + n], peer)
        for n, peer in enumerate(({"gx": ox}, {"band": far_gb}, {"gx": ox, "band": far_gb}))
    ]
    for copy in (spread[2], spread[0], spread[1]):
        copy.start()
    remote(ext_there, ext_there, e_send.at[0], e_recv.at[0], {"gx": ox}).wait_recv()
    for copy in spread:
        copy.wait_recv()
    total = (done[...] + pieces_in[0]) + (pieces_in[1] + pieces_in[2])
    mine_next = ext_all[:, mine] - exchange_coef * cube_root(total)
    v_next[pl.ds(VDEEP, ny), mine] = (mine_next + shift) * SCALE
    next_z = []
    for d in (0, 1):
        z_src = v_next.at[pl.ds(ny if d else VDEEP, VDEEP), mine]
        z_dst = v_next.at[pl.ds(0 if d else ny + VDEEP, VDEEP), mine]
        copies = [
            remote(z_src, z_dst, c_send.at[1, 1 + 2 * d + n], c_recv.at[1, 1 + 2 * d + core], {"gy": z_peer(d), "band": b})
            for n, b in enumerate((gb, mate))
        ]
        next_z.append(copies)

        @pl.when(has[d])
        def _():
            for copy in copies:
                copy.start()

    whole = v_next.at[pl.ds(VDEEP, ny), mine]
    next_mate = remote(whole, whole, c_send.at[1, 0], c_recv.at[1, 0], {"band": mate})
    next_mate.start()
    v_wait(v_next, 1, 0, pl.ds(VDEEP, ny), theirs)
    pot_ref[...] = v_next[pl.ds(VDEEP, ny), here] * (1.0 / SCALE) - shift
    for side in (0, 1):

        @pl.when(has[side])
        def _():
            d = 1 - side
            rows = pl.ds(side * (ny + VDEEP), VDEEP)
            for c in (0, 1):
                v_wait(v_next, 1, 1 + 2 * d + c, rows, pl.ds(nx * c, nx))

    def back_copy(j, q):
        rows = pl.ds(quarter * q, quarter)
        return remote(
            result.at[:, j, rows, there],
            out_ref.at[:, own * gx + j, rows],
            r_send.at[j, q], r_recv.at[j, q], {"gx": ox},
        )

    def back_land(j, q):
        land = out_ref.at[:, own * ox + j, pl.ds(quarter * q, quarter)]
        return remote(land, land, r_send.at[j, q], r_recv.at[j, q], {"gx": ox})

    def stay_copy(j, q):
        rows = pl.ds(quarter * q, quarter)
        return pltpu.make_async_copy(result.at[:, j, rows, here], out_ref.at[:, own * gx + j, rows], l_sem.at[j, q])

    for j in range(own):
        for side in (0, 1):

            @pl.when(has[side])
            def _():
                h_land(j, 1 - side).wait_recv()

        def keep_result(y, x, combine):
            for p, value in enumerate(combine(step_length / 2)):
                result[p, j, y, pl.ds(x, 8)] = value

        def send_back(q):
            back_copy(j, q).start()
            stay_copy(j, q).start()

        exponential(half, v_next, j, keep_result, send_back)

    first.wait_send()
    second.wait_send()
    third.wait_send()
    to_mate.wait_send()
    ext_over.wait_send()
    next_mate.wait_send()
    for copy in to_x + spread:
        copy.wait_send()

    @pl.when(z_ok)
    def _():
        for copy in to_z:
            copy.wait_send()

    for d in (0, 1):

        @pl.when(has[d])
        def _():
            for copy in next_z[d]:
                copy.wait_send()
            for j in range(own):
                z_copy(j, d).wait_send()
                h_copy(j, d).wait_send()
                for q in goes[d]:
                    f_copy(j, d, q).wait_send()

    for j in range(own):
        for q in pieces:
            x_copy(j, q).wait_send()
            back_copy(j, q).wait_send()
            stay_copy(j, q).wait()
            back_land(j, q).wait_recv()


def whole_body(counts, orbitals, external):
    parts, nb, nx, ny, nz = orbitals.shape
    own = nb // 2
    nq = ny // 4
    dma = pltpu.SemaphoreType.DMA
    term = pltpu.VMEM((parts, own, ny + 2 * DEEP, 2 * nx + 16, nz), jnp.float32)
    block = pltpu.VMEM((ny, nx, nz), jnp.float32)
    half_block = pltpu.VMEM((ny // 2, nx, nz), jnp.float32)
    wide = pltpu.VMEM((ny + 2 * VDEEP, 2 * nx, nz), jnp.float32)
    result, potential = pl.pallas_call(
        functools.partial(whole_kernel, counts),
        out_shape=(
            jax.ShapeDtypeStruct((parts, nb, ny, nx, nz), jnp.float32),
            jax.ShapeDtypeStruct((ny, nx, nz), jnp.float32),
        ),
        in_specs=[pl.BlockSpec(memory_space=pltpu.HBM)] * 2,
        out_specs=(pl.BlockSpec(memory_space=pltpu.VMEM),) * 2,
        scratch_shapes=[
            term, term, term, term, term,
            pltpu.VMEM((parts, nb, ny, nx, nz), jnp.float32),
            pltpu.VMEM((ny, 2 * nx, nz), jnp.float32),
            wide, wide,
            block, block, half_block, half_block,
            pltpu.VMEM((ny, 2 * nx, nz), jnp.float32),
            block,
            pltpu.VMEM((3, ny, nx, nz), jnp.float32),
            block,
            pltpu.VMEM((parts, own, ny, 2 * nx, nz), jnp.float32),
            pltpu.VMEM((2 * nz, nz), jnp.bfloat16),
            dma((4,)),
            dma((own, nq)), dma((own, nq)),
            dma((2, own)), dma((2, own)),
            dma((2, own, nq)), dma((2, own, nq)),
            dma((2, own)), dma((2, own)),
            dma((2,)), dma((2,)),
            dma((4,)), dma((4,)),
            dma((2, 7)), dma((2, 7)),
            dma((1,)), dma((1,)),
            dma((own, nq)), dma((own, nq)),
            dma((own, nq)),
            pltpu.SemaphoreType.REGULAR,
        ],
        compiler_params=pltpu.CompilerParams(
            collective_id=0, has_side_effects=True, vmem_limit_bytes=32 * 1024 * 1024
        ),
    )(
        pltpu.with_memory_space_constraint(jnp.transpose(orbitals, (0, 1, 3, 2, 4)), pltpu.HBM),
        pltpu.with_memory_space_constraint(jnp.swapaxes(external, 0, 1), pltpu.HBM),
    )
    return jnp.transpose(result, (0, 1, 3, 2, 4)), jnp.swapaxes(potential, 0, 1)


def body(counts, orbitals, external):
    parts, nb, nx, ny, nz = orbitals.shape
    n_x, n_y, n_b = counts
    if n_x == 2 and n_b == 4 and nb % 2 == 0 and nx % 8 == 0 and ny % 4 == 0 and ny >= 2 * VDEEP:
        return whole_body(counts, orbitals, external)
    return step_body(counts, orbitals, external)


def solution(mesh):
    counts = (mesh.shape["gx"], mesh.shape["gy"], mesh.shape["band"])
    in_specs = (P(None, "band", "gx", "gy", None), P("gx", "gy", None))
    out_specs = (P(None, "band", "gx", "gy", None), P("gx", "gy", None))
    return jax.shard_map(
        functools.partial(body, counts), mesh=mesh, in_specs=in_specs, out_specs=out_specs, check_vma=False
    )
```

```python
import functools

import jax
import jax.numpy as jnp
from jax import lax
from jax.experimental import pallas as pl
from jax.experimental.pallas import tpu as pltpu
from jax.sharding import PartitionSpec as P

step_length = 0.15
exchange_coef = 0.7386
centre_weight = -2.5
near_weight = 4.0 / 3.0
far_weight = -1.0 / 12.0
MESH = pl.DeviceIdType.MESH


def cube_root(d):
    guess = jnp.exp(jnp.log(d) * (1.0 / 3.0))
    better = guess - (guess - d / (guess * guess)) * (1.0 / 3.0)
    return jnp.where(d > 1e-30, better, guess)


def step_kernel(counts, orb_hbm, ext_hbm, out_ref, pot_ref, *scratch):
    terms = scratch[:8]
    orb_ref, ext_ref, pot_wide, density, in_sem, x_send, x_recv, y_send, y_recv, d_send, d_recv = scratch[8:]
    n_x, n_y, n_b = counts
    nf, ny, nx, nz = orb_ref.shape
    gx = lax.axis_index("gx")
    gy = lax.axis_index("gy")
    gb = lax.axis_index("band")
    has = {
        ("gx", 0): gx > 0,
        ("gx", 1): gx < n_x - 1,
        ("gy", 0): gy > 0,
        ("gy", 1): gy < n_y - 1,
    }
    place = {"gx": gx, "gy": gy}
    if n_x == 2:
        x_sides = [("gx", 1 - gx)]
    else:
        x_sides = [("gx", 0), ("gx", 1)]
    y_sides = [("gy", 0), ("gy", 1)]
    sides = [("gx", 0), ("gx", 1)] + y_sides
    peers = [lax.rem(gb + j, n_b) for j in range(1, n_b)]

    def target(side):
        axis, up = side
        return {axis: place[axis] + (2 * up - 1)}

    barrier = pltpu.get_barrier_semaphore()
    partners = n_b - 1
    for side in sides:
        partners = partners + has[side].astype(jnp.int32)

        @pl.when(has[side])
        def _():
            pl.semaphore_signal(barrier, inc=1, device_id=target(side), device_id_type=MESH)

    for peer in peers:
        pl.semaphore_signal(barrier, inc=1, device_id={"band": peer}, device_id_type=MESH)
    orb_in = pltpu.make_async_copy(orb_hbm, orb_ref, in_sem.at[0])
    orb_in.start()
    ext_in = pltpu.make_async_copy(ext_hbm, ext_ref, in_sem.at[1])
    ext_in.start()

    chunks = max(1, min(6, ny // 2))
    x_cuts = [(j * (ny // chunks), ny // chunks + (ny % chunks if j == chunks - 1 else 0)) for j in range(chunks)]
    mid = (nx - 4) // 2
    y_cuts = [(0, 2), (nx - 2, 2), (2, mid), (2 + mid, nx - 4 - mid)]
    d_cuts = [(0, 2), (ny - 2, 2), (2, ny - 4)]
    order = sorted(range(chunks), key=lambda j: 0 if j in (0, chunks - 1) else 1)
    sems = {"gx": (x_send, x_recv), "gy": (y_send, y_recv)}

    def cells(axis, edge, piece):
        if axis == "gx":
            return pl.ds(edge, 2), pl.ds(2 + x_cuts[piece][0], x_cuts[piece][1])
        return pl.ds(2 + y_cuts[piece][0], y_cuts[piece][1]), pl.ds(edge, 2)

    def pick(up, high, low):
        if isinstance(up, int):
            return high if up else low
        return low + up * (high - low)

    def send_copy(step, side, piece):
        axis, up = side
        extent = nx if axis == "gx" else ny
        return pltpu.make_async_remote_copy(
            src_ref=terms[step].at[cells(axis, pick(up, extent, 2), piece)],
            dst_ref=terms[step].at[cells(axis, pick(up, 0, extent + 2), piece)],
            send_sem=sems[axis][0].at[step, up, piece],
            recv_sem=sems[axis][1].at[step, 1 - up, piece],
            device_id=target(side),
            device_id_type=MESH,
        )

    def recv_copy(step, side, piece):
        axis, up = side
        extent = nx if axis == "gx" else ny
        land = terms[step].at[cells(axis, pick(up, extent + 2, 0), piece)]
        return pltpu.make_async_remote_copy(
            src_ref=land,
            dst_ref=land,
            send_sem=sems[axis][0].at[step, up, piece],
            recv_sem=sems[axis][1].at[step, up, piece],
            device_id=target(side),
            device_id_type=MESH,
        )

    def each(side, act):
        if side[0] == "gx" and n_x == 2:
            act()
        else:
            pl.when(has[side])(act)

    def start(step, side, pieces):
        def act():
            for piece in pieces:
                send_copy(step, side, piece).start()

        each(side, act)

    def await_pieces(step, side, pieces):
        def act():
            for piece in pieces:
                recv_copy(step, side, piece).wait_recv()

        each(side, act)

    def density_copy(which, j, piece):
        rows = pl.ds(*d_cuts[piece])
        return pltpu.make_async_remote_copy(
            src_ref=density.at[which, 0, rows],
            dst_ref=density.at[which, n_b - 1 - j, rows],
            send_sem=d_send.at[which, j, piece],
            recv_sem=d_recv.at[which, n_b - 2 - j, piece],
            device_id={"band": peers[j]},
            device_id_type=MESH,
        )

    def start_density(which, piece):
        for j in range(n_b - 1):
            density_copy(which, j, piece).start()

    def finish_potential(which):
        for piece in range(3):
            rows = pl.ds(*d_cuts[piece])
            for slot in range(1, n_b):
                pltpu.make_async_remote_copy(
                    src_ref=density.at[which, slot, rows],
                    dst_ref=density.at[which, slot, rows],
                    send_sem=d_send.at[which, slot - 1, piece],
                    recv_sem=d_recv.at[which, slot - 1, piece],
                    device_id={"band": peers[slot - 1]},
                    device_id_type=MESH,
                ).wait_recv()
        total = density[which, 0]
        for slot in range(1, n_b):
            total = total + density[which, slot]
        pot = ext_ref[...] - exchange_coef * cube_root(total)
        if which == 1:
            pot_ref[...] = pot
        wide = pot - 1.5 * centre_weight
        for y in range(ny):
            for x in range(nx):
                pot_wide[x, y] = jnp.broadcast_to(wide[y, x : x + 1], (nf, nz))

    for side in sides:
        axis, up = side

        @pl.when(jnp.logical_not(has[side]))
        def _():
            for step in range(8):
                if axis == "gx":
                    shape = (2, ny, nf, nz)
                    terms[step][pl.ds(nx + 2 if up else 0, 2), pl.ds(2, ny)] = jnp.zeros(shape, jnp.float32)
                else:
                    shape = (nx, 2, nf, nz)
                    terms[step][pl.ds(2, nx), pl.ds(ny + 2 if up else 0, 2)] = jnp.zeros(shape, jnp.float32)

    orb_in.wait()
    for y in range(ny):
        block = orb_ref[:, y]
        terms[0][pl.ds(2, nx), y + 2] = jnp.swapaxes(block, 0, 1)
        density[0, 0, y] = jnp.sum(block * block, axis=0)
    pl.semaphore_wait(barrier, partners)
    for side in x_sides:
        start(0, side, order)
    for side in y_sides:
        start(0, side, range(4))
    for piece in range(3):
        start_density(0, piece)
    ext_in.wait()

    lane = lax.broadcasted_iota(jnp.int32, (nf, nz), 1)
    near = -0.5 * near_weight
    far = -0.5 * far_weight
    below1 = jnp.where(lane >= 1, near, 0.0)
    above1 = jnp.where(lane < nz - 1, near, 0.0)
    below2 = jnp.where(lane >= 2, far, 0.0)
    above2 = jnp.where(lane < nz - 2, far, 0.0)
    half = nf // 2
    field = lax.broadcasted_iota(jnp.int32, (nf, nz), 0)
    turn_sign = jnp.where(field < half, 1.0, -1.0)

    def turned(v):
        return jnp.concatenate([v[half:], v[:half]], axis=0) * turn_sign

    def image(step, x, y):
        t = terms[step]
        c = t[x + 2, y + 2]
        one = (t[x + 1, y + 2] + t[x + 3, y + 2]) + (
            t[x + 2, y + 1] + t[x + 2, y + 3]
        )
        two = (t[x, y + 2] + t[x + 4, y + 2]) + (
            t[x + 2, y] + t[x + 2, y + 4]
        )
        total = pot_wide[x, y] * c + near * one + far * two
        total = total + pltpu.roll(c, 1, 1) * below1 + pltpu.roll(c, nz - 1, 1) * above1
        return total + (pltpu.roll(c, 2, 1) * below2 + pltpu.roll(c, nz - 2, 1) * above2)

    def combine(parts, s):
        even = parts[0] + (-(s**2) / 2) * parts[2] + (s**4 / 24) * parts[4]
        odd = s * parts[1] + (-(s**3) / 6) * parts[3]
        return even + turned(odd)

    def advance(step, xs, ys):
        at = [(x, y) for x in xs for y in ys]
        new = [image(step, x, y) for x, y in at]
        if step % 4 < 3:
            for (x, y), value in zip(at, new):
                terms[step + 1][x + 2, y + 2] = value
            return
        parts = [[terms[step - 3 + k][x + 2, y + 2] for k in range(4)] + [value] for (x, y), value in zip(at, new)]
        halves = [combine(part, step_length / 2) for part in parts]
        if step == 7:
            for (x, y), value in zip(at, halves):
                out_ref[x, y] = value
            return
        predicted = [combine(part, step_length) for part in parts]
        squares = [jnp.sum(value * value, axis=0, keepdims=True) for value in predicted]
        for (x, y), value, square in zip(at, halves, squares):
            terms[4][x + 2, y + 2] = value
            density[1, 0, y, pl.ds(x, 1)] = square

    rim = [0, 1, nx - 2, nx - 1]
    for step in range(8):
        if step % 4 == 0:
            finish_potential(step // 4)
        for n, j in enumerate(order):
            edges = [("gy", up) for up, at in ((0, 0), (1, chunks - 1)) if at == j]
            for side in x_sides:
                await_pieces(step, side, [j])
            for side in edges:
                await_pieces(step, side, [0, 1])
            advance(step, rim, range(x_cuts[j][0], sum(x_cuts[j])))
            if step < 7:
                for side in x_sides:
                    start(step + 1, side, [j])
                for side in edges:
                    start(step + 1, side, [0, 1])
            if n == min(1, chunks - 1):
                for piece in (2, 3):
                    for side in y_sides:
                        await_pieces(step, side, [piece])
                    advance(step, range(y_cuts[piece][0], sum(y_cuts[piece])), [0, 1, ny - 2, ny - 1])
                    if step < 7:
                        for side in y_sides:
                            start(step + 1, side, [piece])
                if step == 3:
                    start_density(1, 0)
                    start_density(1, 1)
        for x in range(2, nx - 2):
            advance(step, [x], range(2, ny - 2))
        if step == 3:
            start_density(1, 2)

    for side in x_sides + y_sides:

        def drain():
            for step in range(8):
                for piece in range(chunks if side[0] == "gx" else 4):
                    send_copy(step, side, piece).wait_send()

        each(side, drain)

    for which in (0, 1):
        for j in range(n_b - 1):
            for piece in range(3):
                density_copy(which, j, piece).wait_send()


def step_body(counts, orbitals, external):
    parts, bands, nx, ny, nz = orbitals.shape
    nf = parts * bands
    fields = jnp.transpose(orbitals.reshape(nf, nx, ny, nz), (0, 2, 1, 3))
    n_b = counts[2]
    dma = pltpu.SemaphoreType.DMA
    result, potential = pl.pallas_call(
        functools.partial(step_kernel, counts),
        out_shape=(
            jax.ShapeDtypeStruct((nx, ny, nf, nz), jnp.float32),
            jax.ShapeDtypeStruct((ny, nx, nz), jnp.float32),
        ),
        in_specs=[pl.BlockSpec(memory_space=pltpu.HBM)] * 2,
        out_specs=(pl.BlockSpec(memory_space=pltpu.VMEM),) * 2,
        scratch_shapes=[
            *[pltpu.VMEM((nx + 4, ny + 4, nf, nz), jnp.float32)] * 8,
            pltpu.VMEM((nf, ny, nx, nz), jnp.float32),
            pltpu.VMEM((ny, nx, nz), jnp.float32),
            pltpu.VMEM((nx, ny, nf, nz), jnp.float32),
            pltpu.VMEM((2, n_b, ny, nx, nz), jnp.float32),
            dma((2,)),
            dma((8, 2, 6)),
            dma((8, 2, 6)),
            dma((8, 2, 4)),
            dma((8, 2, 4)),
            dma((2, n_b - 1, 3)),
            dma((2, n_b - 1, 3)),
        ],
        compiler_params=pltpu.CompilerParams(
            collective_id=0, has_side_effects=True, vmem_limit_bytes=40 * 1024 * 1024
        ),
    )(fields, jnp.swapaxes(external, 0, 1))
    result = jnp.transpose(result, (2, 0, 1, 3)).reshape(orbitals.shape)
    return (result, jnp.swapaxes(potential, 0, 1))


DEEP = 8
VDEEP = 6
SCALE = 24.0


def whole_kernel(counts, orb_hbm, ext_hbm, out_ref, pot_ref, *scratch):
    (
        psi, half, t1, t2, t3, orb_v, ext_all, v_now, v_next, dens, chip_in, chip_sum, plane_in, partial, swap_in,
        pieces_in, done, result, pot_v, weights, in_sem, x_send, x_recv, z_send, z_recv, f_send, f_recv, h_send, h_recv,
        a_send, a_recv, b_send, b_recv, c_send, c_recv, e_send, e_recv, r_send, r_recv, l_sem,
        s_send, s_recv, p_send, p_recv, v_send, v_recv, m_send, m_recv, ready,
    ) = scratch
    n_x, n_y, n_b = counts
    parts, nb, ny, nx, nz = orb_hbm.shape
    own = nb // 2
    mid = ny // 2
    gx = lax.axis_index("gx")
    gy = lax.axis_index("gy")
    gb = lax.axis_index("band")
    ox = 1 - gx
    core = lax.rem(gb, 2)
    mate = gb + 1 - 2 * core
    far_gb = lax.rem(gb + 2, n_b)
    has = (gy > 0, gy < n_y - 1)
    edge = 8
    here = pl.ds(pl.multiple_of(nx * gx, nx), nx)
    there = pl.ds(pl.multiple_of(nx * ox, nx), nx)
    here_pad = pl.ds(pl.multiple_of(edge + nx * gx, 8), nx)
    there_pad = pl.ds(pl.multiple_of(edge + nx * ox, 8), nx)

    def z_peer(d):
        return gy + (2 * d - 1)

    in_plane = [{"band": mate}, {"band": far_gb}, {"gx": ox}]
    barrier = pltpu.get_barrier_semaphore()
    partners = len(in_plane)
    for peer in in_plane:
        pl.semaphore_signal(barrier, inc=1, device_id=peer, device_id_type=MESH)
    for d in (0, 1):
        partners = partners + has[d].astype(jnp.int32)

        @pl.when(has[d])
        def _():
            pl.semaphore_signal(barrier, inc=1, device_id={"gy": z_peer(d)}, device_id_type=MESH)

    give = pl.ds(pl.multiple_of(own * ox, own), own)
    keep = pl.ds(pl.multiple_of(own * gx, own), own)
    give_in = pltpu.make_async_copy(orb_hbm.at[:, give], orb_v.at[:, give], in_sem.at[0])
    keep_in = pltpu.make_async_copy(orb_hbm.at[:, keep], orb_v.at[:, keep], in_sem.at[1])
    ext_in = pltpu.make_async_copy(ext_hbm, ext_all.at[:, here], in_sem.at[2])
    psi_in = pltpu.make_async_copy(
        orb_hbm.at[:, keep], psi.at[:, :, pl.ds(DEEP, ny), here_pad], in_sem.at[3]
    )
    give_in.start()
    keep_in.start()
    ext_in.start()
    psi_in.start()

    def remote(src, dst, send, recv, peer):
        return pltpu.make_async_remote_copy(
            src_ref=src, dst_ref=dst, send_sem=send, recv_sem=recv, device_id=peer, device_id_type=MESH
        )

    quarter = 4
    pieces = list(range(ny // quarter))
    goes = ([q for q in pieces if quarter * q < DEEP], [q for q in pieces if quarter * q >= ny - DEEP])
    piece_order = sorted(pieces, key=lambda q: 0 if q in goes[0] and q in goes[1] else 1)

    def x_copy(j, q):
        return remote(
            orb_v.at[:, own * ox + j, pl.ds(quarter * q, quarter)],
            psi.at[:, j, pl.ds(DEEP + quarter * q, quarter), here_pad],
            x_send.at[j, q], x_recv.at[j, q], {"gx": ox},
        )

    def x_land(j, q):
        land = psi.at[:, j, pl.ds(DEEP + quarter * q, quarter), there_pad]
        return remote(land, land, x_send.at[j, q], x_recv.at[j, q], {"gx": ox})

    def halo_row(d):
        return 0 if d else DEEP + ny

    def z_copy(j, d):
        return remote(
            orb_v.at[:, own * gx + j, pl.ds(ny - DEEP if d else 0, DEEP)],
            psi.at[:, j, pl.ds(halo_row(d), DEEP), here_pad],
            z_send.at[d, j], z_recv.at[d, j], {"gy": z_peer(d)},
        )

    def z_land(j, d):
        land = psi.at[:, j, pl.ds(halo_row(d), DEEP), here_pad]
        return remote(land, land, z_send.at[d, j], z_recv.at[d, j], {"gy": z_peer(1 - d)})

    def f_row(d, q):
        return DEEP + quarter * q + (-ny if d else ny)

    def f_copy(j, d, q):
        return remote(
            psi.at[:, j, pl.ds(DEEP + quarter * q, quarter), there_pad],
            psi.at[:, j, pl.ds(f_row(d, q), quarter), there_pad],
            f_send.at[d, j, q], f_recv.at[d, j, q], {"gy": z_peer(d)},
        )

    def f_land(j, d, q):
        land = psi.at[:, j, pl.ds(f_row(d, q), quarter), there_pad]
        return remote(land, land, f_send.at[d, j, q], f_recv.at[d, j, q], {"gy": z_peer(1 - d)})

    def h_copy(j, d):
        return remote(
            half.at[:, j, pl.ds(ny if d else DEEP, DEEP), pl.ds(edge, 2 * nx)],
            half.at[:, j, pl.ds(halo_row(d), DEEP), pl.ds(edge, 2 * nx)],
            h_send.at[d, j], h_recv.at[d, j], {"gy": z_peer(d)},
        )

    def h_land(j, d):
        land = half.at[:, j, pl.ds(halo_row(d), DEEP), pl.ds(edge, 2 * nx)]
        return remote(land, land, h_send.at[d, j], h_recv.at[d, j], {"gy": z_peer(1 - d)})

    apart = lax.broadcasted_iota(jnp.int32, (2, nz, nz), 1) - lax.broadcasted_iota(jnp.int32, (2, nz, nz), 2)
    apart = jnp.abs(apart).reshape(2 * nz, nz)
    weights[...] = jnp.where(apart == 1, -16.0, jnp.where(apart == 2, 1.0, 0.0)).astype(jnp.bfloat16)
    zero = jnp.zeros((8, nz), jnp.float32)
    rows_all = ny + 2 * DEEP

    def clear(r, _):
        for p in range(parts):
            for j in range(own):
                for ref in (psi, half, t1, t2, t3):
                    ref[p, j, r, pl.ds(0, 8)] = zero
                    ref[p, j, r, pl.ds(edge + 2 * nx, 8)] = zero
        return 0

    lax.fori_loop(0, rows_all, clear, 0)
    for d in (0, 1):

        @pl.when(jnp.logical_not(has[d]))
        def _():
            def clear_row(i, _):
                r = i + halo_row(1 - d)
                for p in range(parts):
                    for j in range(own):
                        for ref in (psi, half):
                            for x in range(0, 2 * nx, 8):
                                ref[p, j, r, pl.ds(edge + x, 8)] = zero
                return 0

            lax.fori_loop(0, DEEP, clear_row, 0)
            for i in range(VDEEP):
                for x in range(0, 2 * nx, 8):
                    v_now[i + (0 if d == 0 else ny + VDEEP), pl.ds(x, 8)] = zero
                    v_next[i + (0 if d == 0 else ny + VDEEP), pl.ds(x, 8)] = zero

    give_in.wait()
    keep_in.wait()
    pl.semaphore_wait(barrier, partners)
    for j in range(own):
        for q in piece_order:
            x_copy(j, q).start()
    for d in (0, 1):

        @pl.when(has[d])
        def _():
            for j in range(own):
                z_copy(j, d).start()

    for y in range(ny):
        total = None
        for p in range(parts):
            for j in range(nb):
                v = orb_v[p, j, y]
                total = v * v if total is None else total + v * v
        dens[y] = total
    first = remote(dens, chip_in, a_send.at[0], a_recv.at[0], {"band": mate})
    first.start()
    ext_in.wait()
    first.wait_recv()
    pl.semaphore_signal(ready, inc=1, device_id={"gx": ox}, device_id_type=MESH)
    my_rows = pl.ds(mid * core, mid)
    chip_sum[...] = dens[my_rows] + chip_in[my_rows]
    second = remote(chip_sum, plane_in, b_send.at[0], b_recv.at[0], {"band": far_gb})
    second.start()

    def forward(j, q):
        x_land(j, q).wait_recv()
        for d in (0, 1):
            if q in goes[d]:

                @pl.when(has[d])
                def _():
                    f_copy(j, d, q).start()

    todo = [(j, q) for j in range(own) for q in piece_order]
    forward(*todo[0])
    second.wait_recv()
    pl.semaphore_wait(ready, 1)
    shift = -1.5 * centre_weight
    v_rows = pl.ds(VDEEP + mid * core, mid)
    mine_now = ext_all[my_rows, here] - exchange_coef * cube_root(chip_sum[...] + plane_in[...])
    v_now[v_rows, here] = (mine_now + shift) * SCALE

    own_slot = v_now.at[v_rows, here]
    to_mate = remote(own_slot, own_slot, c_send.at[0, 0], c_recv.at[0, 0], {"band": mate})
    to_x = [
        remote(own_slot, own_slot, c_send.at[0, 1 + n], c_recv.at[0, 1 + core], {"gx": ox, "band": b})
        for n, b in enumerate((gb, mate))
    ]
    z_src = v_now.at[pl.ds(VDEEP + core * (ny - VDEEP), VDEEP), here]
    z_dst = v_now.at[pl.ds((1 - core) * (ny + VDEEP), VDEEP), here]
    z_to = gy + 2 * core - 1
    z_ok = jnp.logical_and(z_to >= 0, z_to < n_y)
    to_z = [
        remote(
            z_src, z_dst, c_send.at[0, 3 + 2 * m + n], c_recv.at[0, 5 - 2 * core + m],
            {"gx": x, "gy": z_to, "band": b},
        )
        for m, x in enumerate((gx, ox))
        for n, b in enumerate((gb, mate))
    ]
    for copy in to_x:
        copy.start()

    @pl.when(z_ok)
    def _():
        for copy in to_z[2:] + to_z[:2]:
            copy.start()

    to_mate.start()
    ext_here, ext_there = ext_all.at[:, here], ext_all.at[:, there]
    ext_over = remote(ext_here, ext_here, e_send.at[0], e_recv.at[0], {"gx": ox})
    for pair in todo[1:]:
        forward(*pair)

    def v_wait(ref, which, slot, rows, cols):
        land = ref.at[rows, cols]
        remote(land, land, c_send.at[which, slot], c_recv.at[which, slot], {"band": mate}).wait_recv()

    v_wait(v_now, 0, 0, pl.ds(VDEEP + mid * (1 - core), mid), here)
    for c in (0, 1):
        v_wait(v_now, 0, 1 + c, pl.ds(VDEEP + mid * c, mid), there)
    for side in (0, 1):

        @pl.when(has[side])
        def _():
            rows = pl.ds(side * (ny + VDEEP), VDEEP)
            v_wait(v_now, 0, 3 + 2 * side, rows, here)
            v_wait(v_now, 0, 4 + 2 * side, rows, there)

    psi_in.wait()
    ext_over.start()

    cols = range(0, 2 * nx, 8)
    inside = [has[d].astype(jnp.float32) for d in (0, 1)]
    group = 4

    def images(src, pot, j, first_row, emit):
        centres, lhs = {}, []
        for r in range(first_row, first_row + group):
            for p in range(parts):
                c = src[p, j, r, pl.ds(edge, 2 * nx)]
                top = c.astype(jnp.bfloat16)
                rest = (c - top.astype(jnp.float32)).astype(jnp.bfloat16)
                centres[r, p] = c, 2 * nx * len(lhs)
                lhs.append(jnp.concatenate([top, rest], axis=1))
        lines = jnp.dot(jnp.concatenate(lhs, axis=0), weights[...], preferred_element_type=jnp.float32)
        for r in range(first_row, first_row + group):
            for x in cols:
                v = pot[r - DEEP + VDEEP, pl.ds(x, 8)]
                values = []
                for p in range(parts):

                    def at(row, col):
                        return src[p, j, row, pl.ds(edge + col, 8)]

                    c, place = centres[r, p]
                    one = (at(r, x - 1) + at(r, x + 1)) + (at(r - 1, x) + at(r + 1, x))
                    two = (at(r, x - 2) + at(r, x + 2)) + (at(r - 2, x) + at(r + 2, x))
                    line = lines[place + x : place + x + 8]
                    value = v * c[x : x + 8] + ((two - 16.0 * one) + line)
                    if r < DEEP:
                        value = value * inside[0]
                    if r >= DEEP + ny:
                        value = value * inside[1]
                    values.append(value)
                emit(r, x, values)

    def exponential(start, pot, j, act, after):
        terms = (start, t1, t2, t3)

        def store(dst):
            def emit(r, x, values):
                for p, value in enumerate(values):
                    dst[p, j, r, pl.ds(edge + x, 8)] = value

            return emit

        def finish(r, x, values):
            ts = [[t[p, j, r, pl.ds(edge + x, 8)] for t in terms] + [values[p]] for p in range(parts)]

            def combine(s):
                u = s / SCALE
                even = [ts[p][0] + (-(u**2) / 2) * ts[p][2] + (u**4 / 24) * ts[p][4] for p in range(2)]
                odd = [u * ts[p][1] + (-(u**3) / 6) * ts[p][3] for p in range(2)]
                return even[0] + odd[1], even[1] - odd[0]

            act(r - DEEP, x, combine)

        emits = [store(t1), store(t2), store(t3), finish]
        for g in range((ny + 12) // group + 3):
            for k, emit in enumerate(emits):
                deep = 6 - 2 * k
                i = g - k
                if 0 <= i < (ny + 2 * deep) // group:
                    images(terms[k], pot, j, DEEP - deep + group * i, emit)
                    if k == 3:
                        after(i)

    mine = pl.ds(pl.multiple_of(nx * core, nx), nx)
    theirs = pl.ds(pl.multiple_of(nx * (1 - core), nx), nx)

    def swap_copy(q):
        rows = pl.ds(quarter * q, quarter)
        return remote(partial.at[rows, theirs], swap_in.at[rows], s_send.at[q], s_recv.at[q], {"band": mate})

    def spread_copy(q, n):
        rows = pl.ds(quarter * q, quarter)
        peer = ({"gx": ox, "band": far_gb}, {"gx": ox}, {"band": far_gb})[n]
        return remote(done.at[rows], pieces_in.at[n, rows], p_send.at[q, n], p_recv.at[q, n], peer)

    def halo_span(q, d):
        low, high = (ny - VDEEP, ny) if d else (0, VDEEP)
        return max(low, quarter * q), min(high, quarter * (q + 1))

    def v_halo_out(q, d):
        copies = []
        for n, b in enumerate((gb, mate)):
            low, high = halo_span(q, d)
            src = v_next.at[pl.ds(VDEEP + low, high - low), mine]
            dst = v_next.at[pl.ds(VDEEP + low + (-ny if d else ny), high - low), mine]
            copies.append(
                remote(src, dst, v_send.at[q, d, n], v_recv.at[q, d, core], {"gy": z_peer(d), "band": b})
            )
        return copies

    def v_halo_land(q, d, c):
        low, high = halo_span(q, d)
        land = v_next.at[pl.ds(VDEEP + low + (-ny if d else ny), high - low), pl.ds(nx * c, nx)]
        return remote(land, land, v_send.at[q, d, c], v_recv.at[q, d, c], {"gy": z_peer(1 - d)})

    spans = [[q for q in pieces if halo_span(q, d)[0] < halo_span(q, d)[1]] for d in (0, 1)]

    def v_mate(q, tile):
        rows = v_next.at[pl.ds(VDEEP + quarter * q, quarter), tile]
        return remote(rows, rows, m_send.at[q], m_recv.at[q], {"band": mate})

    for j in range(own):
        for side in (0, 1):

            @pl.when(has[side])
            def _():
                d = 1 - side
                z_land(j, d).wait_recv()
                for q in goes[d]:
                    f_land(j, d, q).wait_recv()

        def keep_both(y, x, combine):
            for p, value in enumerate(combine(step_length / 2)):
                half[p, j, DEEP + y, pl.ds(edge + x, 8)] = value
            re, im = combine(step_length)
            square = re * re + im * im
            if j:
                square = square + partial[y, pl.ds(x, 8)]
            partial[y, pl.ds(x, 8)] = square

        def swap(i):
            if j == own - 1:
                swap_copy(i).start()

        exponential(psi, v_now, j, keep_both, swap)
        for d in (0, 1):

            @pl.when(has[d])
            def _():
                h_copy(j, d).start()

    for q in pieces:
        rows = pl.ds(quarter * q, quarter)
        swap_copy(q).wait_recv()
        done[rows] = partial[rows, mine] + swap_in[rows]
        for n in range(3):
            spread_copy(q, n).start()
    remote(ext_there, ext_there, e_send.at[0], e_recv.at[0], {"gx": ox}).wait_recv()
    for q in pieces:
        rows = pl.ds(quarter * q, quarter)
        for n in range(3):
            spread_copy(q, n).wait_recv()
        total = (done[rows] + pieces_in[0, rows]) + (pieces_in[1, rows] + pieces_in[2, rows])
        mine_next = ext_all[rows, mine] - exchange_coef * cube_root(total)
        v_next[pl.ds(VDEEP + quarter * q, quarter), mine] = (mine_next + shift) * SCALE
        for d in (0, 1):
            if q in spans[d]:

                @pl.when(has[d])
                def _():
                    for copy in v_halo_out(q, d):
                        copy.start()

        v_mate(q, mine).start()
    for q in pieces:
        v_mate(q, theirs).wait_recv()
    pot_v[...] = v_next[pl.ds(VDEEP, ny), here] * (1.0 / SCALE) - shift
    pot_out = pltpu.make_async_copy(pot_v, pot_ref, in_sem.at[4])
    pot_out.start()
    for side in (0, 1):

        @pl.when(has[side])
        def _():
            d = 1 - side
            for q in spans[d]:
                for c in (0, 1):
                    v_halo_land(q, d, c).wait_recv()

    def back_copy(j, q):
        rows = pl.ds(quarter * q, quarter)
        return remote(
            result.at[:, j, rows, there],
            out_ref.at[:, own * gx + j, rows],
            r_send.at[j, q], r_recv.at[j, q], {"gx": ox},
        )

    def back_land(j, q):
        land = out_ref.at[:, own * ox + j, pl.ds(quarter * q, quarter)]
        return remote(land, land, r_send.at[j, q], r_recv.at[j, q], {"gx": ox})

    def stay_copy(j, q):
        rows = pl.ds(quarter * q, quarter)
        return pltpu.make_async_copy(result.at[:, j, rows, here], out_ref.at[:, own * gx + j, rows], l_sem.at[j, q])

    for j in range(own):
        for side in (0, 1):

            @pl.when(has[side])
            def _():
                h_land(j, 1 - side).wait_recv()

        def keep_result(y, x, combine):
            for p, value in enumerate(combine(step_length / 2)):
                result[p, j, y, pl.ds(x, 8)] = value

        def send_back(q):
            back_copy(j, q).start()
            stay_copy(j, q).start()

        exponential(half, v_next, j, keep_result, send_back)

    pot_out.wait()
    first.wait_send()
    second.wait_send()
    to_mate.wait_send()
    ext_over.wait_send()
    for q in pieces:
        swap_copy(q).wait_send()
        v_mate(q, mine).wait_send()
        for n in range(3):
            spread_copy(q, n).wait_send()
    for copy in to_x:
        copy.wait_send()

    @pl.when(z_ok)
    def _():
        for copy in to_z:
            copy.wait_send()

    for d in (0, 1):

        @pl.when(has[d])
        def _():
            for q in spans[d]:
                for copy in v_halo_out(q, d):
                    copy.wait_send()
            for j in range(own):
                z_copy(j, d).wait_send()
                h_copy(j, d).wait_send()
                for q in goes[d]:
                    f_copy(j, d, q).wait_send()

    for j in range(own):
        for q in pieces:
            x_copy(j, q).wait_send()
            back_copy(j, q).wait_send()
            stay_copy(j, q).wait()
            back_land(j, q).wait_recv()


def whole_body(counts, orbitals, external):
    parts, nb, nx, ny, nz = orbitals.shape
    own = nb // 2
    nq = ny // 4
    dma = pltpu.SemaphoreType.DMA
    term = pltpu.VMEM((parts, own, ny + 2 * DEEP, 2 * nx + 16, nz), jnp.float32)
    block = pltpu.VMEM((ny, nx, nz), jnp.float32)
    half_block = pltpu.VMEM((ny // 2, nx, nz), jnp.float32)
    wide = pltpu.VMEM((ny + 2 * VDEEP, 2 * nx, nz), jnp.float32)
    result, potential = pl.pallas_call(
        functools.partial(whole_kernel, counts),
        out_shape=(
            jax.ShapeDtypeStruct((parts, nb, ny, nx, nz), jnp.float32),
            jax.ShapeDtypeStruct((ny, nx, nz), jnp.float32),
        ),
        in_specs=[pl.BlockSpec(memory_space=pltpu.HBM)] * 2,
        out_specs=(pl.BlockSpec(memory_space=pl.ANY),) * 2,
        scratch_shapes=[
            term, term, term, term, term,
            pltpu.VMEM((parts, nb, ny, nx, nz), jnp.float32),
            pltpu.VMEM((ny, 2 * nx, nz), jnp.float32),
            wide, wide,
            block, block, half_block, half_block,
            pltpu.VMEM((ny, 2 * nx, nz), jnp.float32),
            block,
            pltpu.VMEM((3, ny, nx, nz), jnp.float32),
            block,
            pltpu.VMEM((parts, own, ny, 2 * nx, nz), jnp.float32),
            block,
            pltpu.VMEM((2 * nz, nz), jnp.bfloat16),
            dma((5,)),
            dma((own, nq)), dma((own, nq)),
            dma((2, own)), dma((2, own)),
            dma((2, own, nq)), dma((2, own, nq)),
            dma((2, own)), dma((2, own)),
            dma((1,)), dma((1,)),
            dma((1,)), dma((1,)),
            dma((1, 7)), dma((1, 7)),
            dma((1,)), dma((1,)),
            dma((own, nq)), dma((own, nq)),
            dma((own, nq)),
            dma((nq,)), dma((nq,)),
            dma((nq, 3)), dma((nq, 3)),
            dma((nq, 2, 2)), dma((nq, 2, 2)),
            dma((nq,)), dma((nq,)),
            pltpu.SemaphoreType.REGULAR,
        ],
        compiler_params=pltpu.CompilerParams(
            collective_id=0, has_side_effects=True, vmem_limit_bytes=32 * 1024 * 1024
        ),
    )(
        pltpu.with_memory_space_constraint(jnp.transpose(orbitals, (0, 1, 3, 2, 4)), pltpu.HBM),
        pltpu.with_memory_space_constraint(jnp.swapaxes(external, 0, 1), pltpu.HBM),
    )
    return jnp.transpose(result, (0, 1, 3, 2, 4)), jnp.swapaxes(potential, 0, 1)


def body(counts, orbitals, external):
    parts, nb, nx, ny, nz = orbitals.shape
    n_x, n_y, n_b = counts
    if n_x == 2 and n_b == 4 and nb % 2 == 0 and nx % 8 == 0 and ny % 4 == 0 and ny >= 2 * VDEEP:
        return whole_body(counts, orbitals, external)
    return step_body(counts, orbitals, external)


def solution(mesh):
    counts = (mesh.shape["gx"], mesh.shape["gy"], mesh.shape["band"])
    in_specs = (P(None, "band", "gx", "gy", None), P("gx", "gy", None))
    out_specs = (P(None, "band", "gx", "gy", None), P("gx", "gy", None))
    return jax.shard_map(
        functools.partial(body, counts), mesh=mesh, in_specs=in_specs, out_specs=out_specs, check_vma=False
    )
```

```python
import functools

import jax
import jax.numpy as jnp
from jax import lax
from jax.experimental import pallas as pl
from jax.experimental.pallas import tpu as pltpu
from jax.sharding import PartitionSpec as P

step_length = 0.15
exchange_coef = 0.7386
centre_weight = -2.5
near_weight = 4.0 / 3.0
far_weight = -1.0 / 12.0
MESH = pl.DeviceIdType.MESH


def cube_root(d):
    guess = jnp.exp(jnp.log(d) * (1.0 / 3.0))
    better = guess - (guess - d / (guess * guess)) * (1.0 / 3.0)
    return jnp.where(d > 1e-30, better, guess)


def step_kernel(counts, orb_hbm, ext_hbm, out_ref, pot_ref, *scratch):
    terms = scratch[:8]
    orb_ref, ext_ref, pot_wide, density, in_sem, x_send, x_recv, y_send, y_recv, d_send, d_recv = scratch[8:]
    n_x, n_y, n_b = counts
    nf, ny, nx, nz = orb_ref.shape
    gx = lax.axis_index("gx")
    gy = lax.axis_index("gy")
    gb = lax.axis_index("band")
    has = {
        ("gx", 0): gx > 0,
        ("gx", 1): gx < n_x - 1,
        ("gy", 0): gy > 0,
        ("gy", 1): gy < n_y - 1,
    }
    place = {"gx": gx, "gy": gy}
    if n_x == 2:
        x_sides = [("gx", 1 - gx)]
    else:
        x_sides = [("gx", 0), ("gx", 1)]
    y_sides = [("gy", 0), ("gy", 1)]
    sides = [("gx", 0), ("gx", 1)] + y_sides
    peers = [lax.rem(gb + j, n_b) for j in range(1, n_b)]

    def target(side):
        axis, up = side
        return {axis: place[axis] + (2 * up - 1)}

    barrier = pltpu.get_barrier_semaphore()
    partners = n_b - 1
    for side in sides:
        partners = partners + has[side].astype(jnp.int32)

        @pl.when(has[side])
        def _():
            pl.semaphore_signal(barrier, inc=1, device_id=target(side), device_id_type=MESH)

    for peer in peers:
        pl.semaphore_signal(barrier, inc=1, device_id={"band": peer}, device_id_type=MESH)
    orb_in = pltpu.make_async_copy(orb_hbm, orb_ref, in_sem.at[0])
    orb_in.start()
    ext_in = pltpu.make_async_copy(ext_hbm, ext_ref, in_sem.at[1])
    ext_in.start()

    chunks = max(1, min(6, ny // 2))
    x_cuts = [(j * (ny // chunks), ny // chunks + (ny % chunks if j == chunks - 1 else 0)) for j in range(chunks)]
    mid = (nx - 4) // 2
    y_cuts = [(0, 2), (nx - 2, 2), (2, mid), (2 + mid, nx - 4 - mid)]
    d_cuts = [(0, 2), (ny - 2, 2), (2, ny - 4)]
    order = sorted(range(chunks), key=lambda j: 0 if j in (0, chunks - 1) else 1)
    sems = {"gx": (x_send, x_recv), "gy": (y_send, y_recv)}

    def cells(axis, edge, piece):
        if axis == "gx":
            return pl.ds(edge, 2), pl.ds(2 + x_cuts[piece][0], x_cuts[piece][1])
        return pl.ds(2 + y_cuts[piece][0], y_cuts[piece][1]), pl.ds(edge, 2)

    def pick(up, high, low):
        if isinstance(up, int):
            return high if up else low
        return low + up * (high - low)

    def send_copy(step, side, piece):
        axis, up = side
        extent = nx if axis == "gx" else ny
        return pltpu.make_async_remote_copy(
            src_ref=terms[step].at[cells(axis, pick(up, extent, 2), piece)],
            dst_ref=terms[step].at[cells(axis, pick(up, 0, extent + 2), piece)],
            send_sem=sems[axis][0].at[step, up, piece],
            recv_sem=sems[axis][1].at[step, 1 - up, piece],
            device_id=target(side),
            device_id_type=MESH,
        )

    def recv_copy(step, side, piece):
        axis, up = side
        extent = nx if axis == "gx" else ny
        land = terms[step].at[cells(axis, pick(up, extent + 2, 0), piece)]
        return pltpu.make_async_remote_copy(
            src_ref=land,
            dst_ref=land,
            send_sem=sems[axis][0].at[step, up, piece],
            recv_sem=sems[axis][1].at[step, up, piece],
            device_id=target(side),
            device_id_type=MESH,
        )

    def each(side, act):
        if side[0] == "gx" and n_x == 2:
            act()
        else:
            pl.when(has[side])(act)

    def start(step, side, pieces):
        def act():
            for piece in pieces:
                send_copy(step, side, piece).start()

        each(side, act)

    def await_pieces(step, side, pieces):
        def act():
            for piece in pieces:
                recv_copy(step, side, piece).wait_recv()

        each(side, act)

    def density_copy(which, j, piece):
        rows = pl.ds(*d_cuts[piece])
        return pltpu.make_async_remote_copy(
            src_ref=density.at[which, 0, rows],
            dst_ref=density.at[which, n_b - 1 - j, rows],
            send_sem=d_send.at[which, j, piece],
            recv_sem=d_recv.at[which, n_b - 2 - j, piece],
            device_id={"band": peers[j]},
            device_id_type=MESH,
        )

    def start_density(which, piece):
        for j in range(n_b - 1):
            density_copy(which, j, piece).start()

    def finish_potential(which):
        for piece in range(3):
            rows = pl.ds(*d_cuts[piece])
            for slot in range(1, n_b):
                pltpu.make_async_remote_copy(
                    src_ref=density.at[which, slot, rows],
                    dst_ref=density.at[which, slot, rows],
                    send_sem=d_send.at[which, slot - 1, piece],
                    recv_sem=d_recv.at[which, slot - 1, piece],
                    device_id={"band": peers[slot - 1]},
                    device_id_type=MESH,
                ).wait_recv()
        total = density[which, 0]
        for slot in range(1, n_b):
            total = total + density[which, slot]
        pot = ext_ref[...] - exchange_coef * cube_root(total)
        if which == 1:
            pot_ref[...] = pot
        wide = pot - 1.5 * centre_weight
        for y in range(ny):
            for x in range(nx):
                pot_wide[x, y] = jnp.broadcast_to(wide[y, x : x + 1], (nf, nz))

    for side in sides:
        axis, up = side

        @pl.when(jnp.logical_not(has[side]))
        def _():
            for step in range(8):
                if axis == "gx":
                    shape = (2, ny, nf, nz)
                    terms[step][pl.ds(nx + 2 if up else 0, 2), pl.ds(2, ny)] = jnp.zeros(shape, jnp.float32)
                else:
                    shape = (nx, 2, nf, nz)
                    terms[step][pl.ds(2, nx), pl.ds(ny + 2 if up else 0, 2)] = jnp.zeros(shape, jnp.float32)

    orb_in.wait()
    for y in range(ny):
        block = orb_ref[:, y]
        terms[0][pl.ds(2, nx), y + 2] = jnp.swapaxes(block, 0, 1)
        density[0, 0, y] = jnp.sum(block * block, axis=0)
    pl.semaphore_wait(barrier, partners)
    for side in x_sides:
        start(0, side, order)
    for side in y_sides:
        start(0, side, range(4))
    for piece in range(3):
        start_density(0, piece)
    ext_in.wait()

    lane = lax.broadcasted_iota(jnp.int32, (nf, nz), 1)
    near = -0.5 * near_weight
    far = -0.5 * far_weight
    below1 = jnp.where(lane >= 1, near, 0.0)
    above1 = jnp.where(lane < nz - 1, near, 0.0)
    below2 = jnp.where(lane >= 2, far, 0.0)
    above2 = jnp.where(lane < nz - 2, far, 0.0)
    half = nf // 2
    field = lax.broadcasted_iota(jnp.int32, (nf, nz), 0)
    turn_sign = jnp.where(field < half, 1.0, -1.0)

    def turned(v):
        return jnp.concatenate([v[half:], v[:half]], axis=0) * turn_sign

    def image(step, x, y):
        t = terms[step]
        c = t[x + 2, y + 2]
        one = (t[x + 1, y + 2] + t[x + 3, y + 2]) + (
            t[x + 2, y + 1] + t[x + 2, y + 3]
        )
        two = (t[x, y + 2] + t[x + 4, y + 2]) + (
            t[x + 2, y] + t[x + 2, y + 4]
        )
        total = pot_wide[x, y] * c + near * one + far * two
        total = total + pltpu.roll(c, 1, 1) * below1 + pltpu.roll(c, nz - 1, 1) * above1
        return total + (pltpu.roll(c, 2, 1) * below2 + pltpu.roll(c, nz - 2, 1) * above2)

    def combine(parts, s):
        even = parts[0] + (-(s**2) / 2) * parts[2] + (s**4 / 24) * parts[4]
        odd = s * parts[1] + (-(s**3) / 6) * parts[3]
        return even + turned(odd)

    def advance(step, xs, ys):
        at = [(x, y) for x in xs for y in ys]
        new = [image(step, x, y) for x, y in at]
        if step % 4 < 3:
            for (x, y), value in zip(at, new):
                terms[step + 1][x + 2, y + 2] = value
            return
        parts = [[terms[step - 3 + k][x + 2, y + 2] for k in range(4)] + [value] for (x, y), value in zip(at, new)]
        halves = [combine(part, step_length / 2) for part in parts]
        if step == 7:
            for (x, y), value in zip(at, halves):
                out_ref[x, y] = value
            return
        predicted = [combine(part, step_length) for part in parts]
        squares = [jnp.sum(value * value, axis=0, keepdims=True) for value in predicted]
        for (x, y), value, square in zip(at, halves, squares):
            terms[4][x + 2, y + 2] = value
            density[1, 0, y, pl.ds(x, 1)] = square

    rim = [0, 1, nx - 2, nx - 1]
    for step in range(8):
        if step % 4 == 0:
            finish_potential(step // 4)
        for n, j in enumerate(order):
            edges = [("gy", up) for up, at in ((0, 0), (1, chunks - 1)) if at == j]
            for side in x_sides:
                await_pieces(step, side, [j])
            for side in edges:
                await_pieces(step, side, [0, 1])
            advance(step, rim, range(x_cuts[j][0], sum(x_cuts[j])))
            if step < 7:
                for side in x_sides:
                    start(step + 1, side, [j])
                for side in edges:
                    start(step + 1, side, [0, 1])
            if n == min(1, chunks - 1):
                for piece in (2, 3):
                    for side in y_sides:
                        await_pieces(step, side, [piece])
                    advance(step, range(y_cuts[piece][0], sum(y_cuts[piece])), [0, 1, ny - 2, ny - 1])
                    if step < 7:
                        for side in y_sides:
                            start(step + 1, side, [piece])
                if step == 3:
                    start_density(1, 0)
                    start_density(1, 1)
        for x in range(2, nx - 2):
            advance(step, [x], range(2, ny - 2))
        if step == 3:
            start_density(1, 2)

    for side in x_sides + y_sides:

        def drain():
            for step in range(8):
                for piece in range(chunks if side[0] == "gx" else 4):
                    send_copy(step, side, piece).wait_send()

        each(side, drain)

    for which in (0, 1):
        for j in range(n_b - 1):
            for piece in range(3):
                density_copy(which, j, piece).wait_send()


def step_body(counts, orbitals, external):
    parts, bands, nx, ny, nz = orbitals.shape
    nf = parts * bands
    fields = jnp.transpose(orbitals.reshape(nf, nx, ny, nz), (0, 2, 1, 3))
    n_b = counts[2]
    dma = pltpu.SemaphoreType.DMA
    result, potential = pl.pallas_call(
        functools.partial(step_kernel, counts),
        out_shape=(
            jax.ShapeDtypeStruct((nx, ny, nf, nz), jnp.float32),
            jax.ShapeDtypeStruct((ny, nx, nz), jnp.float32),
        ),
        in_specs=[pl.BlockSpec(memory_space=pltpu.HBM)] * 2,
        out_specs=(pl.BlockSpec(memory_space=pltpu.VMEM),) * 2,
        scratch_shapes=[
            *[pltpu.VMEM((nx + 4, ny + 4, nf, nz), jnp.float32)] * 8,
            pltpu.VMEM((nf, ny, nx, nz), jnp.float32),
            pltpu.VMEM((ny, nx, nz), jnp.float32),
            pltpu.VMEM((nx, ny, nf, nz), jnp.float32),
            pltpu.VMEM((2, n_b, ny, nx, nz), jnp.float32),
            dma((2,)),
            dma((8, 2, 6)),
            dma((8, 2, 6)),
            dma((8, 2, 4)),
            dma((8, 2, 4)),
            dma((2, n_b - 1, 3)),
            dma((2, n_b - 1, 3)),
        ],
        compiler_params=pltpu.CompilerParams(
            collective_id=0, has_side_effects=True, vmem_limit_bytes=40 * 1024 * 1024
        ),
    )(fields, jnp.swapaxes(external, 0, 1))
    result = jnp.transpose(result, (2, 0, 1, 3)).reshape(orbitals.shape)
    return (result, jnp.swapaxes(potential, 0, 1))


DEEP = 8
VDEEP = 6
SCALE = 24.0


def whole_kernel(counts, orb_hbm, ext_hbm, out_ref, pot_ref, *scratch):
    (
        psi, half, t1, t2, t3, orb_v, ext_all, v_now, v_next, dens, chip_in, chip_sum, plane_in, partial, swap_in,
        pieces_in, done, result, pot_v, weights,
        in_sem, row_send, block_send, half_send, side_send, v_now_send, v_next_send, stay_sem,
        x_recv, halo_recv, half_recv, first_recv, second_recv, mate_recv, over_recv, v_side_recv,
        ext_recv, swap_recv, spread_recv, v_next_recv, back_recv, ready,
    ) = scratch
    n_x, n_y, n_b = counts
    parts, nb, ny, nx, nz = orb_hbm.shape
    own = nb // 2
    mid = ny // 2
    gx = lax.axis_index("gx")
    gy = lax.axis_index("gy")
    gb = lax.axis_index("band")
    ox = 1 - gx
    core = lax.rem(gb, 2)
    mate = gb + 1 - 2 * core
    far_gb = lax.rem(gb + 2, n_b)
    has = (gy > 0, gy < n_y - 1)
    edge = 8
    here = pl.ds(pl.multiple_of(nx * gx, nx), nx)
    there = pl.ds(pl.multiple_of(nx * ox, nx), nx)
    here_pad = pl.ds(pl.multiple_of(edge + nx * gx, 8), nx)
    there_pad = pl.ds(pl.multiple_of(edge + nx * ox, 8), nx)

    def z_peer(d):
        return gy + (2 * d - 1)

    in_plane = [{"band": mate}, {"band": far_gb}, {"gx": ox}]
    barrier = pltpu.get_barrier_semaphore()
    partners = len(in_plane)
    for peer in in_plane:
        pl.semaphore_signal(barrier, inc=1, device_id=peer, device_id_type=MESH)
    for d in (0, 1):
        partners = partners + has[d].astype(jnp.int32)

        @pl.when(has[d])
        def _():
            pl.semaphore_signal(barrier, inc=1, device_id={"gy": z_peer(d)}, device_id_type=MESH)

    give = pl.ds(pl.multiple_of(own * ox, own), own)
    keep = pl.ds(pl.multiple_of(own * gx, own), own)
    give_in = pltpu.make_async_copy(orb_hbm.at[:, give], orb_v.at[:, give], in_sem.at[0])
    keep_in = pltpu.make_async_copy(orb_hbm.at[:, keep], orb_v.at[:, keep], in_sem.at[1])
    ext_in = pltpu.make_async_copy(ext_hbm, ext_all.at[:, here], in_sem.at[2])
    psi_in = pltpu.make_async_copy(
        orb_hbm.at[:, keep], psi.at[:, :, pl.ds(DEEP, ny), here_pad], in_sem.at[3]
    )
    give_in.start()
    keep_in.start()
    ext_in.start()
    psi_in.start()

    def remote(src, dst, send, recv, peer):
        return pltpu.make_async_remote_copy(
            src_ref=src, dst_ref=dst, send_sem=send, recv_sem=recv, device_id=peer, device_id_type=MESH
        )

    def sent(like, sem):
        remote(like, like, sem, sem, {"band": mate}).wait_send()

    def landed(like, sem):
        remote(like, like, sem, sem, {"band": mate}).wait_recv()

    quarter = 4
    pieces = list(range(ny // quarter))
    goes = ([q for q in pieces if quarter * q < DEEP], [q for q in pieces if quarter * q >= ny - DEEP])
    piece_order = sorted(pieces, key=lambda q: 0 if q in goes[0] and q in goes[1] else 1)

    def x_copy(j, q):
        return remote(
            orb_v.at[:, own * ox + j, pl.ds(quarter * q, quarter)],
            psi.at[:, j, pl.ds(DEEP + quarter * q, quarter), here_pad],
            row_send, x_recv.at[j, q], {"gx": ox},
        )

    def x_land(j, q):
        land = psi.at[:, j, pl.ds(DEEP + quarter * q, quarter), there_pad]
        return remote(land, land, row_send, x_recv.at[j, q], {"gx": ox})

    def halo_row(d):
        return 0 if d else DEEP + ny

    def z_copy(j, d):
        return remote(
            orb_v.at[:, own * gx + j, pl.ds(ny - DEEP if d else 0, DEEP)],
            psi.at[:, j, pl.ds(halo_row(d), DEEP), here_pad],
            side_send.at[d], halo_recv.at[d, j], {"gy": z_peer(d)},
        )

    def halo_land(ref, j, d, sems):
        landed(ref.at[:, j, pl.ds(halo_row(d), DEEP), pl.ds(edge, 2 * nx)], sems.at[d, j])

    def f_row(d, q):
        return DEEP + quarter * q + (-ny if d else ny)

    def f_copy(j, d, q):
        return remote(
            psi.at[:, j, pl.ds(DEEP + quarter * q, quarter), there_pad],
            psi.at[:, j, pl.ds(f_row(d, q), quarter), there_pad],
            side_send.at[d], halo_recv.at[d, j], {"gy": z_peer(d)},
        )

    def h_copy(j, d):
        return remote(
            half.at[:, j, pl.ds(ny if d else DEEP, DEEP), pl.ds(edge, 2 * nx)],
            half.at[:, j, pl.ds(halo_row(d), DEEP), pl.ds(edge, 2 * nx)],
            side_send.at[d], half_recv.at[d, j], {"gy": z_peer(d)},
        )

    apart = lax.broadcasted_iota(jnp.int32, (2, nz, nz), 1) - lax.broadcasted_iota(jnp.int32, (2, nz, nz), 2)
    apart = jnp.abs(apart).reshape(2 * nz, nz)
    weights[...] = jnp.where(apart == 1, -16.0, jnp.where(apart == 2, 1.0, 0.0)).astype(jnp.bfloat16)
    zero = jnp.zeros((8, nz), jnp.float32)
    rows_all = ny + 2 * DEEP

    def clear(r, _):
        for p in range(parts):
            for j in range(own):
                for ref in (psi, half, t1, t2, t3):
                    ref[p, j, r, pl.ds(0, 8)] = zero
                    ref[p, j, r, pl.ds(edge + 2 * nx, 8)] = zero
        return 0

    lax.fori_loop(0, rows_all, clear, 0)
    for d in (0, 1):

        @pl.when(jnp.logical_not(has[d]))
        def _():
            def clear_row(i, _):
                r = i + halo_row(1 - d)
                for p in range(parts):
                    for j in range(own):
                        for ref in (psi, half):
                            for x in range(0, 2 * nx, 8):
                                ref[p, j, r, pl.ds(edge + x, 8)] = zero
                return 0

            lax.fori_loop(0, DEEP, clear_row, 0)
            for i in range(VDEEP):
                for x in range(0, 2 * nx, 8):
                    v_now[i + (0 if d == 0 else ny + VDEEP), pl.ds(x, 8)] = zero
                    v_next[i + (0 if d == 0 else ny + VDEEP), pl.ds(x, 8)] = zero

    give_in.wait()
    keep_in.wait()
    pl.semaphore_wait(barrier, partners)
    for j in range(own):
        for q in piece_order:
            x_copy(j, q).start()
    for d in (0, 1):

        @pl.when(has[d])
        def _():
            for j in range(own):
                z_copy(j, d).start()

    for y in range(ny):
        total = None
        for p in range(parts):
            for j in range(nb):
                v = orb_v[p, j, y]
                total = v * v if total is None else total + v * v
        dens[y] = total
    first = remote(dens, chip_in, block_send, first_recv, {"band": mate})
    first.start()
    ext_in.wait()
    first.wait_recv()
    pl.semaphore_signal(ready, inc=1, device_id={"gx": ox}, device_id_type=MESH)
    my_rows = pl.ds(mid * core, mid)
    chip_sum[...] = dens[my_rows] + chip_in[my_rows]
    second = remote(chip_sum, plane_in, half_send, second_recv, {"band": far_gb})
    second.start()

    def forward(j, q):
        x_land(j, q).wait_recv()
        for d in (0, 1):
            if q in goes[d]:

                @pl.when(has[d])
                def _():
                    f_copy(j, d, q).start()

    todo = [(j, q) for j in range(own) for q in piece_order]
    forward(*todo[0])
    second.wait_recv()
    pl.semaphore_wait(ready, 1)
    shift = -1.5 * centre_weight
    v_rows = pl.ds(VDEEP + mid * core, mid)
    mine_now = ext_all[my_rows, here] - exchange_coef * cube_root(chip_sum[...] + plane_in[...])
    v_now[v_rows, here] = (mine_now + shift) * SCALE

    own_slot = v_now.at[v_rows, here]
    to_mate = remote(own_slot, own_slot, half_send, mate_recv, {"band": mate})
    to_x = [
        remote(own_slot, own_slot, block_send, over_recv, {"gx": ox, "band": b})
        for n, b in enumerate((gb, mate))
    ]
    z_src = v_now.at[pl.ds(VDEEP + core * (ny - VDEEP), VDEEP), here]
    z_dst = v_now.at[pl.ds((1 - core) * (ny + VDEEP), VDEEP), here]
    z_to = gy + 2 * core - 1
    z_ok = jnp.logical_and(z_to >= 0, z_to < n_y)
    to_z = [
        remote(
            z_src, z_dst, v_now_send, v_side_recv.at[1 - core],
            {"gx": x, "gy": z_to, "band": b},
        )
        for m, x in enumerate((gx, ox))
        for n, b in enumerate((gb, mate))
    ]
    for copy in to_x:
        copy.start()

    @pl.when(z_ok)
    def _():
        for copy in to_z[2:] + to_z[:2]:
            copy.start()

    to_mate.start()
    ext_here, ext_there = ext_all.at[:, here], ext_all.at[:, there]
    ext_over = remote(ext_here, ext_here, block_send, ext_recv, {"gx": ox})
    for pair in todo[1:]:
        forward(*pair)

    landed(v_now.at[pl.ds(VDEEP + mid * (1 - core), mid), here], mate_recv)
    landed(v_now.at[pl.ds(VDEEP, ny), there], over_recv)
    for side in (0, 1):

        @pl.when(has[side])
        def _():
            landed(v_now.at[pl.ds(side * (ny + VDEEP), VDEEP)], v_side_recv.at[side])

    psi_in.wait()
    ext_over.start()

    cols = range(0, 2 * nx, 8)
    inside = [has[d].astype(jnp.float32) for d in (0, 1)]
    group = 4

    def images(src, pot, j, first_row, emit):
        centres, lhs = {}, []
        for r in range(first_row, first_row + group):
            for p in range(parts):
                c = src[p, j, r, pl.ds(edge, 2 * nx)]
                top = c.astype(jnp.bfloat16)
                rest = (c - top.astype(jnp.float32)).astype(jnp.bfloat16)
                centres[r, p] = c, 2 * nx * len(lhs)
                lhs.append(jnp.concatenate([top, rest], axis=1))
        lines = jnp.dot(jnp.concatenate(lhs, axis=0), weights[...], preferred_element_type=jnp.float32)
        for r in range(first_row, first_row + group):
            for x in cols:
                v = pot[r - DEEP + VDEEP, pl.ds(x, 8)]
                values = []
                for p in range(parts):

                    def at(row, col):
                        return src[p, j, row, pl.ds(edge + col, 8)]

                    c, place = centres[r, p]
                    one = (at(r, x - 1) + at(r, x + 1)) + (at(r - 1, x) + at(r + 1, x))
                    two = (at(r, x - 2) + at(r, x + 2)) + (at(r - 2, x) + at(r + 2, x))
                    line = lines[place + x : place + x + 8]
                    value = v * c[x : x + 8] + ((two - 16.0 * one) + line)
                    if r < DEEP:
                        value = value * inside[0]
                    if r >= DEEP + ny:
                        value = value * inside[1]
                    values.append(value)
                emit(r, x, values)

    def exponential(start, pot, j, act, after):
        terms = (start, t1, t2, t3)

        def store(dst):
            def emit(r, x, values):
                for p, value in enumerate(values):
                    dst[p, j, r, pl.ds(edge + x, 8)] = value

            return emit

        def finish(r, x, values):
            ts = [[t[p, j, r, pl.ds(edge + x, 8)] for t in terms] + [values[p]] for p in range(parts)]

            def combine(s):
                u = s / SCALE
                even = [ts[p][0] + (-(u**2) / 2) * ts[p][2] + (u**4 / 24) * ts[p][4] for p in range(2)]
                odd = [u * ts[p][1] + (-(u**3) / 6) * ts[p][3] for p in range(2)]
                return even[0] + odd[1], even[1] - odd[0]

            act(r - DEEP, x, combine)

        emits = [store(t1), store(t2), store(t3), finish]
        for g in range((ny + 12) // group + 3):
            for k, emit in enumerate(emits):
                deep = 6 - 2 * k
                i = g - k
                if 0 <= i < (ny + 2 * deep) // group:
                    images(terms[k], pot, j, DEEP - deep + group * i, emit)
                    if k == 3:
                        after(i)

    mine = pl.ds(pl.multiple_of(nx * core, nx), nx)
    theirs = pl.ds(pl.multiple_of(nx * (1 - core), nx), nx)

    def swap_copy(q):
        rows = pl.ds(quarter * q, quarter)
        return remote(partial.at[rows, theirs], swap_in.at[rows], block_send, swap_recv.at[q], {"band": mate})

    def spread_copy(q, n):
        rows = pl.ds(quarter * q, quarter)
        peer = ({"gx": ox, "band": far_gb}, {"gx": ox}, {"band": far_gb})[n]
        return remote(done.at[rows], pieces_in.at[n, rows], block_send, spread_recv.at[q], peer)

    def halo_span(q, d):
        low, high = (ny - VDEEP, ny) if d else (0, VDEEP)
        return max(low, quarter * q), min(high, quarter * (q + 1))

    def v_halo_out(q, d):
        copies = []
        for n, b in enumerate((gb, mate)):
            low, high = halo_span(q, d)
            src = v_next.at[pl.ds(VDEEP + low, high - low), mine]
            dst = v_next.at[pl.ds(VDEEP + low + (-ny if d else ny), high - low), mine]
            copies.append(
                remote(src, dst, v_next_send.at[d], v_next_recv.at[1 - d], {"gy": z_peer(d), "band": b})
            )
        return copies

    spans = [[q for q in pieces if halo_span(q, d)[0] < halo_span(q, d)[1]] for d in (0, 1)]

    def v_mate(q, tile):
        rows = v_next.at[pl.ds(VDEEP + quarter * q, quarter), tile]
        return remote(rows, rows, block_send, mate_recv, {"band": mate})

    for j in range(own):
        for side in (0, 1):

            @pl.when(has[side])
            def _():
                halo_land(psi, j, 1 - side, halo_recv)

        def keep_both(y, x, combine):
            for p, value in enumerate(combine(step_length / 2)):
                half[p, j, DEEP + y, pl.ds(edge + x, 8)] = value
            re, im = combine(step_length)
            square = re * re + im * im
            if j:
                square = square + partial[y, pl.ds(x, 8)]
            partial[y, pl.ds(x, 8)] = square

        def swap(i):
            if j == own - 1:
                swap_copy(i).start()

        exponential(psi, v_now, j, keep_both, swap)
        for d in (0, 1):

            @pl.when(has[d])
            def _():
                h_copy(j, d).start()

    for q in pieces:
        rows = pl.ds(quarter * q, quarter)
        swap_copy(q).wait_recv()
        done[rows] = partial[rows, mine] + swap_in[rows]
        for n in range(3):
            spread_copy(q, n).start()
    remote(ext_there, ext_there, block_send, ext_recv, {"gx": ox}).wait_recv()
    for q in pieces:
        rows = pl.ds(quarter * q, quarter)
        landed(pieces_in.at[:, rows], spread_recv.at[q])
        total = (done[rows] + pieces_in[0, rows]) + (pieces_in[1, rows] + pieces_in[2, rows])
        mine_next = ext_all[rows, mine] - exchange_coef * cube_root(total)
        v_next[pl.ds(VDEEP + quarter * q, quarter), mine] = (mine_next + shift) * SCALE
        for d in (0, 1):
            if q in spans[d]:

                @pl.when(has[d])
                def _():
                    for copy in v_halo_out(q, d):
                        copy.start()

        v_mate(q, mine).start()
    landed(v_next.at[pl.ds(VDEEP, ny), theirs], mate_recv)
    pot_v[...] = v_next[pl.ds(VDEEP, ny), here] * (1.0 / SCALE) - shift
    pot_out = pltpu.make_async_copy(pot_v, pot_ref, in_sem.at[4])
    pot_out.start()
    for side in (0, 1):

        @pl.when(has[side])
        def _():
            landed(v_next.at[pl.ds(side * (ny + VDEEP), VDEEP)], v_next_recv.at[side])

    def back_copy(j, q):
        rows = pl.ds(quarter * q, quarter)
        return remote(
            result.at[:, j, rows, there],
            out_ref.at[:, own * gx + j, rows],
            row_send, back_recv, {"gx": ox},
        )

    def stay_copy(j, q):
        rows = pl.ds(quarter * q, quarter)
        return pltpu.make_async_copy(result.at[:, j, rows, here], out_ref.at[:, own * gx + j, rows], stay_sem)

    for j in range(own):
        for side in (0, 1):

            @pl.when(has[side])
            def _():
                halo_land(half, j, 1 - side, half_recv)

        def keep_result(y, x, combine):
            for p, value in enumerate(combine(step_length / 2)):
                result[p, j, y, pl.ds(x, 8)] = value

        def send_back(q):
            back_copy(j, q).start()
            stay_copy(j, q).start()

        exponential(half, v_next, j, keep_result, send_back)

    pot_out.wait()
    sent(orb_v, row_send)
    sent(orb_v, block_send)
    sent(dens, half_send)

    @pl.when(z_ok)
    def _():
        sent(v_now.at[pl.ds(0, 2 * VDEEP)], v_now_send)

    for d in (0, 1):

        @pl.when(has[d])
        def _():
            sent(v_next.at[pl.ds(0, VDEEP)], v_next_send.at[d])
            sent(half.at[:, :, pl.ds(0, 2 * DEEP), pl.ds(edge, 2 * nx)], side_send.at[d])

    pltpu.make_async_copy(result.at[..., here, :], out_ref.at[:, keep], stay_sem).wait()
    landed(out_ref.at[:, give], back_recv)


def whole_body(counts, orbitals, external):
    parts, nb, nx, ny, nz = orbitals.shape
    own = nb // 2
    nq = ny // 4
    dma = pltpu.SemaphoreType.DMA
    term = pltpu.VMEM((parts, own, ny + 2 * DEEP, 2 * nx + 16, nz), jnp.float32)
    block = pltpu.VMEM((ny, nx, nz), jnp.float32)
    half_block = pltpu.VMEM((ny // 2, nx, nz), jnp.float32)
    wide = pltpu.VMEM((ny + 2 * VDEEP, 2 * nx, nz), jnp.float32)
    result, potential = pl.pallas_call(
        functools.partial(whole_kernel, counts),
        out_shape=(
            jax.ShapeDtypeStruct((parts, nb, ny, nx, nz), jnp.float32),
            jax.ShapeDtypeStruct((ny, nx, nz), jnp.float32),
        ),
        in_specs=[pl.BlockSpec(memory_space=pltpu.HBM)] * 2,
        out_specs=(pl.BlockSpec(memory_space=pl.ANY),) * 2,
        scratch_shapes=[
            term, term, term, term, term,
            pltpu.VMEM((parts, nb, ny, nx, nz), jnp.float32),
            pltpu.VMEM((ny, 2 * nx, nz), jnp.float32),
            wide, wide,
            block, block, half_block, half_block,
            pltpu.VMEM((ny, 2 * nx, nz), jnp.float32),
            block,
            pltpu.VMEM((3, ny, nx, nz), jnp.float32),
            block,
            pltpu.VMEM((parts, own, ny, 2 * nx, nz), jnp.float32),
            block,
            pltpu.VMEM((2 * nz, nz), jnp.bfloat16),
            dma((5,)), dma, dma, dma, dma((2,)), dma, dma((2,)), dma,
            dma((own, nq)), dma((2, own)), dma((2, own)), dma, dma, dma, dma, dma((2,)),
            dma, dma((nq,)), dma((nq,)), dma((2,)), dma,
            pltpu.SemaphoreType.REGULAR,
        ],
        compiler_params=pltpu.CompilerParams(
            collective_id=0, has_side_effects=True, vmem_limit_bytes=32 * 1024 * 1024
        ),
    )(
        pltpu.with_memory_space_constraint(jnp.transpose(orbitals, (0, 1, 3, 2, 4)), pltpu.HBM),
        pltpu.with_memory_space_constraint(jnp.swapaxes(external, 0, 1), pltpu.HBM),
    )
    return jnp.transpose(result, (0, 1, 3, 2, 4)), jnp.swapaxes(potential, 0, 1)


def body(counts, orbitals, external):
    parts, nb, nx, ny, nz = orbitals.shape
    n_x, n_y, n_b = counts
    if n_x == 2 and n_b == 4 and parts * nb == 8 and nx % 8 == 0 and ny % 4 == 0 and ny >= 2 * VDEEP:
        return whole_body(counts, orbitals, external)
    return step_body(counts, orbitals, external)


def solution(mesh):
    counts = (mesh.shape["gx"], mesh.shape["gy"], mesh.shape["band"])
    in_specs = (P(None, "band", "gx", "gy", None), P("gx", "gy", None))
    out_specs = (P(None, "band", "gx", "gy", None), P("gx", "gy", None))
    return jax.shard_map(
        functools.partial(body, counts), mesh=mesh, in_specs=in_specs, out_specs=out_specs, check_vma=False
    )
```

```python
import functools

import jax
import jax.numpy as jnp
from jax import lax
from jax.experimental import pallas as pl
from jax.experimental.pallas import tpu as pltpu
from jax.sharding import PartitionSpec as P

step_length = 0.15
exchange_coef = 0.7386
centre_weight = -2.5
near_weight = 4.0 / 3.0
far_weight = -1.0 / 12.0
MESH = pl.DeviceIdType.MESH


def cube_root(d):
    guess = jnp.exp(jnp.log(d) * (1.0 / 3.0))
    better = guess - (guess - d / (guess * guess)) * (1.0 / 3.0)
    return jnp.where(d > 1e-30, better, guess)


def step_kernel(counts, orb_hbm, ext_hbm, out_ref, pot_ref, *scratch):
    terms = scratch[:8]
    orb_ref, ext_ref, pot_wide, density, in_sem, x_send, x_recv, y_send, y_recv, d_send, d_recv = scratch[8:]
    n_x, n_y, n_b = counts
    nf, ny, nx, nz = orb_ref.shape
    gx = lax.axis_index("gx")
    gy = lax.axis_index("gy")
    gb = lax.axis_index("band")
    has = {
        ("gx", 0): gx > 0,
        ("gx", 1): gx < n_x - 1,
        ("gy", 0): gy > 0,
        ("gy", 1): gy < n_y - 1,
    }
    place = {"gx": gx, "gy": gy}
    if n_x == 2:
        x_sides = [("gx", 1 - gx)]
    else:
        x_sides = [("gx", 0), ("gx", 1)]
    y_sides = [("gy", 0), ("gy", 1)]
    sides = [("gx", 0), ("gx", 1)] + y_sides
    peers = [lax.rem(gb + j, n_b) for j in range(1, n_b)]

    def target(side):
        axis, up = side
        return {axis: place[axis] + (2 * up - 1)}

    barrier = pltpu.get_barrier_semaphore()
    partners = n_b - 1
    for side in sides:
        partners = partners + has[side].astype(jnp.int32)

        @pl.when(has[side])
        def _():
            pl.semaphore_signal(barrier, inc=1, device_id=target(side), device_id_type=MESH)

    for peer in peers:
        pl.semaphore_signal(barrier, inc=1, device_id={"band": peer}, device_id_type=MESH)
    orb_in = pltpu.make_async_copy(orb_hbm, orb_ref, in_sem.at[0])
    orb_in.start()
    ext_in = pltpu.make_async_copy(ext_hbm, ext_ref, in_sem.at[1])
    ext_in.start()

    chunks = max(1, min(6, ny // 2))
    x_cuts = [(j * (ny // chunks), ny // chunks + (ny % chunks if j == chunks - 1 else 0)) for j in range(chunks)]
    mid = (nx - 4) // 2
    y_cuts = [(0, 2), (nx - 2, 2), (2, mid), (2 + mid, nx - 4 - mid)]
    d_cuts = [(0, 2), (ny - 2, 2), (2, ny - 4)]
    order = sorted(range(chunks), key=lambda j: 0 if j in (0, chunks - 1) else 1)
    sems = {"gx": (x_send, x_recv), "gy": (y_send, y_recv)}

    def cells(axis, edge, piece):
        if axis == "gx":
            return pl.ds(edge, 2), pl.ds(2 + x_cuts[piece][0], x_cuts[piece][1])
        return pl.ds(2 + y_cuts[piece][0], y_cuts[piece][1]), pl.ds(edge, 2)

    def pick(up, high, low):
        if isinstance(up, int):
            return high if up else low
        return low + up * (high - low)

    def send_copy(step, side, piece):
        axis, up = side
        extent = nx if axis == "gx" else ny
        return pltpu.make_async_remote_copy(
            src_ref=terms[step].at[cells(axis, pick(up, extent, 2), piece)],
            dst_ref=terms[step].at[cells(axis, pick(up, 0, extent + 2), piece)],
            send_sem=sems[axis][0].at[step, up, piece],
            recv_sem=sems[axis][1].at[step, 1 - up, piece],
            device_id=target(side),
            device_id_type=MESH,
        )

    def recv_copy(step, side, piece):
        axis, up = side
        extent = nx if axis == "gx" else ny
        land = terms[step].at[cells(axis, pick(up, extent + 2, 0), piece)]
        return pltpu.make_async_remote_copy(
            src_ref=land,
            dst_ref=land,
            send_sem=sems[axis][0].at[step, up, piece],
            recv_sem=sems[axis][1].at[step, up, piece],
            device_id=target(side),
            device_id_type=MESH,
        )

    def each(side, act):
        if side[0] == "gx" and n_x == 2:
            act()
        else:
            pl.when(has[side])(act)

    def start(step, side, pieces):
        def act():
            for piece in pieces:
                send_copy(step, side, piece).start()

        each(side, act)

    def await_pieces(step, side, pieces):
        def act():
            for piece in pieces:
                recv_copy(step, side, piece).wait_recv()

        each(side, act)

    def density_copy(which, j, piece):
        rows = pl.ds(*d_cuts[piece])
        return pltpu.make_async_remote_copy(
            src_ref=density.at[which, 0, rows],
            dst_ref=density.at[which, n_b - 1 - j, rows],
            send_sem=d_send.at[which, j, piece],
            recv_sem=d_recv.at[which, n_b - 2 - j, piece],
            device_id={"band": peers[j]},
            device_id_type=MESH,
        )

    def start_density(which, piece):
        for j in range(n_b - 1):
            density_copy(which, j, piece).start()

    def finish_potential(which):
        for piece in range(3):
            rows = pl.ds(*d_cuts[piece])
            for slot in range(1, n_b):
                pltpu.make_async_remote_copy(
                    src_ref=density.at[which, slot, rows],
                    dst_ref=density.at[which, slot, rows],
                    send_sem=d_send.at[which, slot - 1, piece],
                    recv_sem=d_recv.at[which, slot - 1, piece],
                    device_id={"band": peers[slot - 1]},
                    device_id_type=MESH,
                ).wait_recv()
        total = density[which, 0]
        for slot in range(1, n_b):
            total = total + density[which, slot]
        pot = ext_ref[...] - exchange_coef * cube_root(total)
        if which == 1:
            pot_ref[...] = pot
        wide = pot - 1.5 * centre_weight
        for y in range(ny):
            for x in range(nx):
                pot_wide[x, y] = jnp.broadcast_to(wide[y, x : x + 1], (nf, nz))

    for side in sides:
        axis, up = side

        @pl.when(jnp.logical_not(has[side]))
        def _():
            for step in range(8):
                if axis == "gx":
                    shape = (2, ny, nf, nz)
                    terms[step][pl.ds(nx + 2 if up else 0, 2), pl.ds(2, ny)] = jnp.zeros(shape, jnp.float32)
                else:
                    shape = (nx, 2, nf, nz)
                    terms[step][pl.ds(2, nx), pl.ds(ny + 2 if up else 0, 2)] = jnp.zeros(shape, jnp.float32)

    orb_in.wait()
    for y in range(ny):
        block = orb_ref[:, y]
        terms[0][pl.ds(2, nx), y + 2] = jnp.swapaxes(block, 0, 1)
        density[0, 0, y] = jnp.sum(block * block, axis=0)
    pl.semaphore_wait(barrier, partners)
    for side in x_sides:
        start(0, side, order)
    for side in y_sides:
        start(0, side, range(4))
    for piece in range(3):
        start_density(0, piece)
    ext_in.wait()

    lane = lax.broadcasted_iota(jnp.int32, (nf, nz), 1)
    near = -0.5 * near_weight
    far = -0.5 * far_weight
    below1 = jnp.where(lane >= 1, near, 0.0)
    above1 = jnp.where(lane < nz - 1, near, 0.0)
    below2 = jnp.where(lane >= 2, far, 0.0)
    above2 = jnp.where(lane < nz - 2, far, 0.0)
    half = nf // 2
    field = lax.broadcasted_iota(jnp.int32, (nf, nz), 0)
    turn_sign = jnp.where(field < half, 1.0, -1.0)

    def turned(v):
        return jnp.concatenate([v[half:], v[:half]], axis=0) * turn_sign

    def image(step, x, y):
        t = terms[step]
        c = t[x + 2, y + 2]
        one = (t[x + 1, y + 2] + t[x + 3, y + 2]) + (
            t[x + 2, y + 1] + t[x + 2, y + 3]
        )
        two = (t[x, y + 2] + t[x + 4, y + 2]) + (
            t[x + 2, y] + t[x + 2, y + 4]
        )
        total = pot_wide[x, y] * c + near * one + far * two
        total = total + pltpu.roll(c, 1, 1) * below1 + pltpu.roll(c, nz - 1, 1) * above1
        return total + (pltpu.roll(c, 2, 1) * below2 + pltpu.roll(c, nz - 2, 1) * above2)

    def combine(parts, s):
        even = parts[0] + (-(s**2) / 2) * parts[2] + (s**4 / 24) * parts[4]
        odd = s * parts[1] + (-(s**3) / 6) * parts[3]
        return even + turned(odd)

    def advance(step, xs, ys):
        at = [(x, y) for x in xs for y in ys]
        new = [image(step, x, y) for x, y in at]
        if step % 4 < 3:
            for (x, y), value in zip(at, new):
                terms[step + 1][x + 2, y + 2] = value
            return
        parts = [[terms[step - 3 + k][x + 2, y + 2] for k in range(4)] + [value] for (x, y), value in zip(at, new)]
        halves = [combine(part, step_length / 2) for part in parts]
        if step == 7:
            for (x, y), value in zip(at, halves):
                out_ref[x, y] = value
            return
        predicted = [combine(part, step_length) for part in parts]
        squares = [jnp.sum(value * value, axis=0, keepdims=True) for value in predicted]
        for (x, y), value, square in zip(at, halves, squares):
            terms[4][x + 2, y + 2] = value
            density[1, 0, y, pl.ds(x, 1)] = square

    rim = [0, 1, nx - 2, nx - 1]
    for step in range(8):
        if step % 4 == 0:
            finish_potential(step // 4)
        for n, j in enumerate(order):
            edges = [("gy", up) for up, at in ((0, 0), (1, chunks - 1)) if at == j]
            for side in x_sides:
                await_pieces(step, side, [j])
            for side in edges:
                await_pieces(step, side, [0, 1])
            advance(step, rim, range(x_cuts[j][0], sum(x_cuts[j])))
            if step < 7:
                for side in x_sides:
                    start(step + 1, side, [j])
                for side in edges:
                    start(step + 1, side, [0, 1])
            if n == min(1, chunks - 1):
                for piece in (2, 3):
                    for side in y_sides:
                        await_pieces(step, side, [piece])
                    advance(step, range(y_cuts[piece][0], sum(y_cuts[piece])), [0, 1, ny - 2, ny - 1])
                    if step < 7:
                        for side in y_sides:
                            start(step + 1, side, [piece])
                if step == 3:
                    start_density(1, 0)
                    start_density(1, 1)
        for x in range(2, nx - 2):
            advance(step, [x], range(2, ny - 2))
        if step == 3:
            start_density(1, 2)

    for side in x_sides + y_sides:

        def drain():
            for step in range(8):
                for piece in range(chunks if side[0] == "gx" else 4):
                    send_copy(step, side, piece).wait_send()

        each(side, drain)

    for which in (0, 1):
        for j in range(n_b - 1):
            for piece in range(3):
                density_copy(which, j, piece).wait_send()


def step_body(counts, orbitals, external):
    parts, bands, nx, ny, nz = orbitals.shape
    nf = parts * bands
    fields = jnp.transpose(orbitals.reshape(nf, nx, ny, nz), (0, 2, 1, 3))
    n_b = counts[2]
    dma = pltpu.SemaphoreType.DMA
    result, potential = pl.pallas_call(
        functools.partial(step_kernel, counts),
        out_shape=(
            jax.ShapeDtypeStruct((nx, ny, nf, nz), jnp.float32),
            jax.ShapeDtypeStruct((ny, nx, nz), jnp.float32),
        ),
        in_specs=[pl.BlockSpec(memory_space=pltpu.HBM)] * 2,
        out_specs=(pl.BlockSpec(memory_space=pltpu.VMEM),) * 2,
        scratch_shapes=[
            *[pltpu.VMEM((nx + 4, ny + 4, nf, nz), jnp.float32)] * 8,
            pltpu.VMEM((nf, ny, nx, nz), jnp.float32),
            pltpu.VMEM((ny, nx, nz), jnp.float32),
            pltpu.VMEM((nx, ny, nf, nz), jnp.float32),
            pltpu.VMEM((2, n_b, ny, nx, nz), jnp.float32),
            dma((2,)),
            dma((8, 2, 6)),
            dma((8, 2, 6)),
            dma((8, 2, 4)),
            dma((8, 2, 4)),
            dma((2, n_b - 1, 3)),
            dma((2, n_b - 1, 3)),
        ],
        compiler_params=pltpu.CompilerParams(
            collective_id=0, has_side_effects=True, vmem_limit_bytes=40 * 1024 * 1024
        ),
    )(fields, jnp.swapaxes(external, 0, 1))
    result = jnp.transpose(result, (2, 0, 1, 3)).reshape(orbitals.shape)
    return (result, jnp.swapaxes(potential, 0, 1))


DEEP = 8
VDEEP = 6
SCALE = 24.0


def whole_kernel(counts, orb_hbm, ext_hbm, out_ref, pot_ref, *scratch):
    (
        psi, half, t1, t2, t3, orb_v, ext_all, v_now, v_next, dens, chip_in, chip_sum, plane_in, partial, swap_in,
        pieces_in, done, result, pot_v, weights,
        in_sem, row_send, block_send, half_send, side_send, v_now_send, v_next_send, stay_sem,
        x_recv, halo_recv, half_recv, first_recv, second_recv, mate_recv, over_recv, v_side_recv,
        ext_recv, swap_recv, spread_recv, v_next_recv, back_recv, ready,
    ) = scratch
    n_x, n_y, n_b = counts
    parts, nb, ny, nx, nz = orb_hbm.shape
    own = nb // 2
    mid = ny // 2
    gx = lax.axis_index("gx")
    gy = lax.axis_index("gy")
    gb = lax.axis_index("band")
    ox = 1 - gx
    core = lax.rem(gb, 2)
    mate = gb + 1 - 2 * core
    far_gb = lax.rem(gb + 2, n_b)
    has = (gy > 0, gy < n_y - 1)
    edge = 8
    here = pl.ds(pl.multiple_of(nx * gx, nx), nx)
    there = pl.ds(pl.multiple_of(nx * ox, nx), nx)
    here_pad = pl.ds(pl.multiple_of(edge + nx * gx, 8), nx)
    there_pad = pl.ds(pl.multiple_of(edge + nx * ox, 8), nx)

    def z_peer(d):
        return gy + (2 * d - 1)

    in_plane = [{"band": mate}, {"band": far_gb}, {"gx": ox}]
    barrier = pltpu.get_barrier_semaphore()
    partners = len(in_plane)
    for peer in in_plane:
        pl.semaphore_signal(barrier, inc=1, device_id=peer, device_id_type=MESH)
    for d in (0, 1):
        partners = partners + has[d].astype(jnp.int32)

        @pl.when(has[d])
        def _():
            pl.semaphore_signal(barrier, inc=1, device_id={"gy": z_peer(d)}, device_id_type=MESH)

    give = pl.ds(pl.multiple_of(own * ox, own), own)
    keep = pl.ds(pl.multiple_of(own * gx, own), own)
    give_in = pltpu.make_async_copy(orb_hbm.at[:, give], orb_v.at[:, give], in_sem.at[0])
    keep_in = pltpu.make_async_copy(orb_hbm.at[:, keep], orb_v.at[:, keep], in_sem.at[1])
    ext_in = pltpu.make_async_copy(ext_hbm, ext_all.at[:, here], in_sem.at[2])
    psi_in = pltpu.make_async_copy(
        orb_hbm.at[:, keep], psi.at[:, :, pl.ds(DEEP, ny), here_pad], in_sem.at[3]
    )
    give_in.start()
    keep_in.start()
    ext_in.start()
    psi_in.start()

    def remote(src, dst, send, recv, peer):
        return pltpu.make_async_remote_copy(
            src_ref=src, dst_ref=dst, send_sem=send, recv_sem=recv, device_id=peer, device_id_type=MESH
        )

    def sent(like, sem):
        remote(like, like, sem, sem, {"band": mate}).wait_send()

    def landed(like, sem):
        remote(like, like, sem, sem, {"band": mate}).wait_recv()

    quarter = 4
    pieces = list(range(ny // quarter))
    goes = ([q for q in pieces if quarter * q < DEEP], [q for q in pieces if quarter * q >= ny - DEEP])
    piece_order = sorted(pieces, key=lambda q: 0 if q in goes[0] and q in goes[1] else 1)

    def x_copy(j, q):
        return remote(
            orb_v.at[:, own * ox + j, pl.ds(quarter * q, quarter)],
            psi.at[:, j, pl.ds(DEEP + quarter * q, quarter), here_pad],
            row_send, x_recv.at[j, q], {"gx": ox},
        )

    def x_land(j, q):
        land = psi.at[:, j, pl.ds(DEEP + quarter * q, quarter), there_pad]
        return remote(land, land, row_send, x_recv.at[j, q], {"gx": ox})

    def halo_row(d):
        return 0 if d else DEEP + ny

    def z_copy(j, d):
        return remote(
            orb_v.at[:, own * gx + j, pl.ds(ny - DEEP if d else 0, DEEP)],
            psi.at[:, j, pl.ds(halo_row(d), DEEP), here_pad],
            side_send.at[d], halo_recv.at[d, j], {"gy": z_peer(d)},
        )

    def halo_land(ref, j, d, sems):
        landed(ref.at[:, j, pl.ds(halo_row(d), DEEP), pl.ds(edge, 2 * nx)], sems.at[d, j])

    def f_row(d, q):
        return DEEP + quarter * q + (-ny if d else ny)

    def f_copy(j, d, q):
        return remote(
            psi.at[:, j, pl.ds(DEEP + quarter * q, quarter), there_pad],
            psi.at[:, j, pl.ds(f_row(d, q), quarter), there_pad],
            side_send.at[d], halo_recv.at[d, j], {"gy": z_peer(d)},
        )

    def h_copy(j, d):
        return remote(
            half.at[:, j, pl.ds(ny if d else DEEP, DEEP), pl.ds(edge, 2 * nx)],
            half.at[:, j, pl.ds(halo_row(d), DEEP), pl.ds(edge, 2 * nx)],
            side_send.at[d], half_recv.at[d, j], {"gy": z_peer(d)},
        )

    apart = lax.broadcasted_iota(jnp.int32, (2, nz, nz), 1) - lax.broadcasted_iota(jnp.int32, (2, nz, nz), 2)
    apart = jnp.abs(apart).reshape(2 * nz, nz)
    weights[...] = jnp.where(apart == 1, -16.0, jnp.where(apart == 2, 1.0, 0.0)).astype(jnp.bfloat16)
    zero = jnp.zeros((8, nz), jnp.float32)
    rows_all = ny + 2 * DEEP

    def clear(r, _):
        for p in range(parts):
            for j in range(own):
                for ref in (psi, half, t1, t2, t3):
                    ref[p, j, r, pl.ds(0, 8)] = zero
                    ref[p, j, r, pl.ds(edge + 2 * nx, 8)] = zero
        return 0

    lax.fori_loop(0, rows_all, clear, 0)
    for d in (0, 1):

        @pl.when(jnp.logical_not(has[d]))
        def _():
            def clear_row(i, _):
                r = i + halo_row(1 - d)
                for p in range(parts):
                    for j in range(own):
                        for ref in (psi, half):
                            for x in range(0, 2 * nx, 8):
                                ref[p, j, r, pl.ds(edge + x, 8)] = zero
                return 0

            lax.fori_loop(0, DEEP, clear_row, 0)
            for i in range(VDEEP):
                for x in range(0, 2 * nx, 8):
                    v_now[i + (0 if d == 0 else ny + VDEEP), pl.ds(x, 8)] = zero
                    v_next[i + (0 if d == 0 else ny + VDEEP), pl.ds(x, 8)] = zero

    give_in.wait()
    keep_in.wait()
    pl.semaphore_wait(barrier, partners)
    for j in range(own):
        for q in piece_order:
            x_copy(j, q).start()
    for d in (0, 1):

        @pl.when(has[d])
        def _():
            for j in range(own):
                z_copy(j, d).start()

    for y in range(ny):
        total = None
        for p in range(parts):
            for j in range(nb):
                v = orb_v[p, j, y]
                total = v * v if total is None else total + v * v
        dens[y] = total
    first = remote(dens, chip_in, block_send, first_recv, {"band": mate})
    first.start()
    ext_in.wait()
    first.wait_recv()
    pl.semaphore_signal(ready, inc=1, device_id={"gx": ox}, device_id_type=MESH)
    my_rows = pl.ds(mid * core, mid)
    chip_sum[...] = dens[my_rows] + chip_in[my_rows]
    second = remote(chip_sum, plane_in, half_send, second_recv, {"band": far_gb})
    second.start()

    def forward(j, q):
        x_land(j, q).wait_recv()
        for d in (0, 1):
            if q in goes[d]:

                @pl.when(has[d])
                def _():
                    f_copy(j, d, q).start()

    todo = [(j, q) for j in range(own) for q in piece_order]
    forward(*todo[0])
    second.wait_recv()
    pl.semaphore_wait(ready, 1)
    shift = -1.5 * centre_weight
    v_rows = pl.ds(VDEEP + mid * core, mid)
    mine_now = ext_all[my_rows, here] - exchange_coef * cube_root(chip_sum[...] + plane_in[...])
    v_now[v_rows, here] = (mine_now + shift) * SCALE

    own_slot = v_now.at[v_rows, here]
    to_mate = remote(own_slot, own_slot, half_send, mate_recv, {"band": mate})
    to_x = [
        remote(own_slot, own_slot, block_send, over_recv, {"gx": ox, "band": b})
        for n, b in enumerate((gb, mate))
    ]
    z_src = v_now.at[pl.ds(VDEEP + core * (ny - VDEEP), VDEEP), here]
    z_dst = v_now.at[pl.ds((1 - core) * (ny + VDEEP), VDEEP), here]
    z_to = gy + 2 * core - 1
    z_ok = jnp.logical_and(z_to >= 0, z_to < n_y)
    to_z = [
        remote(
            z_src, z_dst, v_now_send, v_side_recv.at[1 - core],
            {"gx": x, "gy": z_to, "band": b},
        )
        for m, x in enumerate((gx, ox))
        for n, b in enumerate((gb, mate))
    ]
    for copy in to_x:
        copy.start()

    @pl.when(z_ok)
    def _():
        for copy in to_z[2:] + to_z[:2]:
            copy.start()

    to_mate.start()
    ext_here, ext_there = ext_all.at[:, here], ext_all.at[:, there]
    ext_over = remote(ext_here, ext_here, block_send, ext_recv, {"gx": ox})
    for pair in todo[1:]:
        forward(*pair)

    landed(v_now.at[pl.ds(VDEEP + mid * (1 - core), mid), here], mate_recv)
    landed(v_now.at[pl.ds(VDEEP, ny), there], over_recv)
    for side in (0, 1):

        @pl.when(has[side])
        def _():
            landed(v_now.at[pl.ds(side * (ny + VDEEP), VDEEP)], v_side_recv.at[side])

    psi_in.wait()
    ext_over.start()

    cols = range(0, 2 * nx, 8)
    inside = [has[d].astype(jnp.float32) for d in (0, 1)]
    group = 4

    def images(src, pot, j, first_row, emit):
        centres, lhs = {}, []
        for r in range(first_row, first_row + group):
            for p in range(parts):
                c = src[p, j, r, pl.ds(edge, 2 * nx)]
                top = c.astype(jnp.bfloat16)
                rest = (c - top.astype(jnp.float32)).astype(jnp.bfloat16)
                centres[r, p] = c, 2 * nx * len(lhs)
                lhs.append(jnp.concatenate([top, rest], axis=1))
        lines = jnp.dot(jnp.concatenate(lhs, axis=0), weights[...], preferred_element_type=jnp.float32)
        for r in range(first_row, first_row + group):
            for x in cols:
                v = pot[r - DEEP + VDEEP, pl.ds(x, 8)]
                values = []
                for p in range(parts):

                    def at(row, col):
                        return src[p, j, row, pl.ds(edge + col, 8)]

                    c, place = centres[r, p]
                    one = (at(r, x - 1) + at(r, x + 1)) + (at(r - 1, x) + at(r + 1, x))
                    two = (at(r, x - 2) + at(r, x + 2)) + (at(r - 2, x) + at(r + 2, x))
                    line = lines[place + x : place + x + 8]
                    value = v * c[x : x + 8] + ((two - 16.0 * one) + line)
                    if r < DEEP:
                        value = value * inside[0]
                    if r >= DEEP + ny:
                        value = value * inside[1]
                    values.append(value)
                emit(r, x, values)

    def exponential(start, pot, j, act, after):
        terms = (start, t1, t2, t3)

        def store(dst):
            def emit(r, x, values):
                for p, value in enumerate(values):
                    dst[p, j, r, pl.ds(edge + x, 8)] = value

            return emit

        def finish(r, x, values):
            ts = [[t[p, j, r, pl.ds(edge + x, 8)] for t in terms] + [values[p]] for p in range(parts)]

            def combine(s):
                u = s / SCALE
                even = [ts[p][0] + (-(u**2) / 2) * ts[p][2] + (u**4 / 24) * ts[p][4] for p in range(2)]
                odd = [u * ts[p][1] + (-(u**3) / 6) * ts[p][3] for p in range(2)]
                return even[0] + odd[1], even[1] - odd[0]

            act(r - DEEP, x, combine)

        emits = [store(t1), store(t2), store(t3), finish]
        for g in range((ny + 12) // group + 3):
            for k, emit in enumerate(emits):
                deep = 6 - 2 * k
                i = g - k
                if 0 <= i < (ny + 2 * deep) // group:
                    images(terms[k], pot, j, DEEP - deep + group * i, emit)
                    if k == 3:
                        after(i)

    mine = pl.ds(pl.multiple_of(nx * core, nx), nx)
    theirs = pl.ds(pl.multiple_of(nx * (1 - core), nx), nx)

    def swap_copy(q):
        rows = pl.ds(quarter * q, quarter)
        return remote(partial.at[rows, theirs], swap_in.at[rows], block_send, swap_recv.at[q], {"band": mate})

    def spread_copy(q, n):
        rows = pl.ds(quarter * q, quarter)
        peer = ({"gx": ox, "band": far_gb}, {"gx": ox}, {"band": far_gb})[n]
        return remote(done.at[rows], pieces_in.at[n, rows], block_send, spread_recv.at[q], peer)

    def halo_span(q, d):
        low, high = (ny - VDEEP, ny) if d else (0, VDEEP)
        return max(low, quarter * q), min(high, quarter * (q + 1))

    def v_halo_out(q, d):
        copies = []
        for n, b in enumerate((gb, mate)):
            low, high = halo_span(q, d)
            src = v_next.at[pl.ds(VDEEP + low, high - low), mine]
            dst = v_next.at[pl.ds(VDEEP + low + (-ny if d else ny), high - low), mine]
            copies.append(
                remote(src, dst, v_next_send.at[d], v_next_recv.at[1 - d], {"gy": z_peer(d), "band": b})
            )
        return copies

    spans = [[q for q in pieces if halo_span(q, d)[0] < halo_span(q, d)[1]] for d in (0, 1)]

    def v_mate(q, tile):
        rows = v_next.at[pl.ds(VDEEP + quarter * q, quarter), tile]
        return remote(rows, rows, block_send, mate_recv, {"band": mate})

    for j in range(own):
        for side in (0, 1):

            @pl.when(has[side])
            def _():
                halo_land(psi, j, 1 - side, halo_recv)

        def keep_both(y, x, combine):
            for p, value in enumerate(combine(step_length / 2)):
                half[p, j, DEEP + y, pl.ds(edge + x, 8)] = value
            re, im = combine(step_length)
            square = re * re + im * im
            if j:
                square = square + partial[y, pl.ds(x, 8)]
            partial[y, pl.ds(x, 8)] = square

        def swap(i):
            if j == own - 1:
                swap_copy(i).start()

        exponential(psi, v_now, j, keep_both, swap)
        for d in (0, 1):

            @pl.when(has[d])
            def _():
                h_copy(j, d).start()

    for q in pieces:
        rows = pl.ds(quarter * q, quarter)
        swap_copy(q).wait_recv()
        done[rows] = partial[rows, mine] + swap_in[rows]
        for n in range(3):
            spread_copy(q, n).start()
    remote(ext_there, ext_there, block_send, ext_recv, {"gx": ox}).wait_recv()
    for q in pieces:
        rows = pl.ds(quarter * q, quarter)
        landed(pieces_in.at[:, rows], spread_recv.at[q])
        total = (done[rows] + pieces_in[0, rows]) + (pieces_in[1, rows] + pieces_in[2, rows])
        mine_next = ext_all[rows, mine] - exchange_coef * cube_root(total)
        v_next[pl.ds(VDEEP + quarter * q, quarter), mine] = (mine_next + shift) * SCALE
        for d in (0, 1):
            if q in spans[d]:

                @pl.when(has[d])
                def _():
                    for copy in v_halo_out(q, d):
                        copy.start()

        v_mate(q, mine).start()
    landed(v_next.at[pl.ds(VDEEP, ny), theirs], mate_recv)
    pot_v[...] = v_next[pl.ds(VDEEP, ny), here] * (1.0 / SCALE) - shift
    pot_out = pltpu.make_async_copy(pot_v, pot_ref, in_sem.at[4])
    pot_out.start()
    for side in (0, 1):

        @pl.when(has[side])
        def _():
            landed(v_next.at[pl.ds(side * (ny + VDEEP), VDEEP)], v_next_recv.at[side])

    def back_copy(j, q):
        rows = pl.ds(quarter * q, quarter)
        return remote(
            result.at[:, j, rows, there],
            out_ref.at[:, own * gx + j, rows],
            row_send, back_recv, {"gx": ox},
        )

    def stay_copy(j, q):
        rows = pl.ds(quarter * q, quarter)
        return pltpu.make_async_copy(result.at[:, j, rows, here], out_ref.at[:, own * gx + j, rows], stay_sem)

    for j in range(own):
        for side in (0, 1):

            @pl.when(has[side])
            def _():
                halo_land(half, j, 1 - side, half_recv)

        def keep_result(y, x, combine):
            for p, value in enumerate(combine(step_length / 2)):
                result[p, j, y, pl.ds(x, 8)] = value

        def send_back(q):
            back_copy(j, q).start()
            stay_copy(j, q).start()

        exponential(half, v_next, j, keep_result, send_back)

    pot_out.wait()
    sent(orb_v, row_send)
    sent(orb_v, block_send)
    sent(dens, half_send)

    @pl.when(z_ok)
    def _():
        sent(v_now.at[pl.ds(0, 2 * VDEEP)], v_now_send)

    for d in (0, 1):

        @pl.when(has[d])
        def _():
            sent(v_next.at[pl.ds(0, VDEEP)], v_next_send.at[d])
            sent(half.at[:, :, pl.ds(0, 2 * DEEP), pl.ds(edge, 2 * nx)], side_send.at[d])

    pltpu.make_async_copy(result.at[..., here, :], out_ref.at[:, keep], stay_sem).wait()
    landed(out_ref.at[:, give], back_recv)


def leave(result, potential, result_out, potential_out, sems):
    copies = [
        pltpu.make_async_copy(result, result_out, sems.at[0]),
        pltpu.make_async_copy(potential, potential_out, sems.at[1]),
    ]
    for copy in copies:
        copy.start()
    for copy in copies:
        copy.wait()


def whole_body(counts, orbitals, external):
    parts, nb, nx, ny, nz = orbitals.shape
    own = nb // 2
    nq = ny // 4
    dma = pltpu.SemaphoreType.DMA
    term = pltpu.VMEM((parts, own, ny + 2 * DEEP, 2 * nx + 16, nz), jnp.float32)
    block = pltpu.VMEM((ny, nx, nz), jnp.float32)
    half_block = pltpu.VMEM((ny // 2, nx, nz), jnp.float32)
    wide = pltpu.VMEM((ny + 2 * VDEEP, 2 * nx, nz), jnp.float32)
    result, potential = pl.pallas_call(
        functools.partial(whole_kernel, counts),
        out_shape=(
            jax.ShapeDtypeStruct((parts, nb, ny, nx, nz), jnp.float32),
            jax.ShapeDtypeStruct((ny, nx, nz), jnp.float32),
        ),
        in_specs=[pl.BlockSpec(memory_space=pltpu.HBM)] * 2,
        out_specs=(pl.BlockSpec(memory_space=pl.ANY),) * 2,
        scratch_shapes=[
            term, term, term, term, term,
            pltpu.VMEM((parts, nb, ny, nx, nz), jnp.float32),
            pltpu.VMEM((ny, 2 * nx, nz), jnp.float32),
            wide, wide,
            block, block, half_block, half_block,
            pltpu.VMEM((ny, 2 * nx, nz), jnp.float32),
            block,
            pltpu.VMEM((3, ny, nx, nz), jnp.float32),
            block,
            pltpu.VMEM((parts, own, ny, 2 * nx, nz), jnp.float32),
            block,
            pltpu.VMEM((2 * nz, nz), jnp.bfloat16),
            dma((5,)), dma, dma, dma, dma((2,)), dma, dma((2,)), dma,
            dma((own, nq)), dma((2, own)), dma((2, own)), dma, dma, dma, dma, dma((2,)),
            dma, dma((nq,)), dma((nq,)), dma((2,)), dma,
            pltpu.SemaphoreType.REGULAR,
        ],
        compiler_params=pltpu.CompilerParams(
            collective_id=0, has_side_effects=True, vmem_limit_bytes=32 * 1024 * 1024
        ),
    )(
        pltpu.with_memory_space_constraint(jnp.transpose(orbitals, (0, 1, 3, 2, 4)), pltpu.HBM),
        pltpu.with_memory_space_constraint(jnp.swapaxes(external, 0, 1), pltpu.HBM),
    )
    result, potential = pl.pallas_call(
        leave,
        out_shape=tuple(jax.ShapeDtypeStruct(a.shape, a.dtype) for a in (result, potential)),
        in_specs=[pl.BlockSpec(memory_space=pl.ANY)] * 2,
        out_specs=(pl.BlockSpec(memory_space=pl.ANY),) * 2,
        scratch_shapes=[dma((2,))],
        compiler_params=pltpu.CompilerParams(vmem_limit_bytes=4 * 1024 * 1024),
    )(result, potential)
    return jnp.transpose(result, (0, 1, 3, 2, 4)), jnp.swapaxes(potential, 0, 1)


def body(counts, orbitals, external):
    parts, nb, nx, ny, nz = orbitals.shape
    n_x, n_y, n_b = counts
    if n_x == 2 and n_b == 4 and parts * nb == 8 and nx % 8 == 0 and ny % 4 == 0 and ny >= 2 * VDEEP:
        return whole_body(counts, orbitals, external)
    return step_body(counts, orbitals, external)


def solution(mesh):
    counts = (mesh.shape["gx"], mesh.shape["gy"], mesh.shape["band"])
    in_specs = (P(None, "band", "gx", "gy", None), P("gx", "gy", None))
    out_specs = (P(None, "band", "gx", "gy", None), P("gx", "gy", None))
    return jax.shard_map(
        functools.partial(body, counts), mesh=mesh, in_specs=in_specs, out_specs=out_specs, check_vma=False
    )
```

```python
import functools

import jax
import jax.numpy as jnp
from jax import lax
from jax.experimental import pallas as pl
from jax.experimental.pallas import tpu as pltpu
from jax.sharding import PartitionSpec as P

step_length = 0.15
exchange_coef = 0.7386
centre_weight = -2.5
near_weight = 4.0 / 3.0
far_weight = -1.0 / 12.0
MESH = pl.DeviceIdType.MESH


def cube_root(d):
    guess = jnp.exp(jnp.log(d) * (1.0 / 3.0))
    better = guess - (guess - d / (guess * guess)) * (1.0 / 3.0)
    return jnp.where(d > 1e-30, better, guess)


def step_kernel(counts, orb_hbm, ext_hbm, out_ref, pot_ref, *scratch):
    terms = scratch[:8]
    orb_ref, ext_ref, pot_wide, density, in_sem, x_send, x_recv, y_send, y_recv, d_send, d_recv = scratch[8:]
    n_x, n_y, n_b = counts
    nf, ny, nx, nz = orb_ref.shape
    gx = lax.axis_index("gx")
    gy = lax.axis_index("gy")
    gb = lax.axis_index("band")
    has = {
        ("gx", 0): gx > 0,
        ("gx", 1): gx < n_x - 1,
        ("gy", 0): gy > 0,
        ("gy", 1): gy < n_y - 1,
    }
    place = {"gx": gx, "gy": gy}
    if n_x == 2:
        x_sides = [("gx", 1 - gx)]
    else:
        x_sides = [("gx", 0), ("gx", 1)]
    y_sides = [("gy", 0), ("gy", 1)]
    sides = [("gx", 0), ("gx", 1)] + y_sides
    peers = [lax.rem(gb + j, n_b) for j in range(1, n_b)]

    def target(side):
        axis, up = side
        return {axis: place[axis] + (2 * up - 1)}

    barrier = pltpu.get_barrier_semaphore()
    partners = n_b - 1
    for side in sides:
        partners = partners + has[side].astype(jnp.int32)

        @pl.when(has[side])
        def _():
            pl.semaphore_signal(barrier, inc=1, device_id=target(side), device_id_type=MESH)

    for peer in peers:
        pl.semaphore_signal(barrier, inc=1, device_id={"band": peer}, device_id_type=MESH)
    orb_in = pltpu.make_async_copy(orb_hbm, orb_ref, in_sem.at[0])
    orb_in.start()
    ext_in = pltpu.make_async_copy(ext_hbm, ext_ref, in_sem.at[1])
    ext_in.start()

    chunks = max(1, min(6, ny // 2))
    x_cuts = [(j * (ny // chunks), ny // chunks + (ny % chunks if j == chunks - 1 else 0)) for j in range(chunks)]
    mid = (nx - 4) // 2
    y_cuts = [(0, 2), (nx - 2, 2), (2, mid), (2 + mid, nx - 4 - mid)]
    d_cuts = [(0, 2), (ny - 2, 2), (2, ny - 4)]
    order = sorted(range(chunks), key=lambda j: 0 if j in (0, chunks - 1) else 1)
    sems = {"gx": (x_send, x_recv), "gy": (y_send, y_recv)}

    def cells(axis, edge, piece):
        if axis == "gx":
            return pl.ds(edge, 2), pl.ds(2 + x_cuts[piece][0], x_cuts[piece][1])
        return pl.ds(2 + y_cuts[piece][0], y_cuts[piece][1]), pl.ds(edge, 2)

    def pick(up, high, low):
        if isinstance(up, int):
            return high if up else low
        return low + up * (high - low)

    def send_copy(step, side, piece):
        axis, up = side
        extent = nx if axis == "gx" else ny
        return pltpu.make_async_remote_copy(
            src_ref=terms[step].at[cells(axis, pick(up, extent, 2), piece)],
            dst_ref=terms[step].at[cells(axis, pick(up, 0, extent + 2), piece)],
            send_sem=sems[axis][0].at[step, up, piece],
            recv_sem=sems[axis][1].at[step, 1 - up, piece],
            device_id=target(side),
            device_id_type=MESH,
        )

    def recv_copy(step, side, piece):
        axis, up = side
        extent = nx if axis == "gx" else ny
        land = terms[step].at[cells(axis, pick(up, extent + 2, 0), piece)]
        return pltpu.make_async_remote_copy(
            src_ref=land,
            dst_ref=land,
            send_sem=sems[axis][0].at[step, up, piece],
            recv_sem=sems[axis][1].at[step, up, piece],
            device_id=target(side),
            device_id_type=MESH,
        )

    def each(side, act):
        if side[0] == "gx" and n_x == 2:
            act()
        else:
            pl.when(has[side])(act)

    def start(step, side, pieces):
        def act():
            for piece in pieces:
                send_copy(step, side, piece).start()

        each(side, act)

    def await_pieces(step, side, pieces):
        def act():
            for piece in pieces:
                recv_copy(step, side, piece).wait_recv()

        each(side, act)

    def density_copy(which, j, piece):
        rows = pl.ds(*d_cuts[piece])
        return pltpu.make_async_remote_copy(
            src_ref=density.at[which, 0, rows],
            dst_ref=density.at[which, n_b - 1 - j, rows],
            send_sem=d_send.at[which, j, piece],
            recv_sem=d_recv.at[which, n_b - 2 - j, piece],
            device_id={"band": peers[j]},
            device_id_type=MESH,
        )

    def start_density(which, piece):
        for j in range(n_b - 1):
            density_copy(which, j, piece).start()

    def finish_potential(which):
        for piece in range(3):
            rows = pl.ds(*d_cuts[piece])
            for slot in range(1, n_b):
                pltpu.make_async_remote_copy(
                    src_ref=density.at[which, slot, rows],
                    dst_ref=density.at[which, slot, rows],
                    send_sem=d_send.at[which, slot - 1, piece],
                    recv_sem=d_recv.at[which, slot - 1, piece],
                    device_id={"band": peers[slot - 1]},
                    device_id_type=MESH,
                ).wait_recv()
        total = density[which, 0]
        for slot in range(1, n_b):
            total = total + density[which, slot]
        pot = ext_ref[...] - exchange_coef * cube_root(total)
        if which == 1:
            pot_ref[...] = pot
        wide = pot - 1.5 * centre_weight
        for y in range(ny):
            for x in range(nx):
                pot_wide[x, y] = jnp.broadcast_to(wide[y, x : x + 1], (nf, nz))

    for side in sides:
        axis, up = side

        @pl.when(jnp.logical_not(has[side]))
        def _():
            for step in range(8):
                if axis == "gx":
                    shape = (2, ny, nf, nz)
                    terms[step][pl.ds(nx + 2 if up else 0, 2), pl.ds(2, ny)] = jnp.zeros(shape, jnp.float32)
                else:
                    shape = (nx, 2, nf, nz)
                    terms[step][pl.ds(2, nx), pl.ds(ny + 2 if up else 0, 2)] = jnp.zeros(shape, jnp.float32)

    orb_in.wait()
    for y in range(ny):
        block = orb_ref[:, y]
        terms[0][pl.ds(2, nx), y + 2] = jnp.swapaxes(block, 0, 1)
        density[0, 0, y] = jnp.sum(block * block, axis=0)
    pl.semaphore_wait(barrier, partners)
    for side in x_sides:
        start(0, side, order)
    for side in y_sides:
        start(0, side, range(4))
    for piece in range(3):
        start_density(0, piece)
    ext_in.wait()

    lane = lax.broadcasted_iota(jnp.int32, (nf, nz), 1)
    near = -0.5 * near_weight
    far = -0.5 * far_weight
    below1 = jnp.where(lane >= 1, near, 0.0)
    above1 = jnp.where(lane < nz - 1, near, 0.0)
    below2 = jnp.where(lane >= 2, far, 0.0)
    above2 = jnp.where(lane < nz - 2, far, 0.0)
    half = nf // 2
    field = lax.broadcasted_iota(jnp.int32, (nf, nz), 0)
    turn_sign = jnp.where(field < half, 1.0, -1.0)

    def turned(v):
        return jnp.concatenate([v[half:], v[:half]], axis=0) * turn_sign

    def image(step, x, y):
        t = terms[step]
        c = t[x + 2, y + 2]
        one = (t[x + 1, y + 2] + t[x + 3, y + 2]) + (
            t[x + 2, y + 1] + t[x + 2, y + 3]
        )
        two = (t[x, y + 2] + t[x + 4, y + 2]) + (
            t[x + 2, y] + t[x + 2, y + 4]
        )
        total = pot_wide[x, y] * c + near * one + far * two
        total = total + pltpu.roll(c, 1, 1) * below1 + pltpu.roll(c, nz - 1, 1) * above1
        return total + (pltpu.roll(c, 2, 1) * below2 + pltpu.roll(c, nz - 2, 1) * above2)

    def combine(parts, s):
        even = parts[0] + (-(s**2) / 2) * parts[2] + (s**4 / 24) * parts[4]
        odd = s * parts[1] + (-(s**3) / 6) * parts[3]
        return even + turned(odd)

    def advance(step, xs, ys):
        at = [(x, y) for x in xs for y in ys]
        new = [image(step, x, y) for x, y in at]
        if step % 4 < 3:
            for (x, y), value in zip(at, new):
                terms[step + 1][x + 2, y + 2] = value
            return
        parts = [[terms[step - 3 + k][x + 2, y + 2] for k in range(4)] + [value] for (x, y), value in zip(at, new)]
        halves = [combine(part, step_length / 2) for part in parts]
        if step == 7:
            for (x, y), value in zip(at, halves):
                out_ref[x, y] = value
            return
        predicted = [combine(part, step_length) for part in parts]
        squares = [jnp.sum(value * value, axis=0, keepdims=True) for value in predicted]
        for (x, y), value, square in zip(at, halves, squares):
            terms[4][x + 2, y + 2] = value
            density[1, 0, y, pl.ds(x, 1)] = square

    rim = [0, 1, nx - 2, nx - 1]
    for step in range(8):
        if step % 4 == 0:
            finish_potential(step // 4)
        for n, j in enumerate(order):
            edges = [("gy", up) for up, at in ((0, 0), (1, chunks - 1)) if at == j]
            for side in x_sides:
                await_pieces(step, side, [j])
            for side in edges:
                await_pieces(step, side, [0, 1])
            advance(step, rim, range(x_cuts[j][0], sum(x_cuts[j])))
            if step < 7:
                for side in x_sides:
                    start(step + 1, side, [j])
                for side in edges:
                    start(step + 1, side, [0, 1])
            if n == min(1, chunks - 1):
                for piece in (2, 3):
                    for side in y_sides:
                        await_pieces(step, side, [piece])
                    advance(step, range(y_cuts[piece][0], sum(y_cuts[piece])), [0, 1, ny - 2, ny - 1])
                    if step < 7:
                        for side in y_sides:
                            start(step + 1, side, [piece])
                if step == 3:
                    start_density(1, 0)
                    start_density(1, 1)
        for x in range(2, nx - 2):
            advance(step, [x], range(2, ny - 2))
        if step == 3:
            start_density(1, 2)

    for side in x_sides + y_sides:

        def drain():
            for step in range(8):
                for piece in range(chunks if side[0] == "gx" else 4):
                    send_copy(step, side, piece).wait_send()

        each(side, drain)

    for which in (0, 1):
        for j in range(n_b - 1):
            for piece in range(3):
                density_copy(which, j, piece).wait_send()


def step_body(counts, orbitals, external):
    parts, bands, nx, ny, nz = orbitals.shape
    nf = parts * bands
    fields = jnp.transpose(orbitals.reshape(nf, nx, ny, nz), (0, 2, 1, 3))
    n_b = counts[2]
    dma = pltpu.SemaphoreType.DMA
    result, potential = pl.pallas_call(
        functools.partial(step_kernel, counts),
        out_shape=(
            jax.ShapeDtypeStruct((nx, ny, nf, nz), jnp.float32),
            jax.ShapeDtypeStruct((ny, nx, nz), jnp.float32),
        ),
        in_specs=[pl.BlockSpec(memory_space=pltpu.HBM)] * 2,
        out_specs=(pl.BlockSpec(memory_space=pltpu.VMEM),) * 2,
        scratch_shapes=[
            *[pltpu.VMEM((nx + 4, ny + 4, nf, nz), jnp.float32)] * 8,
            pltpu.VMEM((nf, ny, nx, nz), jnp.float32),
            pltpu.VMEM((ny, nx, nz), jnp.float32),
            pltpu.VMEM((nx, ny, nf, nz), jnp.float32),
            pltpu.VMEM((2, n_b, ny, nx, nz), jnp.float32),
            dma((2,)),
            dma((8, 2, 6)),
            dma((8, 2, 6)),
            dma((8, 2, 4)),
            dma((8, 2, 4)),
            dma((2, n_b - 1, 3)),
            dma((2, n_b - 1, 3)),
        ],
        compiler_params=pltpu.CompilerParams(
            collective_id=0, has_side_effects=True, vmem_limit_bytes=40 * 1024 * 1024
        ),
    )(fields, jnp.swapaxes(external, 0, 1))
    result = jnp.transpose(result, (2, 0, 1, 3)).reshape(orbitals.shape)
    return (result, jnp.swapaxes(potential, 0, 1))


DEEP = 8
VDEEP = 6
SCALE = 24.0


def whole_kernel(counts, orb_hbm, ext_hbm, out_ref, pot_ref, *scratch):
    (
        psi, half, t1, t2, t3, orb_v, ext_all, v_now, v_next, dens, chip_in, chip_sum, plane_in, partial, swap_in,
        pieces_in, done, result, local_result, pot_v, weights,
        in_sem, row_send, block_send, half_send, side_send, v_now_send, v_next_send, stay_sem,
        x_recv, halo_recv, half_recv, first_recv, second_recv, mate_recv, over_recv, v_side_recv,
        ext_recv, swap_recv, spread_recv, v_next_recv, back_recv, back_send, share_recv, share_side_send, share_halo_recv,
        local_sem, ready,
    ) = scratch
    n_x, n_y, n_b = counts
    parts, nb, ny, nx, nz = orb_hbm.shape
    own = nb // 2
    mid = ny // 2
    gx = lax.axis_index("gx")
    gy = lax.axis_index("gy")
    gb = lax.axis_index("band")
    ox = 1 - gx
    core = lax.rem(gb, 2)
    mate = gb + 1 - 2 * core
    far_gb = lax.rem(gb + 2, n_b)
    has = (gy > 0, gy < n_y - 1)
    edge = 8
    here = pl.ds(pl.multiple_of(nx * gx, nx), nx)
    there = pl.ds(pl.multiple_of(nx * ox, nx), nx)
    here_pad = pl.ds(pl.multiple_of(edge + nx * gx, 8), nx)
    there_pad = pl.ds(pl.multiple_of(edge + nx * ox, 8), nx)

    def z_peer(d):
        return gy + (2 * d - 1)

    in_plane = [{"band": mate}, {"band": far_gb}, {"gx": ox}]
    barrier = pltpu.get_barrier_semaphore()
    partners = len(in_plane)
    for peer in in_plane:
        pl.semaphore_signal(barrier, inc=1, device_id=peer, device_id_type=MESH)
    for d in (0, 1):
        partners = partners + has[d].astype(jnp.int32)

        @pl.when(has[d])
        def _():
            pl.semaphore_signal(barrier, inc=1, device_id={"gy": z_peer(d)}, device_id_type=MESH)

    give = pl.ds(pl.multiple_of(own * ox, own), own)
    keep = pl.ds(pl.multiple_of(own * gx, own), own)
    give_in = pltpu.make_async_copy(orb_hbm.at[:, give], orb_v.at[:, give], in_sem.at[0])
    keep_in = pltpu.make_async_copy(orb_hbm.at[:, keep], orb_v.at[:, keep], in_sem.at[1])
    ext_in = pltpu.make_async_copy(ext_hbm, ext_all.at[:, here], in_sem.at[2])
    psi_in = pltpu.make_async_copy(
        orb_hbm.at[:, keep], psi.at[:, :, pl.ds(DEEP, ny), here_pad], in_sem.at[3]
    )
    give_in.start()
    keep_in.start()
    ext_in.start()
    psi_in.start()

    def remote(src, dst, send, recv, peer):
        return pltpu.make_async_remote_copy(
            src_ref=src, dst_ref=dst, send_sem=send, recv_sem=recv, device_id=peer, device_id_type=MESH
        )

    def sent(like, sem):
        remote(like, like, sem, sem, {"band": mate}).wait_send()

    def landed(like, sem):
        remote(like, like, sem, sem, {"band": mate}).wait_recv()

    quarter = 4
    pieces = list(range(ny // quarter))
    goes = ([q for q in pieces if quarter * q < DEEP], [q for q in pieces if quarter * q >= ny - DEEP])
    piece_order = sorted(pieces, key=lambda q: 0 if q in goes[0] and q in goes[1] else 1)

    def x_copy(j, q):
        return remote(
            orb_v.at[:, own * ox + j, pl.ds(quarter * q, quarter)],
            psi.at[:, j, pl.ds(DEEP + quarter * q, quarter), here_pad],
            row_send, x_recv.at[j, q], {"gx": ox},
        )

    def x_land(j, q):
        land = psi.at[:, j, pl.ds(DEEP + quarter * q, quarter), there_pad]
        return remote(land, land, row_send, x_recv.at[j, q], {"gx": ox})

    def halo_row(d):
        return 0 if d else DEEP + ny

    def z_copy(j, d):
        return remote(
            orb_v.at[:, own * gx + j, pl.ds(ny - DEEP if d else 0, DEEP)],
            psi.at[:, j, pl.ds(halo_row(d), DEEP), here_pad],
            side_send.at[d], halo_recv.at[d, j], {"gy": z_peer(d)},
        )

    def halo_land(ref, j, d, sems):
        landed(ref.at[:, j, pl.ds(halo_row(d), DEEP), pl.ds(edge, 2 * nx)], sems.at[d, j])

    def f_row(d, q):
        return DEEP + quarter * q + (-ny if d else ny)

    def f_copy(j, d, q):
        return remote(
            psi.at[:, j, pl.ds(DEEP + quarter * q, quarter), there_pad],
            psi.at[:, j, pl.ds(f_row(d, q), quarter), there_pad],
            side_send.at[d], halo_recv.at[d, j], {"gy": z_peer(d)},
        )

    def h_copy(j, d):
        return remote(
            half.at[:, j, pl.ds(ny if d else DEEP, DEEP), pl.ds(edge, 2 * nx)],
            half.at[:, j, pl.ds(halo_row(d), DEEP), pl.ds(edge, 2 * nx)],
            side_send.at[d], half_recv.at[d, j], {"gy": z_peer(d)},
        )

    shared, guest, lone = 0, own, own - 1
    data = pl.ds(edge, 2 * nx)

    def share_copy(q):
        rows = pl.ds(DEEP + quarter * q, quarter)
        return remote(
            half.at[:, shared, rows, data], half.at[:, guest, rows, data], row_send, share_recv.at[q], {"gx": ox}
        )

    def share_rows(q):
        return half.at[:, guest, pl.ds(DEEP + quarter * q, quarter), data]

    def share_forward(q):
        rows = share_rows(q)
        for d in (0, 1):
            if q in goes[d]:

                @pl.when(has[d])
                def _():
                    remote(
                        rows, half.at[:, guest, pl.ds(f_row(d, q), quarter), data],
                        share_side_send.at[d], share_halo_recv.at[d], {"gy": z_peer(d)},
                    ).start()

    apart = lax.broadcasted_iota(jnp.int32, (2, nz, nz), 1) - lax.broadcasted_iota(jnp.int32, (2, nz, nz), 2)
    apart = jnp.abs(apart).reshape(2 * nz, nz)
    weights[...] = jnp.where(apart == 1, -16.0, jnp.where(apart == 2, 1.0, 0.0)).astype(jnp.bfloat16)
    zero = jnp.zeros((8, nz), jnp.float32)
    rows_all = ny + 2 * DEEP

    def clear(r, _):
        for p in range(parts):
            for ref in (psi, half, t1, t2, t3):
                for j in range(ref.shape[1]):
                    ref[p, j, r, pl.ds(0, 8)] = zero
                    ref[p, j, r, pl.ds(edge + 2 * nx, 8)] = zero
        return 0

    lax.fori_loop(0, rows_all, clear, 0)
    for d in (0, 1):

        @pl.when(jnp.logical_not(has[d]))
        def _():
            def clear_row(i, _):
                r = i + halo_row(1 - d)
                for p in range(parts):
                    for ref in (psi, half):
                        for j in range(ref.shape[1]):
                            for x in range(0, 2 * nx, 8):
                                ref[p, j, r, pl.ds(edge + x, 8)] = zero
                return 0

            lax.fori_loop(0, DEEP, clear_row, 0)
            for i in range(VDEEP):
                for x in range(0, 2 * nx, 8):
                    v_now[i + (0 if d == 0 else ny + VDEEP), pl.ds(x, 8)] = zero
                    v_next[i + (0 if d == 0 else ny + VDEEP), pl.ds(x, 8)] = zero

    give_in.wait()
    keep_in.wait()
    pl.semaphore_wait(barrier, partners)
    for j in range(own):
        for q in piece_order:
            x_copy(j, q).start()
    for d in (0, 1):

        @pl.when(has[d])
        def _():
            for j in range(own):
                z_copy(j, d).start()

    for y in range(ny):
        total = None
        for p in range(parts):
            for j in range(nb):
                v = orb_v[p, j, y]
                total = v * v if total is None else total + v * v
        dens[y] = total
    first = remote(dens, chip_in, block_send, first_recv, {"band": mate})
    first.start()
    ext_in.wait()
    first.wait_recv()
    pl.semaphore_signal(ready, inc=1, device_id={"gx": ox}, device_id_type=MESH)
    my_rows = pl.ds(mid * core, mid)
    chip_sum[...] = dens[my_rows] + chip_in[my_rows]
    second = remote(chip_sum, plane_in, half_send, second_recv, {"band": far_gb})
    second.start()

    def forward(j, q):
        x_land(j, q).wait_recv()
        for d in (0, 1):
            if q in goes[d]:

                @pl.when(has[d])
                def _():
                    f_copy(j, d, q).start()

    todo = [(j, q) for j in range(own) for q in piece_order]
    forward(*todo[0])
    second.wait_recv()
    pl.semaphore_wait(ready, 1)
    shift = -1.5 * centre_weight
    v_rows = pl.ds(VDEEP + mid * core, mid)
    mine_now = ext_all[my_rows, here] - exchange_coef * cube_root(chip_sum[...] + plane_in[...])
    v_now[v_rows, here] = (mine_now + shift) * SCALE

    own_slot = v_now.at[v_rows, here]
    to_mate = remote(own_slot, own_slot, half_send, mate_recv, {"band": mate})
    to_x = [
        remote(own_slot, own_slot, block_send, over_recv, {"gx": ox, "band": b})
        for n, b in enumerate((gb, mate))
    ]
    z_src = v_now.at[pl.ds(VDEEP + core * (ny - VDEEP), VDEEP), here]
    z_dst = v_now.at[pl.ds((1 - core) * (ny + VDEEP), VDEEP), here]
    z_to = gy + 2 * core - 1
    z_ok = jnp.logical_and(z_to >= 0, z_to < n_y)
    to_z = [
        remote(
            z_src, z_dst, v_now_send, v_side_recv.at[1 - core],
            {"gx": x, "gy": z_to, "band": b},
        )
        for m, x in enumerate((gx, ox))
        for n, b in enumerate((gb, mate))
    ]
    for copy in to_x:
        copy.start()

    @pl.when(z_ok)
    def _():
        for copy in to_z[2:] + to_z[:2]:
            copy.start()

    to_mate.start()
    ext_here, ext_there = ext_all.at[:, here], ext_all.at[:, there]
    ext_over = remote(ext_here, ext_here, block_send, ext_recv, {"gx": ox})
    for pair in todo[1:]:
        forward(*pair)

    landed(v_now.at[pl.ds(VDEEP + mid * (1 - core), mid), here], mate_recv)
    landed(v_now.at[pl.ds(VDEEP, ny), there], over_recv)
    for side in (0, 1):

        @pl.when(has[side])
        def _():
            landed(v_now.at[pl.ds(side * (ny + VDEEP), VDEEP)], v_side_recv.at[side])

    psi_in.wait()
    ext_over.start()

    cols = range(0, 2 * nx, 8)
    inside = [has[d].astype(jnp.float32) for d in (0, 1)]
    group = 4

    def images(src, pot, j, first_row, emit):
        centres, lhs = {}, []
        for r in range(first_row, first_row + group):
            for p in range(parts):
                c = src[p, j, r, pl.ds(edge, 2 * nx)]
                top = c.astype(jnp.bfloat16)
                rest = (c - top.astype(jnp.float32)).astype(jnp.bfloat16)
                centres[r, p] = c, 2 * nx * len(lhs)
                lhs.append(jnp.concatenate([top, rest], axis=1))
        lines = jnp.dot(jnp.concatenate(lhs, axis=0), weights[...], preferred_element_type=jnp.float32)
        for r in range(first_row, first_row + group):
            for x in cols:
                v = pot[r - DEEP + VDEEP, pl.ds(x, 8)]
                values = []
                for p in range(parts):

                    def at(row, col):
                        return src[p, j, row, pl.ds(edge + col, 8)]

                    c, place = centres[r, p]
                    one = (at(r, x - 1) + at(r, x + 1)) + (at(r - 1, x) + at(r + 1, x))
                    two = (at(r, x - 2) + at(r, x + 2)) + (at(r - 2, x) + at(r + 2, x))
                    line = lines[place + x : place + x + 8]
                    value = v * c[x : x + 8] + ((two - 16.0 * one) + line)
                    if r < DEEP:
                        value = value * inside[0]
                    if r >= DEEP + ny:
                        value = value * inside[1]
                    values.append(value)
                emit(r, x, values)

    def images_here(src, pot, j, first_row, emit):
        for x in range(0, nx, 8):
            base = edge + nx * gx + x
            centres, lhs = {}, []
            for r in range(first_row, first_row + group):
                cs = [src[p, j, r, pl.ds(pl.multiple_of(base, 8), 8)] for p in range(parts)]
                c = jnp.concatenate(cs, axis=0)
                top = c.astype(jnp.bfloat16)
                rest = (c - top.astype(jnp.float32)).astype(jnp.bfloat16)
                centres[r] = cs, 8 * parts * len(lhs)
                lhs.append(jnp.concatenate([top, rest], axis=1))
            lines = jnp.dot(jnp.concatenate(lhs, axis=0), weights[...], preferred_element_type=jnp.float32)
            for r in range(first_row, first_row + group):
                v = pot[r - DEEP + VDEEP, pl.ds(pl.multiple_of(nx * gx + x, 8), 8)]
                values = []
                for p in range(parts):

                    def at(row, col):
                        return src[p, j, row, pl.ds(base + col, 8)]

                    def by(row):
                        return src[p, j, row, pl.ds(pl.multiple_of(base, 8), 8)]

                    cs, place = centres[r]
                    one = (at(r, -1) + at(r, 1)) + (by(r - 1) + by(r + 1))
                    two = (at(r, -2) + at(r, 2)) + (by(r - 2) + by(r + 2))
                    line = lines[place + 8 * p : place + 8 * p + 8]
                    values.append(v * cs[p] + ((two - 16.0 * one) + line))
                emit(r, x, values)

    def exponential(start, pot, j, act, after, only_here=False):
        terms = (start, t1, t2, t3)

        def store(dst):
            def emit(r, x, values):
                for p, value in enumerate(values):
                    dst[p, j, r, pl.ds(edge + x, 8)] = value

            return emit

        def finish(r, x, values):
            place = pl.multiple_of(edge + nx * gx + x, 8) if only_here else edge + x
            ts = [[t[p, j, r, pl.ds(place, 8)] for t in terms] + [values[p]] for p in range(parts)]

            def combine(s):
                u = s / SCALE
                even = [ts[p][0] + (-(u**2) / 2) * ts[p][2] + (u**4 / 24) * ts[p][4] for p in range(2)]
                odd = [u * ts[p][1] + (-(u**3) / 6) * ts[p][3] for p in range(2)]
                return even[0] + odd[1], even[1] - odd[0]

            act(r - DEEP, x, combine)

        emits = [store(t1), store(t2), store(t3), finish]
        for g in range((ny + 12) // group + 3):
            for k, emit in enumerate(emits):
                deep = 6 - 2 * k
                i = g - k
                if 0 <= i < (ny + 2 * deep) // group:
                    make = images_here if only_here and k == 3 else images
                    make(terms[k], pot, j, DEEP - deep + group * i, emit)
                    if k == 3:
                        after(i)

    mine = pl.ds(pl.multiple_of(nx * core, nx), nx)
    theirs = pl.ds(pl.multiple_of(nx * (1 - core), nx), nx)

    def swap_copy(q):
        rows = pl.ds(quarter * q, quarter)
        return remote(partial.at[rows, theirs], swap_in.at[rows], block_send, swap_recv.at[q], {"band": mate})

    def spread_copy(q, n):
        rows = pl.ds(quarter * q, quarter)
        peer = ({"gx": ox, "band": far_gb}, {"gx": ox}, {"band": far_gb})[n]
        return remote(done.at[rows], pieces_in.at[n, rows], block_send, spread_recv.at[q], peer)

    def halo_span(q, d):
        low, high = (ny - VDEEP, ny) if d else (0, VDEEP)
        return max(low, quarter * q), min(high, quarter * (q + 1))

    def v_halo_out(q, d):
        copies = []
        for n, b in enumerate((gb, mate)):
            low, high = halo_span(q, d)
            src = v_next.at[pl.ds(VDEEP + low, high - low), mine]
            dst = v_next.at[pl.ds(VDEEP + low + (-ny if d else ny), high - low), mine]
            copies.append(
                remote(src, dst, v_next_send.at[d], v_next_recv.at[1 - d], {"gy": z_peer(d), "band": b})
            )
        return copies

    spans = [[q for q in pieces if halo_span(q, d)[0] < halo_span(q, d)[1]] for d in (0, 1)]

    def v_mate(q, tile):
        rows = v_next.at[pl.ds(VDEEP + quarter * q, quarter), tile]
        return remote(rows, rows, block_send, mate_recv, {"band": mate})

    for j in range(own):
        for side in (0, 1):

            @pl.when(has[side])
            def _():
                halo_land(psi, j, 1 - side, halo_recv)

        def keep_both(y, x, combine):
            for p, value in enumerate(combine(step_length / 2)):
                half[p, j, DEEP + y, pl.ds(edge + x, 8)] = value
            re, im = combine(step_length)
            square = re * re + im * im
            if j:
                square = square + partial[y, pl.ds(x, 8)]
            partial[y, pl.ds(x, 8)] = square

        def swap(i):
            if j == own - 1:
                swap_copy(i).start()

        exponential(psi, v_now, j, keep_both, swap)
        for d in (0, 1):

            @pl.when(has[d])
            def _():
                h_copy(j, d).start()

        if j == shared:
            share_copy(piece_order[0]).start()

    for q in pieces:
        rows = pl.ds(quarter * q, quarter)
        swap_copy(q).wait_recv()
        done[rows] = partial[rows, mine] + swap_in[rows]
        for n in range(3):
            spread_copy(q, n).start()
    landed(share_rows(piece_order[0]), share_recv.at[piece_order[0]])
    for q in piece_order[1:]:
        share_copy(q).start()
    remote(ext_there, ext_there, block_send, ext_recv, {"gx": ox}).wait_recv()
    for q in pieces:
        rows = pl.ds(quarter * q, quarter)
        landed(pieces_in.at[:, rows], spread_recv.at[q])
        total = (done[rows] + pieces_in[0, rows]) + (pieces_in[1, rows] + pieces_in[2, rows])
        mine_next = ext_all[rows, mine] - exchange_coef * cube_root(total)
        v_next[pl.ds(VDEEP + quarter * q, quarter), mine] = (mine_next + shift) * SCALE
        for d in (0, 1):
            if q in spans[d]:

                @pl.when(has[d])
                def _():
                    for copy in v_halo_out(q, d):
                        copy.start()

        v_mate(q, mine).start()
    share_forward(piece_order[0])
    landed(v_next.at[pl.ds(VDEEP, ny), theirs], mate_recv)
    pot_v[...] = v_next[pl.ds(VDEEP, ny), here] * (1.0 / SCALE) - shift
    pot_out = pltpu.make_async_copy(pot_v, pot_ref, in_sem.at[4])
    pot_out.start()
    for q in piece_order[1:]:
        landed(share_rows(q), share_recv.at[q])
        share_forward(q)
    for side in (0, 1):

        @pl.when(has[side])
        def _():
            landed(v_next.at[pl.ds(side * (ny + VDEEP), VDEEP)], v_next_recv.at[side])

    for side in (0, 1):

        @pl.when(has[side])
        def _():
            halo_land(half, lone, 1 - side, half_recv)

    def keep_result(y, x, combine):
        for p, value in enumerate(combine(step_length / 2)):
            result[p, y, pl.ds(x, 8)] = value

    def send_back(q):
        rows = pl.ds(quarter * q, quarter)
        place = own * gx + lone
        remote(result.at[:, rows, there], out_ref.at[:, place, rows], back_send, back_recv, {"gx": ox}).start()
        pltpu.make_async_copy(result.at[:, rows, here], out_ref.at[:, place, rows], stay_sem).start()

    exponential(half, v_next, lone, keep_result, send_back)
    for n, (j, side_x) in enumerate(((shared, gx), (guest, ox))):
        for side in (0, 1):

            @pl.when(has[side])
            def _():
                if j == guest:
                    landed(half.at[:, guest, pl.ds(halo_row(1 - side), DEEP), data], share_halo_recv.at[1 - side])
                else:
                    halo_land(half, j, 1 - side, half_recv)

        def keep_local(y, x, combine):
            for p, value in enumerate(combine(step_length / 2)):
                local_result[p, n, y, pl.ds(x, 8)] = value

        exponential(half, v_next, j, keep_local, lambda i: None, only_here=True)
        pltpu.make_async_copy(local_result.at[:, n], out_ref.at[:, own * side_x + shared], local_sem).start()

    pot_out.wait()
    sent(orb_v, row_send)
    sent(orb_v, block_send)
    sent(dens, half_send)

    @pl.when(z_ok)
    def _():
        sent(v_now.at[pl.ds(0, 2 * VDEEP)], v_now_send)

    for d in (0, 1):

        @pl.when(has[d])
        def _():
            sent(v_next.at[pl.ds(0, VDEEP)], v_next_send.at[d])
            sent(half.at[:, pl.ds(0, own), pl.ds(0, 2 * DEEP), data], side_send.at[d])
            sent(half.at[:, guest, pl.ds(0, DEEP), data], share_side_send.at[d])

    sent(orb_v.at[:, 0], back_send)
    pltpu.make_async_copy(orb_v.at[:, 0], out_ref.at[:, 0], stay_sem).wait()
    pltpu.make_async_copy(orb_v.at[:, pl.ds(0, own)], out_ref.at[:, pl.ds(0, own)], local_sem).wait()
    landed(out_ref.at[:, own * ox + lone], back_recv)


def leave(result, potential, result_out, potential_out, sems):
    copies = [
        pltpu.make_async_copy(result, result_out, sems.at[0]),
        pltpu.make_async_copy(potential, potential_out, sems.at[1]),
    ]
    for copy in copies:
        copy.start()
    for copy in copies:
        copy.wait()


def whole_body(counts, orbitals, external):
    parts, nb, nx, ny, nz = orbitals.shape
    own = nb // 2
    nq = ny // 4
    dma = pltpu.SemaphoreType.DMA
    start, term = [pltpu.VMEM((parts, n, ny + 2 * DEEP, 2 * nx + 16, nz), jnp.float32) for n in (own, own + 1)]
    block = pltpu.VMEM((ny, nx, nz), jnp.float32)
    half_block = pltpu.VMEM((ny // 2, nx, nz), jnp.float32)
    wide = pltpu.VMEM((ny + 2 * VDEEP, 2 * nx, nz), jnp.float32)
    result, potential = pl.pallas_call(
        functools.partial(whole_kernel, counts),
        out_shape=(
            jax.ShapeDtypeStruct((parts, nb, ny, nx, nz), jnp.float32),
            jax.ShapeDtypeStruct((ny, nx, nz), jnp.float32),
        ),
        in_specs=[pl.BlockSpec(memory_space=pltpu.HBM)] * 2,
        out_specs=(pl.BlockSpec(memory_space=pl.ANY),) * 2,
        scratch_shapes=[
            start, term, term, term, term,
            pltpu.VMEM((parts, nb, ny, nx, nz), jnp.float32),
            pltpu.VMEM((ny, 2 * nx, nz), jnp.float32),
            wide, wide,
            block, block, half_block, half_block,
            pltpu.VMEM((ny, 2 * nx, nz), jnp.float32),
            block,
            pltpu.VMEM((3, ny, nx, nz), jnp.float32),
            block,
            pltpu.VMEM((parts, ny, 2 * nx, nz), jnp.float32),
            pltpu.VMEM((parts, 2, ny, nx, nz), jnp.float32),
            block,
            pltpu.VMEM((2 * nz, nz), jnp.bfloat16),
            dma((5,)), dma, dma, dma, dma((2,)), dma, dma((2,)), dma,
            dma((own, nq)), dma((2, own)), dma((2, own)), dma, dma, dma, dma, dma((2,)),
            dma, dma((nq,)), dma((nq,)), dma((2,)), dma, dma, dma((nq,)), dma((2,)), dma((2,)),
            dma,
            pltpu.SemaphoreType.REGULAR,
        ],
        compiler_params=pltpu.CompilerParams(
            collective_id=0, has_side_effects=True, vmem_limit_bytes=32 * 1024 * 1024
        ),
    )(
        pltpu.with_memory_space_constraint(jnp.transpose(orbitals, (0, 1, 3, 2, 4)), pltpu.HBM),
        pltpu.with_memory_space_constraint(jnp.swapaxes(external, 0, 1), pltpu.HBM),
    )
    result, potential = pl.pallas_call(
        leave,
        out_shape=tuple(jax.ShapeDtypeStruct(a.shape, a.dtype) for a in (result, potential)),
        in_specs=[pl.BlockSpec(memory_space=pl.ANY)] * 2,
        out_specs=(pl.BlockSpec(memory_space=pl.ANY),) * 2,
        scratch_shapes=[dma((2,))],
        compiler_params=pltpu.CompilerParams(vmem_limit_bytes=4 * 1024 * 1024),
    )(result, potential)
    return jnp.transpose(result, (0, 1, 3, 2, 4)), jnp.swapaxes(potential, 0, 1)


def body(counts, orbitals, external):
    parts, nb, nx, ny, nz = orbitals.shape
    n_x, n_y, n_b = counts
    if n_x == 2 and n_b == 4 and parts * nb == 8 and nx % 8 == 0 and ny % 4 == 0 and ny >= 2 * VDEEP:
        return whole_body(counts, orbitals, external)
    return step_body(counts, orbitals, external)


def solution(mesh):
    counts = (mesh.shape["gx"], mesh.shape["gy"], mesh.shape["band"])
    in_specs = (P(None, "band", "gx", "gy", None), P("gx", "gy", None))
    out_specs = (P(None, "band", "gx", "gy", None), P("gx", "gy", None))
    return jax.shard_map(
        functools.partial(body, counts), mesh=mesh, in_specs=in_specs, out_specs=out_specs, check_vma=False
    )
```
